32 devices in a mesh: dp: 2 (over x), tp: 4 (over z), sp: 4 (over y, core).
Axes of the slice: x: 2, y: 2, z: 4, core: 2. Of those that a mesh axis runs over, the one named last changes fastest.
Arguments:
- k_cache: bfloat16 [4, 8, 8, 8192, 64], P(None, 'dp', 'tp', 'sp'), parts along dimension 1
- v_cache: bfloat16 [4, 8, 8, 8192, 64], P(None, 'dp', 'tp', 'sp'), parts along dimension 1
- lengths: int32 [8], P('dp'), parts along dimension 0
- hidden: bfloat16 [8, 2048], P(('dp', 'sp')), parts along dimension 0
- ln_gain: bfloat16 [4, 2048], replicated
- w_query: bfloat16 [4, 2048, 2048], P(None, None, 'tp')
- w_key: bfloat16 [4, 2048, 512], P(None, None, 'tp')
- w_value: bfloat16 [4, 2048, 512], P(None, None, 'tp')
- w_out: bfloat16 [4, 2048, 2048], P(None, 'tp')
- w_gate: bfloat16 [4, 2048, 8192], P(None, None, 'tp')
- w_up: bfloat16 [4, 2048, 8192], P(None, None, 'tp')
- w_down: bfloat16 [4, 8192, 2048], P(None, 'tp')
Outputs:
- output 1: bfloat16 [8, 2048], P(('dp', 'sp')), parts along dimension 0
- output 2: bfloat16 [3, 8, 8, 4096, 64], P(None, ('dp', 'sp'), 'tp'), parts along dimension 1
- output 3: bfloat16 [3, 8, 8, 4096, 64], P(None, ('dp', 'sp'), 'tp'), parts along dimension 1
- output 4: bfloat16 [8, 8, 8192, 64], P(('dp', 'sp'), 'tp'), parts along dimension 0
- output 5: bfloat16 [8, 8, 8192, 64], P(('dp', 'sp'), 'tp'), parts along dimension 0
There are 2 independent parts. The reference program is written for one: setup_inputs(seed, part) draws one part's arguments, and reference() takes and returns one part's arrays. A program takes and returns all parts, laid end to end along the dimension named above; an argument that names none is the same for every part.
All inputs are finite; a program needn't handle non-finite values.
Results may differ from the reference program's by a relative error of at most 0.02.
Values are sent between devices in bfloat16 or wider.
A program may use at most 1 GiB of HBM per device.

```python
import jax
import jax.numpy as jnp
from jax import lax

N_ROWS = 4
SEQ_LEN = 8192
MODEL_DIM = 2048
N_HEADS = 32
KV_HEADS = 8
HEAD_DIM = 64
FFN_DIM = 8192
WINDOW = 4096
ROPE_BASE = 50000
N_LAYERS = 4
NORM_EPS = 1e-5


def scaled_normal(key_in, shape, fan_in, spread=1.0):
    return (jax.random.normal(key_in, shape, jnp.float32) * (spread * fan_in ** -0.5)).astype(jnp.bfloat16)


def draw_lengths(len_key):
    key_lo, key_hi = jax.random.split(len_key)
    lengths = jax.random.randint(key_lo, (N_ROWS,), WINDOW + 1, SEQ_LEN, jnp.int32)
    order = jax.random.permutation(key_hi, N_ROWS)
    lengths = lengths.at[order[0]].set(SEQ_LEN - 1)
    return lengths.at[order[1]].set(WINDOW + 1)


def setup_inputs(seed: int = 0, part: int = 0) -> dict:
    base_key = jax.random.key(seed)
    part_key = jax.random.fold_in(base_key, part)
    part_keys = jax.random.split(part_key, 3)
    cache_shape = (N_LAYERS, N_ROWS, KV_HEADS, SEQ_LEN, HEAD_DIM)
    k_cache = (2.5 * jax.random.normal(part_keys[0], cache_shape, jnp.float32)).astype(jnp.bfloat16)
    v_cache = jax.random.normal(part_keys[1], cache_shape, jnp.float32).astype(jnp.bfloat16)
    hidden = jax.random.normal(part_keys[2], (N_ROWS, MODEL_DIM), jnp.float32).astype(jnp.bfloat16)
    lengths = draw_lengths(jax.random.fold_in(part_key, 3))
    shared = jax.random.split(jax.random.fold_in(base_key, 1000), 8)
    q_width = N_HEADS * HEAD_DIM
    kv_width = KV_HEADS * HEAD_DIM
    ln_gain = jax.random.uniform(shared[0], (N_LAYERS, MODEL_DIM), jnp.float32, 0.5, 1.5).astype(jnp.bfloat16)
    return {
        "k_cache": k_cache,
        "v_cache": v_cache,
        "lengths": lengths,
        "hidden": hidden,
        "ln_gain": ln_gain,
        "w_query": scaled_normal(shared[1], (N_LAYERS, MODEL_DIM, q_width), MODEL_DIM),
        "w_key": scaled_normal(shared[2], (N_LAYERS, MODEL_DIM, kv_width), MODEL_DIM, 8.0),
        "w_value": scaled_normal(shared[3], (N_LAYERS, MODEL_DIM, kv_width), MODEL_DIM, 2.0),
        "w_out": scaled_normal(shared[4], (N_LAYERS, q_width, MODEL_DIM), q_width),
        "w_gate": scaled_normal(shared[5], (N_LAYERS, MODEL_DIM, FFN_DIM), MODEL_DIM),
        "w_up": scaled_normal(shared[6], (N_LAYERS, MODEL_DIM, FFN_DIM), MODEL_DIM),
        "w_down": scaled_normal(shared[7], (N_LAYERS, FFN_DIM, MODEL_DIM), FFN_DIM),
    }


def layer_norm(rows_in, gain):
    rows32 = rows_in.astype(jnp.float32)
    centered = rows32 - rows32.mean(axis=-1, keepdims=True)
    variance = (centered * centered).mean(axis=-1, keepdims=True)
    scaled = centered * lax.rsqrt(variance + NORM_EPS)
    return (scaled * gain.astype(jnp.float32)).astype(jnp.bfloat16)


def rotary(proj, positions, n_groups):
    half_dim = HEAD_DIM // 2
    inv_freq = 1.0 / (ROPE_BASE ** (jnp.arange(half_dim, dtype=jnp.float32) * 2.0 / HEAD_DIM))
    angles = positions.astype(jnp.float32)[:, None] * inv_freq[None, :]
    cosine = jnp.cos(angles)[:, None, :]
    sine = jnp.sin(angles)[:, None, :]
    heads = proj.reshape(proj.shape[0], n_groups, HEAD_DIM)
    first = heads[..., :half_dim]
    second = heads[..., half_dim:]
    turned = jnp.concatenate([first * cosine - second * sine, second * cosine + first * sine], axis=-1)
    return turned.reshape(proj.shape)


def attend(query, keys, values, key_valid):
    group_size = N_HEADS // KV_HEADS

    def one_row(row):
        q_row, k_row, v_row, ok_row = row
        grouped = q_row.reshape(KV_HEADS, group_size, HEAD_DIM).astype(jnp.float32)
        scores = jnp.einsum("kgd,ksd->kgs", grouped, k_row.astype(jnp.float32)) * HEAD_DIM ** -0.5
        scores = jnp.where(ok_row[None, None, :], scores, -1e30)
        weights = jax.nn.softmax(scores, axis=-1).astype(jnp.bfloat16)
        mixed = jnp.einsum("kgs,ksd->kgd", weights.astype(jnp.float32), v_row.astype(jnp.float32))
        return mixed.astype(jnp.bfloat16).reshape(N_HEADS * HEAD_DIM)

    return lax.map(one_row, (query, keys, values, key_valid))


def reference(k_cache, v_cache, lengths, hidden, ln_gain, w_query, w_key, w_value, w_out, w_gate, w_up, w_down):
    slot_ids = jnp.arange(WINDOW, dtype=jnp.int32)
    slot_pos = lengths[:, None] - (lengths[:, None] - slot_ids[None, :]) % WINDOW
    seq_ids = jnp.arange(SEQ_LEN, dtype=jnp.int32)
    window_valid = jnp.ones((N_ROWS, WINDOW), dtype=jnp.bool_)
    global_valid = seq_ids[None, :] <= lengths[:, None]
    before_new = (seq_ids[None, :] < lengths[:, None])[:, None, :, None]
    at_new = (seq_ids[None, :] == lengths[:, None])[:, None, :, None]
    slot_new = (slot_pos == lengths[:, None])[:, None, :, None]
    slot_index = slot_pos[:, None, :, None]
    residual = hidden
    windows_k = []
    windows_v = []
    for layer in range(N_LAYERS):
        sliding = layer < N_LAYERS - 1
        normed = layer_norm(residual, ln_gain[layer])
        query = jnp.dot(normed, w_query[layer], preferred_element_type=jnp.float32)
        key_new = jnp.dot(normed, w_key[layer], preferred_element_type=jnp.float32)
        value_new = jnp.dot(normed, w_value[layer], preferred_element_type=jnp.float32)
        if sliding:
            query = rotary(query, lengths, N_HEADS)
            key_new = rotary(key_new, lengths, KV_HEADS)
        query = query.astype(jnp.bfloat16).reshape(N_ROWS, N_HEADS, HEAD_DIM)
        key_new = key_new.astype(jnp.bfloat16).reshape(N_ROWS, KV_HEADS, 1, HEAD_DIM)
        value_new = value_new.astype(jnp.bfloat16).reshape(N_ROWS, KV_HEADS, 1, HEAD_DIM)
        if sliding:
            keys = jnp.where(slot_new, key_new, jnp.take_along_axis(k_cache[layer], slot_index, axis=2))
            values = jnp.where(slot_new, value_new, jnp.take_along_axis(v_cache[layer], slot_index, axis=2))
            windows_k.append(keys)
            windows_v.append(values)
            key_valid = window_valid
        else:
            keys = jnp.where(at_new, key_new, jnp.where(before_new, k_cache[layer], 0))
            values = jnp.where(at_new, value_new, jnp.where(before_new, v_cache[layer], 0))
            key_valid = global_valid
        mixed = attend(query, keys, values, key_valid)
        attn_out = jnp.dot(mixed, w_out[layer], preferred_element_type=jnp.float32)
        gate_proj = jnp.dot(normed, w_gate[layer], preferred_element_type=jnp.float32)
        up_proj = jnp.dot(normed, w_up[layer], preferred_element_type=jnp.float32)
        activated = (jax.nn.silu(gate_proj) * up_proj).astype(jnp.bfloat16)
        mlp_out = jnp.dot(activated, w_down[layer], preferred_element_type=jnp.float32)
        residual = (residual.astype(jnp.float32) + attn_out + mlp_out).astype(jnp.bfloat16)
    return residual, jnp.stack(windows_k), jnp.stack(windows_v), keys, values
```

```python
import functools

import jax
import jax.numpy as jnp
from jax import lax
from jax.experimental import pallas as pl
from jax.experimental.pallas import tpu as pltpu
from jax.sharding import PartitionSpec as P

WINDOW = 4096
ROPE_BASE = 50000
NORM_EPS = 1e-5
UNIT = 128


def layer_norm(rows_in, gain):
    rows32 = rows_in.astype(jnp.float32)
    centered = rows32 - rows32.mean(axis=-1, keepdims=True)
    variance = (centered * centered).mean(axis=-1, keepdims=True)
    scaled = centered * lax.rsqrt(variance + NORM_EPS)
    return (scaled * gain.astype(jnp.float32)).astype(jnp.bfloat16)


def rotary(proj, positions, head_dim):
    half_dim = head_dim // 2
    inv_freq = 1.0 / (ROPE_BASE ** (jnp.arange(half_dim, dtype=jnp.float32) * 2.0 / head_dim))
    angles = positions.astype(jnp.float32)[:, None] * inv_freq[None, :]
    cosine = jnp.cos(angles)[:, None, :]
    sine = jnp.sin(angles)[:, None, :]
    heads = proj.reshape(proj.shape[0], -1, head_dim)
    first = heads[..., :half_dim]
    second = heads[..., half_dim:]
    turned = jnp.concatenate([first * cosine - second * sine, second * cosine + first * sine], axis=-1)
    return turned.reshape(proj.shape)


def attend_body(layer, sliding, n_units, shard_units, ids, q_ref, new_ref, k_own, v_own, near, far, cross, k_in, v_in, o_ref, k_out, v_out, kv, edge, sems, out_sems):
    me = ids[0]
    length = ids[1]
    own_layer = ids[2]
    beta = length - WINDOW if sliding else length
    last = beta // UNIT
    halves = n_units // shard_units

    def fetch(w, low, part, dst, sem):
        block = w
        if sliding:
            block = jnp.where(jnp.logical_and(w <= last, jnp.logical_not(low)), w + halves * shard_units, w)
        relation = jnp.bitwise_xor(block // shard_units, me)
        at = pl.ds(pl.multiple_of(lax.rem(w, shard_units) * UNIT, UNIT), UNIT)

        @pl.when(relation == 0)
        def _():
            pltpu.make_async_copy((k_own, v_own)[part].at[own_layer, me, :, :, at], dst, sem).start()

        for other, ref in ((1, near), (2, far), (3, cross)):
            @pl.when(relation == other)
            def _(ref=ref):
                pltpu.make_async_copy(ref.at[part, :, :, at], dst, sem).start()

    for part in range(2):
        def issue(w, carry, part=part):
            fetch(w, False, part, kv.at[part, :, :, pl.ds(pl.multiple_of(w * UNIT, UNIT), UNIT)], sems.at[part])
            return carry
        lax.fori_loop(0, n_units, issue, 0)
        if sliding:
            fetch(last, True, part, edge.at[part], sems.at[part])

    lane = lax.broadcasted_iota(jnp.int32, (1, 1, UNIT), 2)

    def settle(part):
        pltpu.make_async_copy(kv.at[part], kv.at[part], sems.at[part]).wait()
        if sliding:
            pltpu.make_async_copy(edge.at[part], edge.at[part], sems.at[part]).wait()
        fresh = new_ref[part][:, :, None]

        def fix(w, carry):
            at = pl.ds(pl.multiple_of(w * UNIT, UNIT), UNIT)
            pos = lane + w * UNIT
            old = kv[part, :, :, at]
            rest = edge[part] if sliding else jnp.zeros_like(old)
            kv[part, :, :, at] = jnp.where(pos < beta, old, jnp.where(pos == beta, fresh, rest))
            return carry

        if sliding:
            fix(last, 0)
        else:
            lax.fori_loop(last, n_units, fix, 0)

    q = q_ref[...]
    upper = lax.broadcasted_iota(jnp.int32, (q.shape[0], 1), 0) < q.shape[0] // 2
    settle(0)
    s0 = jnp.dot(q, kv[0, 0], preferred_element_type=jnp.float32)
    s1 = jnp.dot(q, kv[0, 1], preferred_element_type=jnp.float32)
    k_copy = pltpu.make_async_copy(kv.at[0], k_out.at[layer], out_sems.at[0])
    k_copy.start()
    scores = jnp.where(upper, s0, s1) * (q.shape[1] ** -0.5)
    if not sliding:
        where = lax.broadcasted_iota(jnp.int32, (1, n_units * UNIT), 1)
        scores = jnp.where(where <= beta, scores, -1e30)
    top = scores.max(axis=-1, keepdims=True)
    expd = jnp.exp(scores - top)
    weights = (expd / expd.sum(axis=-1, keepdims=True)).astype(jnp.bfloat16)
    settle(1)
    dims = (((1,), (1,)), ((), ()))
    m0 = lax.dot_general(weights, kv[1, 0], dims, preferred_element_type=jnp.float32)
    m1 = lax.dot_general(weights, kv[1, 1], dims, preferred_element_type=jnp.float32)
    v_copy = pltpu.make_async_copy(kv.at[1], v_out.at[layer], out_sems.at[1])
    v_copy.start()
    o_ref[...] = jnp.where(upper, m0, m1).astype(jnp.bfloat16)
    k_copy.wait()
    v_copy.wait()


def attend(layer, own_layer, sliding, me, length, query, new_kv, k_t, v_t, parts, k_buf, v_buf):
    heads, dim, shard = k_t.shape[2:]
    n_units = k_buf.shape[-1] // UNIT
    ids = jnp.stack([me, length, jnp.int32(own_layer)])
    hbm = pl.BlockSpec(memory_space=pltpu.HBM)
    vmem = pl.BlockSpec(memory_space=pltpu.VMEM)
    return pl.pallas_call(
        functools.partial(attend_body, layer, sliding, n_units, shard // UNIT),
        in_specs=[pl.BlockSpec(memory_space=pltpu.SMEM), vmem, vmem] + [hbm] * 7,
        out_specs=[vmem, hbm, hbm],
        out_shape=[jax.ShapeDtypeStruct(query.shape, jnp.bfloat16), jax.ShapeDtypeStruct(k_buf.shape, k_buf.dtype), jax.ShapeDtypeStruct(v_buf.shape, v_buf.dtype)],
        scratch_shapes=[
            pltpu.VMEM((2, heads, dim, n_units * UNIT), jnp.bfloat16),
            pltpu.VMEM((2, heads, dim, UNIT), jnp.bfloat16),
            pltpu.SemaphoreType.DMA((2,)),
            pltpu.SemaphoreType.DMA((2,)),
        ],
        input_output_aliases={8: 1, 9: 2},
        cost_estimate=pl.CostEstimate(flops=100000000, bytes_accessed=8 * heads * dim * n_units * UNIT * 2, transcendentals=0),
        name="attend",
    )(ids, query, new_kv, k_t, v_t, *parts, k_buf, v_buf)


def fresh_body(*refs):
    pass


def fresh_buffers(shapes):
    hbm = pl.BlockSpec(memory_space=pltpu.HBM)
    return pl.pallas_call(fresh_body, out_specs=[hbm] * len(shapes), out_shape=[jax.ShapeDtypeStruct(s, jnp.bfloat16) for s in shapes], name="fresh")()


def solution(mesh):
    cache_spec = P(None, "dp", "tp", "sp", None)
    row_spec = P(("dp", "sp"), None)
    col_spec = P(None, None, "tp")
    inner_spec = P(None, "tp", None)
    window_spec = P(None, ("dp", "sp"), "tp", None, None)
    global_spec = P(("dp", "sp"), "tp", None, None)
    in_specs = (cache_spec, cache_spec, P("dp"), row_spec, P(None, None), col_spec, col_spec, col_spec, inner_spec, col_spec, col_spec, inner_spec)
    out_specs = (row_spec, window_spec, window_spec, global_spec, global_spec)
    n_sp = mesh.shape["sp"]

    def device_step(k_cache, v_cache, lengths, hidden, ln_gain, w_query, w_key, w_value, w_out, w_gate, w_up, w_down):
        n_layers = w_query.shape[0]
        heads, shard, dim = k_cache.shape[2:]
        seq = shard * n_sp
        me = lax.axis_index("sp").astype(jnp.int32)
        my_length = lax.dynamic_slice_in_dim(lengths, me, 1)
        k_t = jnp.swapaxes(k_cache, 3, 4)
        v_t = jnp.swapaxes(v_cache, 3, 4)
        k_win, v_win, k_glob, v_glob = fresh_buffers([(n_layers - 1, heads, dim, WINDOW)] * 2 + [(1, heads, dim, seq)] * 2)

        def exchange(layer, relation):
            peer = jnp.bitwise_xor(me, relation)
            block = lambda t: lax.dynamic_slice(t, (layer, peer, 0, 0, 0), (1, 1, heads, dim, shard))[0, 0]
            return lax.ppermute(jnp.stack([block(k_t), block(v_t)]), "sp", [(i, i ^ relation) for i in range(n_sp)])

        moved = [[exchange(layer, relation) for relation in (1, 2, 3)] for layer in range(n_layers)]
        residual = hidden
        for layer in range(n_layers):
            sliding = layer < n_layers - 1
            normed = layer_norm(residual, ln_gain[layer])
            query = jnp.dot(normed, w_query[layer], preferred_element_type=jnp.float32)
            key_new = jnp.dot(normed, w_key[layer], preferred_element_type=jnp.float32)
            value_new = jnp.dot(normed, w_value[layer], preferred_element_type=jnp.float32)
            if sliding:
                query = rotary(query, my_length, dim)
                key_new = rotary(key_new, my_length, dim)
            query = query.astype(jnp.bfloat16).reshape(-1, dim)
            new_kv = jnp.stack([key_new.astype(jnp.bfloat16).reshape(heads, dim), value_new.astype(jnp.bfloat16).reshape(heads, dim)])
            gate_proj = jnp.dot(normed, w_gate[layer], preferred_element_type=jnp.float32)
            up_proj = jnp.dot(normed, w_up[layer], preferred_element_type=jnp.float32)
            activated = (jax.nn.silu(gate_proj) * up_proj).astype(jnp.bfloat16)
            mlp_out = jnp.dot(activated, w_down[layer], preferred_element_type=jnp.float32)
            if sliding:
                mixed, k_win, v_win = attend(layer, layer, True, me, my_length[0], query, new_kv, k_t, v_t, moved[layer], k_win, v_win)
            else:
                mixed, k_glob, v_glob = attend(0, layer, False, me, my_length[0], query, new_kv, k_t, v_t, moved[layer], k_glob, v_glob)
            attn_out = jnp.dot(mixed.reshape(1, -1), w_out[layer], preferred_element_type=jnp.float32)
            both = lax.psum(attn_out + mlp_out, "tp")
            residual = (residual.astype(jnp.float32) + both).astype(jnp.bfloat16)
        back = lambda t: jnp.swapaxes(t, -1, -2)
        return residual, back(k_win)[:, None], back(v_win)[:, None], back(k_glob), back(v_glob)

    return jax.shard_map(device_step, mesh=mesh, in_specs=in_specs, out_specs=out_specs, check_vma=False)
```

```python
import functools

import jax
import jax.numpy as jnp
from jax import lax
from jax.experimental import pallas as pl
from jax.experimental.pallas import tpu as pltpu
from jax.sharding import PartitionSpec as P

WINDOW = 4096
ROPE_BASE = 50000
NORM_EPS = 1e-5
UNIT = 128
SIZES = (16, 20, 24, 28, 32)
FFN_STEPS = 4
HBM = pl.BlockSpec(memory_space=pltpu.HBM)
VMEM = pl.BlockSpec(memory_space=pltpu.VMEM)
SMEM = pl.BlockSpec(memory_space=pltpu.SMEM)
F32 = jnp.float32
BF16 = jnp.bfloat16


def cost(n_bytes):
    return pl.CostEstimate(flops=n_bytes, bytes_accessed=n_bytes, transcendentals=0)


def lanes(block, count=1):
    return pl.ds(pl.multiple_of(block * UNIT, UNIT), count * UNIT)


def crossing(beta, on_second_chip, n_units):
    above = (beta + 1) // UNIT
    below = (beta + UNIT - 1) // UNIT
    return jnp.where(on_second_chip, above, 0), jnp.where(on_second_chip, n_units - above, below)


def move(pairs):
    for src, dst, sem in pairs:
        pltpu.make_async_copy(src, dst, sem).start()


def pack_body(layer, size, half, ids, k_own, v_own, near, *refs):
    outs, (buf, sem, out_sem) = refs[:-3], refs[-3:]
    me = ids[0]
    core = lax.rem(me, 2)
    base = (1 - me // 2) * 2
    second = base == 2
    row, other = base + core, base + 1 - core
    first, count = crossing(ids[1 + row] - WINDOW, second, 2 * half)
    other_first, other_count = crossing(ids[1 + other] - WINDOW, second, 2 * half)
    over = jnp.maximum(other_count - size, 0)

    def issue(i, carry):
        mine = i < count
        dest = jnp.where(mine, row, other)
        unit = jnp.where(mine, first + i, other_first + size + i - (size - over))
        unit = jnp.clip(unit, 0, 2 * half - 1)
        at = lanes(lax.rem(unit, half))
        local = unit // half == core

        @pl.when(local)
        def _():
            move([(k_own.at[layer, dest, :, :, at], buf.at[0, :, :, lanes(i)], sem), (v_own.at[layer, dest, :, :, at], buf.at[1, :, :, lanes(i)], sem)])

        @pl.when(jnp.logical_not(local))
        def _():
            move([(near.at[p, dest, :, :, at], buf.at[p, :, :, lanes(i)], sem) for p in range(2)])

        return carry

    lax.fori_loop(0, size, issue, 0)
    pltpu.make_async_copy(buf, buf, sem).wait()
    cut = size - half
    copies = [pltpu.make_async_copy(buf.at[:, :, :, cut * UNIT:], outs[0], out_sem)]
    if cut:
        copies.append(pltpu.make_async_copy(buf.at[:, :, :, :cut * UNIT], outs[1], out_sem))
    for copy in copies:
        copy.start()
    for copy in copies:
        copy.wait()


def pack(layer, size, ids, k_t, v_t, near):
    heads, dim, shard = k_t.shape[2:]
    half = shard // UNIT
    widths = [half] + ([size - half] if size > half else [])
    return pl.pallas_call(
        functools.partial(pack_body, layer, size, half),
        in_specs=[SMEM, HBM, HBM, HBM],
        out_specs=[HBM] * len(widths),
        out_shape=[jax.ShapeDtypeStruct((2, heads, dim, w * UNIT), BF16) for w in widths],
        scratch_shapes=[pltpu.VMEM((2, heads, dim, size * UNIT), BF16), pltpu.SemaphoreType.DMA, pltpu.SemaphoreType.DMA],
        cost_estimate=cost(8 * heads * dim * size * UNIT),
        name="pack",
    )(ids, k_t, v_t, near)


def settle(kv, new_rows, beta, rest_of, units):
    fresh = new_rows[:, :, None]
    lane = lax.broadcasted_iota(jnp.int32, (1, 1, UNIT), 2)

    def fix(w, carry):
        pos = lane + w * UNIT
        old = kv[:, :, lanes(w)].astype(F32)
        put = jnp.where(pos < beta, old, jnp.where(pos == beta, fresh, rest_of(old)))
        kv[:, :, lanes(w)] = put.astype(BF16)
        return carry

    lax.fori_loop(*units, fix, 0)


def stacked(q_ref):
    return jnp.concatenate([q_ref[j] for j in range(q_ref.shape[0])], axis=0).astype(BF16)


def softmax_weights(q, keys, beta):
    upper = lax.broadcasted_iota(jnp.int32, (q.shape[0], 1), 0) < q.shape[0] // 2
    s0 = jnp.dot(q, keys[0], preferred_element_type=F32)
    s1 = jnp.dot(q, keys[1], preferred_element_type=F32)
    scores = jnp.where(upper, s0, s1) * (q.shape[1] ** -0.5)
    if beta is not None:
        scores = jnp.where(lax.broadcasted_iota(jnp.int32, (1, scores.shape[1]), 1) <= beta, scores, -1e30)
    top = scores.max(axis=-1, keepdims=True)
    expd = jnp.exp(scores - top)
    return (expd / expd.sum(axis=-1, keepdims=True)).astype(BF16)


def mix_and_project(weights, values, wo, mlp):
    rows = weights.shape[0]
    upper = lax.broadcasted_iota(jnp.int32, (rows, 1), 0) < rows // 2
    dims = (((1,), (1,)), ((), ()))
    m0 = lax.dot_general(weights, values[0], dims, preferred_element_type=F32)
    m1 = lax.dot_general(weights, values[1], dims, preferred_element_type=F32)
    mixed = jnp.where(upper, m0, m1).astype(BF16).astype(F32)
    flat = jnp.concatenate([mixed[j:j + 1] for j in range(rows)], axis=1)
    flat = jnp.broadcast_to(flat, (8, flat.shape[1])).astype(BF16)
    return jnp.dot(flat, wo[...], preferred_element_type=F32)[0:1] + mlp


def window_body(layer, size, half, n_pipe, ids, q_ref, new_ref, mlp_ref, wo_hbm, k_own, v_own, near, *refs):
    pipe = refs[:n_pipe]
    k_out, v_out = refs[n_pipe + 3:n_pipe + 5]
    part_ref = refs[n_pipe + 2]
    kv, edge, wo, sems, out_sems, wo_sem = refs[n_pipe + 5:]
    me = ids[0]
    core = lax.rem(me, 2)
    second = me // 2 == 1
    beta = ids[1 + me] - WINDOW
    last = beta // UNIT
    first, count = crossing(beta, second, 2 * half)
    over = jnp.maximum(count - size, 0)
    cut = size - half

    def fetch(w, low, part, dst, sem):
        high = jnp.logical_and(w <= last, jnp.logical_not(low))
        crosses = jnp.logical_xor(high, second)
        at = lanes(lax.rem(w, half))
        local = w // half == core
        idx = jnp.clip(w - first, 0, 2 * half - 1)
        stay = jnp.logical_not(crosses)

        @pl.when(jnp.logical_and(stay, local))
        def _():
            move([((k_own, v_own)[part].at[layer, me, :, :, at], dst, sem)])

        @pl.when(jnp.logical_and(stay, jnp.logical_not(local)))
        def _():
            move([(near.at[part, me, :, :, at], dst, sem)])

        @pl.when(jnp.logical_and(crosses, jnp.logical_and(idx >= cut, idx < size)))
        def _():
            move([(pipe[0].at[part, :, :, lanes(idx - cut)], dst, sem)])

        if cut:
            @pl.when(jnp.logical_and(crosses, idx < cut))
            def _():
                move([(pipe[1].at[part, :, :, lanes(idx)], dst, sem)])

        if size < 2 * half:
            @pl.when(jnp.logical_and(crosses, idx >= size))
            def _():
                move([(pipe[-1].at[part, :, :, lanes(jnp.clip(half - over + idx - size, 0, half - 1))], dst, sem)])

    wo_copy = pltpu.make_async_copy(wo_hbm.at[layer], wo, wo_sem)
    for part in range(2):
        def issue(w, carry, part=part):
            fetch(w, False, part, kv.at[part, :, :, lanes(w)], sems.at[part])
            return carry
        lax.fori_loop(0, 2 * half, issue, 0)
        fetch(last, True, part, edge.at[part], sems.at[part])
    wo_copy.start()

    def ready(part):
        pltpu.make_async_copy(kv.at[part], kv.at[part], sems.at[part]).wait()
        pltpu.make_async_copy(edge.at[part], edge.at[part], sems.at[part]).wait()
        settle(kv.at[part], new_ref[part], beta, lambda old: edge[part].astype(F32), (last, last + 1))

    ready(0)
    weights = softmax_weights(stacked(q_ref), kv.at[0], None)
    k_copy = pltpu.make_async_copy(kv.at[0], k_out.at[layer], out_sems.at[0])
    k_copy.start()
    ready(1)
    wo_copy.wait()
    part_ref[...] = mix_and_project(weights, kv.at[1], wo, mlp_ref[...])
    v_copy = pltpu.make_async_copy(kv.at[1], v_out.at[layer], out_sems.at[1])
    v_copy.start()
    k_copy.wait()
    v_copy.wait()


def attend_window(layer, size, ids, q, new_kv, mlp, w_out, k_t, v_t, near, pipe, k_buf, v_buf):
    heads, dim, shard = k_t.shape[2:]
    half = shard // UNIT
    n_pipe = len(pipe)
    return pl.pallas_call(
        functools.partial(window_body, layer, size, half, n_pipe),
        in_specs=[SMEM, VMEM, VMEM, VMEM] + [HBM] * (4 + n_pipe + 2),
        out_specs=[VMEM, HBM, HBM],
        out_shape=[jax.ShapeDtypeStruct(mlp.shape, F32), jax.ShapeDtypeStruct(k_buf.shape, BF16), jax.ShapeDtypeStruct(v_buf.shape, BF16)],
        scratch_shapes=[
            pltpu.VMEM((2, heads, dim, 2 * shard), BF16),
            pltpu.VMEM((2, heads, dim, UNIT), BF16),
            pltpu.VMEM(w_out.shape[1:], BF16),
            pltpu.SemaphoreType.DMA((2,)),
            pltpu.SemaphoreType.DMA((2,)),
            pltpu.SemaphoreType.DMA,
        ],
        input_output_aliases={8 + n_pipe: 1, 9 + n_pipe: 2},
        cost_estimate=cost(16 * heads * dim * shard),
        name="attend_window",
    )(ids, q, new_kv, mlp, w_out, k_t, v_t, near, *pipe, k_buf, v_buf)


def fetch_row(layer, me, own, blocks, kv, sem):
    shard = blocks[0].shape[-1]
    for s in range(4):
        for relation in range(4):
            @pl.when(jnp.bitwise_xor(me, s) == relation)
            def _(s=s, relation=relation):
                src = own.at[layer, me] if relation == 0 else blocks[relation - 1]
                move([(src, kv.at[:, :, s * shard:(s + 1) * shard], sem)])


def scores_body(layer, ids, q_ref, new_ref, own, b1, b2, b3, w_ref, k_out, kv, sem, out_sem):
    me = ids[0]
    length = ids[1 + me]
    fetch_row(layer, me, own, (b1, b2, b3), kv, sem)
    pltpu.make_async_copy(kv, kv, sem).wait()
    settle(kv, new_ref[0], length, jnp.zeros_like, (length // UNIT, kv.shape[-1] // UNIT))
    w_ref[...] = softmax_weights(stacked(q_ref), kv, length)
    copy = pltpu.make_async_copy(kv, k_out, out_sem)
    copy.start()
    copy.wait()


def values_body(layer, ids, w_ref, new_ref, mlp_ref, wo_hbm, own, b1, b2, b3, part_ref, v_out, kv, wo, sem, out_sem, wo_sem):
    me = ids[0]
    length = ids[1 + me]
    fetch_row(layer, me, own, (b1, b2, b3), kv, sem)
    wo_copy = pltpu.make_async_copy(wo_hbm.at[layer], wo, wo_sem)
    wo_copy.start()
    pltpu.make_async_copy(kv, kv, sem).wait()
    settle(kv, new_ref[1], length, jnp.zeros_like, (length // UNIT, kv.shape[-1] // UNIT))
    wo_copy.wait()
    part_ref[...] = mix_and_project(w_ref[...], kv, wo, mlp_ref[...])
    copy = pltpu.make_async_copy(kv, v_out, out_sem)
    copy.start()
    copy.wait()


def attend_global(layer, ids, q, new_kv, mlp, w_out, k_t, v_t, k_blocks, v_blocks):
    heads, dim, shard = k_t.shape[2:]
    row = jax.ShapeDtypeStruct((heads, dim, 4 * shard), BF16)
    scratch = [pltpu.VMEM(row.shape, BF16), pltpu.SemaphoreType.DMA, pltpu.SemaphoreType.DMA]
    n_q = q.shape[0] * q.shape[1]
    weights, k_glob = pl.pallas_call(
        functools.partial(scores_body, layer),
        in_specs=[SMEM, VMEM, VMEM] + [HBM] * 4,
        out_specs=[VMEM, HBM],
        out_shape=[jax.ShapeDtypeStruct((n_q, 4 * shard), BF16), row],
        scratch_shapes=scratch,
        cost_estimate=cost(16 * heads * dim * shard),
        name="scores",
    )(ids, q, new_kv, k_t, *k_blocks)
    part, v_glob = pl.pallas_call(
        functools.partial(values_body, layer),
        in_specs=[SMEM, VMEM, VMEM, VMEM] + [HBM] * 5,
        out_specs=[VMEM, HBM],
        out_shape=[jax.ShapeDtypeStruct(mlp.shape, F32), row],
        scratch_shapes=scratch[:1] + [pltpu.VMEM(w_out.shape[1:], BF16)] + [pltpu.SemaphoreType.DMA] * 3,
        cost_estimate=cost(16 * heads * dim * shard),
        name="values",
    )(ids, weights, new_kv, mlp, w_out, v_t, *v_blocks)
    return part, k_glob, v_glob


def summed(tp, residual, parts):
    total = residual.astype(F32)
    for t in range(4):
        at = jnp.bitwise_xor(tp, t)
        pick = parts[3][...]
        for r in range(3):
            pick = jnp.where(at == r, parts[r][...], pick)
        total = pick if t == 0 else total + pick
    return (residual.astype(F32) + total).astype(BF16)


def front_body(layer, dim, n_parts, tp_ref, h_ref, *refs):
    parts, (gain, cosine, sine, wq, wk, wv, wg, wu, wd, h_out, q_out, new_out, mlp_out, u, acc) = refs[:n_parts], refs[n_parts:]
    step = pl.program_id(0)

    def turn(proj):
        if cosine is None:
            return proj
        width = proj.shape[1]
        lane = lax.broadcasted_iota(jnp.int32, proj.shape, 1)
        ahead = pltpu.roll(proj, width - dim // 2, 1)
        behind = pltpu.roll(proj, dim // 2, 1)
        swapped = jnp.where(lax.rem(lane, dim) < dim // 2, -ahead, behind)
        return proj * cosine[...] + swapped * sine[...]

    def rounded(proj):
        return proj.astype(BF16).astype(F32)

    @pl.when(step == 0)
    def _():
        h = summed(tp_ref[0], h_ref[...], parts) if n_parts else h_ref[...]
        h_out[...] = h
        rows32 = h.astype(F32)
        centered = rows32 - rows32.mean(axis=-1, keepdims=True)
        variance = (centered * centered).mean(axis=-1, keepdims=True)
        scaled = centered * lax.rsqrt(variance + NORM_EPS) * gain[...].astype(F32)[layer:layer + 1]
        u[...] = jnp.broadcast_to(scaled, u.shape).astype(BF16)
        acc[...] = jnp.zeros_like(acc)
        key_new = rounded(turn(jnp.dot(u[...], wk[0], preferred_element_type=F32)))
        value_new = rounded(jnp.dot(u[...], wv[0], preferred_element_type=F32))
        for part, new in ((0, key_new), (1, value_new)):
            for head in range(new_out.shape[1]):
                new_out[part, head:head + 1, :] = new[0:1, head * dim:(head + 1) * dim]

    query = rounded(turn(jnp.dot(u[...], wq[0], preferred_element_type=F32)))
    for head in range(q_out.shape[1]):
        q_out[0, head:head + 1, :] = query[0:1, head * dim:(head + 1) * dim]
    gate = jnp.dot(u[...], wg[0], preferred_element_type=F32)
    up = jnp.dot(u[...], wu[0], preferred_element_type=F32)
    active = (jax.nn.silu(gate) * up).astype(BF16)
    acc[...] += jnp.dot(active, wd[0], preferred_element_type=F32)

    @pl.when(step == FFN_STEPS - 1)
    def _():
        mlp_out[...] = acc[0:1, :]


def plain_front_body(layer, dim, n_parts, tp_ref, h_ref, *refs):
    front_body(layer, dim, n_parts, tp_ref, h_ref, *refs[:n_parts + 1], None, None, *refs[n_parts + 1:])


def front(layer, dim, tp, residual, parts, ln_gain, turns, w_query, w_key, w_value, w_gate, w_up, w_down):
    width = residual.shape[1]
    q_width, kv_width, ffn = w_query.shape[2], w_key.shape[2], w_gate.shape[2]
    q_step, ffn_step = q_width // FFN_STEPS, ffn // FFN_STEPS
    whole = lambda *shape: pl.BlockSpec(shape, lambda j: (0,) * len(shape))
    col = lambda rows, cols: pl.BlockSpec((1, rows, cols), lambda j: (layer, 0, j))
    fixed = lambda rows, cols: pl.BlockSpec((1, rows, cols), lambda j: (layer, 0, 0))
    n_parts = len(parts)
    body = front_body if turns else plain_front_body
    return pl.pallas_call(
        functools.partial(body, layer, dim, n_parts),
        grid=(FFN_STEPS,),
        in_specs=[SMEM, whole(1, width)] + [whole(1, width)] * n_parts + [whole(*ln_gain.shape)] + [whole(1, kv_width)] * len(turns)
        + [col(width, q_step), fixed(width, kv_width), fixed(width, kv_width), col(width, ffn_step), col(width, ffn_step), pl.BlockSpec((1, ffn_step, width), lambda j: (layer, j, 0))],
        out_specs=[whole(1, width), pl.BlockSpec((1, q_step // dim, dim), lambda j: (j, 0, 0)), whole(2, kv_width // dim, dim), whole(1, width)],
        out_shape=[
            jax.ShapeDtypeStruct((1, width), BF16),
            jax.ShapeDtypeStruct((FFN_STEPS, q_step // dim, dim), F32),
            jax.ShapeDtypeStruct((2, kv_width // dim, dim), F32),
            jax.ShapeDtypeStruct((1, width), F32),
        ],
        scratch_shapes=[pltpu.VMEM((8, width), BF16), pltpu.VMEM((8, width), F32)],
        compiler_params=pltpu.CompilerParams(dimension_semantics=("arbitrary",)),
        cost_estimate=cost(2 * width * (q_width + 2 * kv_width + 3 * ffn)),
        name="front",
    )(tp, residual, *parts, ln_gain, *turns, w_query, w_key, w_value, w_gate, w_up, w_down)


def close_body(tp_ref, h_ref, p0, p1, p2, p3, out_ref):
    out_ref[...] = summed(tp_ref[0], h_ref[...], (p0, p1, p2, p3))


def close(tp, residual, parts):
    return pl.pallas_call(
        close_body,
        in_specs=[SMEM] + [VMEM] * 5,
        out_specs=VMEM,
        out_shape=jax.ShapeDtypeStruct(residual.shape, BF16),
        name="close",
    )(tp, residual, *parts)


def fresh_body(*refs):
    pass


def fresh_buffers(shapes):
    return pl.pallas_call(fresh_body, out_specs=[HBM] * len(shapes), out_shape=[jax.ShapeDtypeStruct(s, BF16) for s in shapes], name="fresh")()


def solution(mesh):
    cache_spec = P(None, "dp", "tp", "sp", None)
    row_spec = P(("dp", "sp"), None)
    col_spec = P(None, None, "tp")
    inner_spec = P(None, "tp", None)
    window_spec = P(None, ("dp", "sp"), "tp", None, None)
    global_spec = P(("dp", "sp"), "tp", None, None)
    in_specs = (cache_spec, cache_spec, P("dp"), row_spec, P(None, None), col_spec, col_spec, col_spec, inner_spec, col_spec, col_spec, inner_spec)
    out_specs = (row_spec, window_spec, window_spec, global_spec, global_spec)
    n_sp, n_tp = mesh.shape["sp"], mesh.shape["tp"]

    def swap(t, axis, relation):
        return lax.ppermute(t, axis, [(i, i ^ relation) for i in range(n_sp if axis == "sp" else n_tp)])

    def device_step(k_cache, v_cache, lengths, hidden, ln_gain, w_query, w_key, w_value, w_out, w_gate, w_up, w_down):
        n_layers = w_query.shape[0]
        heads, shard, dim = k_cache.shape[2:]
        half = shard // UNIT
        final = n_layers - 1
        me = lax.axis_index("sp").astype(jnp.int32)
        tp = lax.axis_index("tp").astype(jnp.int32)[None]
        ids = jnp.concatenate([me[None], lengths])
        k_t = jnp.swapaxes(k_cache, 3, 4)
        v_t = jnp.swapaxes(v_cache, 3, 4)

        inv_freq = 1.0 / (ROPE_BASE ** (jnp.arange(dim // 2, dtype=F32) * 2.0 / dim))
        angles = lax.dynamic_slice_in_dim(lengths, me, 1).astype(F32)[:, None] * inv_freq[None, :]
        repeat = 2 * w_key.shape[2] // dim
        turns = (jnp.tile(jnp.cos(angles), (1, repeat)), jnp.tile(jnp.sin(angles), (1, repeat)))

        _, counts = crossing(lengths - WINDOW, jnp.arange(n_sp) >= n_sp // 2, 2 * half)
        need = lax.pmax(jnp.max((counts.reshape(2, -1).sum(axis=1) + 1) // 2), "dp")
        choice = sum((need > size).astype(jnp.int32) for size in SIZES[:-1])

        def block(t, relation):
            return lax.dynamic_slice(t, (final, jnp.bitwise_xor(me, relation), 0, 0, 0), (1, 1, heads, dim, shard))[0, 0]

        nears = [swap(jnp.stack([k_t[0], v_t[0]]), "sp", 1)]
        k_far = swap(block(k_t, 2), "sp", 2)

        def run(size):
            k_win, v_win = fresh_buffers([(final, heads, dim, WINDOW)] * 2)
            k_blocks = [swap(block(k_t, 1), "sp", 1), k_far, swap(block(k_t, 3), "sp", 3)]
            near = list(nears)
            near += [swap(jnp.stack([k_t[layer], v_t[layer]]), "sp", 1) for layer in range(1, final)]
            pipes = []
            for layer in range(final):
                packed = pack(layer, size, ids, k_t, v_t, near[layer])
                came = [swap(p, "sp", 2) for p in packed]
                if size < 2 * half:
                    came.append(swap(came[0], "sp", 1))
                pipes.append(came)
            v_cut = lax.optimization_barrier((packed[0], [block(v_t, r) for r in (1, 2, 3)]))[1]
            v_blocks = [swap(v_cut[r - 1], "sp", r) for r in (1, 2, 3)]
            residual, parts = hidden, ()
            for layer in range(n_layers):
                sliding = layer < final
                residual, q, new_kv, mlp = front(layer, dim, tp, residual, parts, ln_gain, turns if sliding else (), w_query, w_key, w_value, w_gate, w_up, w_down)
                if sliding:
                    part, k_win, v_win = attend_window(layer, size, ids, q, new_kv, mlp, w_out, k_t, v_t, near[layer], pipes[layer], k_win, v_win)
                else:
                    part, k_glob, v_glob = attend_global(layer, ids, q, new_kv, mlp, w_out, k_t, v_t, k_blocks, v_blocks)
                parts = (part,) + tuple(swap(part, "tp", r) for r in (1, 2, 3))
            return close(tp, residual, parts), k_win, v_win, k_glob, v_glob

        if len(SIZES) == 1:
            out, k_win, v_win, k_glob, v_glob = run(SIZES[0])
        else:
            out, k_win, v_win, k_glob, v_glob = lax.switch(choice, [functools.partial(run, size) for size in SIZES])
        back = lambda t: jnp.swapaxes(t, -1, -2)
        return out, back(k_win)[:, None], back(v_win)[:, None], back(k_glob)[None], back(v_glob)[None]

    return jax.shard_map(device_step, mesh=mesh, in_specs=in_specs, out_specs=out_specs, check_vma=False)
```

```python
import functools

import jax
import jax.numpy as jnp
from jax import lax
from jax.experimental import pallas as pl
from jax.experimental.pallas import tpu as pltpu
from jax.sharding import PartitionSpec as P


WINDOW = 4096
ROPE_BASE = 50000
NORM_EPS = 1e-5
UNIT = 128
SIZES = (16, 20, 24, 28, 32)
FFN_STEPS = 4
CHUNK = 8
HBM = pl.BlockSpec(memory_space=pltpu.HBM)
VMEM = pl.BlockSpec(memory_space=pltpu.VMEM)
SMEM = pl.BlockSpec(memory_space=pltpu.SMEM)
F32 = jnp.float32
BF16 = jnp.bfloat16


def cost(n_bytes):
    return pl.CostEstimate(flops=n_bytes, bytes_accessed=n_bytes, transcendentals=0)


def lanes(block, count=1):
    return pl.ds(pl.multiple_of(block * UNIT, UNIT), count * UNIT)


def crossing(beta, on_second_chip, n_units):
    above = (beta + 1) // UNIT
    below = (beta + UNIT - 1) // UNIT
    return jnp.where(on_second_chip, above, 0), jnp.where(on_second_chip, n_units - above, below)


def move(pairs):
    for src, dst, sem in pairs:
        pltpu.make_async_copy(src, dst, sem).start()


def pack_body(layer, size, half, ids, k_own, v_own, near, *refs):
    outs, (buf, sem, out_sem) = refs[:-3], refs[-3:]
    me = ids[0]
    core = lax.rem(me, 2)
    base = (1 - me // 2) * 2
    second = base == 2
    row, other = base + core, base + 1 - core
    first, count = crossing(ids[1 + row] - WINDOW, second, 2 * half)
    other_first, other_count = crossing(ids[1 + other] - WINDOW, second, 2 * half)
    over = jnp.maximum(other_count - size, 0)

    def issue(i, carry):
        mine = i < count
        dest = jnp.where(mine, row, other)
        unit = jnp.where(mine, first + i, other_first + size + i - (size - over))
        unit = jnp.clip(unit, 0, 2 * half - 1)
        at = lanes(lax.rem(unit, half))
        local = unit // half == core

        @pl.when(local)
        def _():
            move([(k_own.at[layer, dest, :, :, at], buf.at[0, :, :, lanes(i)], sem), (v_own.at[layer, dest, :, :, at], buf.at[1, :, :, lanes(i)], sem)])

        @pl.when(jnp.logical_not(local))
        def _():
            move([(near.at[p, dest, :, :, at], buf.at[p, :, :, lanes(i)], sem) for p in range(2)])

        return carry

    lax.fori_loop(0, size, issue, 0)
    pltpu.make_async_copy(buf, buf, sem).wait()
    cut = size - half
    copies = [pltpu.make_async_copy(buf.at[:, :, :, cut * UNIT:], outs[0], out_sem)]
    if cut:
        copies.append(pltpu.make_async_copy(buf.at[:, :, :, :cut * UNIT], outs[1], out_sem))
    for copy in copies:
        copy.start()
    for copy in copies:
        copy.wait()


def pack(layer, size, ids, k_t, v_t, near):
    heads, dim, shard = k_t.shape[2:]
    half = shard // UNIT
    widths = [half] + ([size - half] if size > half else [])
    return pl.pallas_call(
        functools.partial(pack_body, layer, size, half),
        in_specs=[SMEM, HBM, HBM, HBM],
        out_specs=[HBM] * len(widths),
        out_shape=[jax.ShapeDtypeStruct((2, heads, dim, w * UNIT), BF16) for w in widths],
        scratch_shapes=[pltpu.VMEM((2, heads, dim, size * UNIT), BF16), pltpu.SemaphoreType.DMA, pltpu.SemaphoreType.DMA],
        cost_estimate=cost(8 * heads * dim * size * UNIT),
        name="pack",
    )(ids, k_t, v_t, near)


def cut_body(layer, ids, k_own, v_own, out, buf, in_sems, out_sem):
    rows = k_own.shape[1]
    loads = [pltpu.make_async_copy((k_own, v_own)[i // rows].at[layer, i % rows], buf.at[i], in_sems.at[i]) for i in range(2 * rows)]
    stores = [pltpu.make_async_copy(buf.at[i], out.at[i // rows, i % rows], out_sem) for i in range(2 * rows)]
    for load in loads:
        load.start()
    for load, store in zip(loads, stores):
        load.wait()
        store.start()
    for store in stores:
        store.wait()


def cut(layer, ids, k_t, v_t):
    shape = k_t.shape[1:]
    return pl.pallas_call(
        functools.partial(cut_body, layer),
        in_specs=[SMEM, HBM, HBM],
        out_specs=HBM,
        out_shape=jax.ShapeDtypeStruct((2,) + shape, BF16),
        scratch_shapes=[pltpu.VMEM((2 * shape[0],) + shape[1:], BF16), pltpu.SemaphoreType.DMA((2 * shape[0],)), pltpu.SemaphoreType.DMA],
        cost_estimate=cost(8 * k_t.size // k_t.shape[0]),
        name="cut",
    )(ids, k_t, v_t)


def after(value, *others):
    return lax.optimization_barrier((value, others))[0]


def settle(kv, new_rows, beta, rest_of, units):
    fresh = new_rows[:, :, None]
    lane = lax.broadcasted_iota(jnp.int32, (1, 1, UNIT), 2)

    def fix(w, carry):
        pos = lane + w * UNIT
        old = kv[:, :, lanes(w)].astype(F32)
        put = jnp.where(pos < beta, old, jnp.where(pos == beta, fresh, rest_of(old)))
        kv[:, :, lanes(w)] = put.astype(BF16)
        return carry

    lax.fori_loop(*units, fix, 0)


def stacked(q_ref):
    return jnp.concatenate([q_ref[j] for j in range(q_ref.shape[0])], axis=0).astype(BF16)


def softmax_weights(q, keys, scores, beta):
    upper = lax.broadcasted_iota(jnp.int32, (q.shape[0], 1), 0) < q.shape[0] // 2

    def chunk(i, carry):
        at = lanes(i * CHUNK, CHUNK)
        s0 = jnp.dot(q, keys[0, :, at], preferred_element_type=F32)
        s1 = jnp.dot(q, keys[1, :, at], preferred_element_type=F32)
        part = jnp.where(upper, s0, s1) * (q.shape[1] ** -0.5)
        if beta is not None:
            part = jnp.where(lax.broadcasted_iota(jnp.int32, (1, part.shape[1]), 1) + i * CHUNK * UNIT <= beta, part, -1e30)
        scores[:, at] = part
        return carry

    lax.fori_loop(0, keys.shape[-1] // (CHUNK * UNIT), chunk, 0)
    top = scores[...].max(axis=-1, keepdims=True)
    expd = jnp.exp(scores[...] - top)
    return (expd / expd.sum(axis=-1, keepdims=True)).astype(BF16)


def mix_and_project(weights, values, wo, mlp, out):
    rows = weights.shape[0]
    dim = values.shape[1]
    upper = lax.broadcasted_iota(jnp.int32, (rows, 1), 0) < rows // 2
    dims = (((1,), (1,)), ((), ()))

    def chunk(i, carry):
        at = lanes(i * CHUNK, CHUNK)
        return tuple(carry[h] + lax.dot_general(weights[:, at], values[h, :, at], dims, preferred_element_type=F32) for h in range(2))

    m0, m1 = lax.fori_loop(0, values.shape[-1] // (CHUNK * UNIT), chunk, (jnp.zeros((rows, dim), F32),) * 2)
    mixed = jnp.where(upper, m0, m1).astype(BF16).astype(F32)
    flat = jnp.concatenate([mixed[j:j + 1] for j in range(rows)], axis=1)
    flat = jnp.broadcast_to(flat, (8, flat.shape[1])).astype(BF16)

    def project(i, carry):
        at = lanes(i * 4, 4)
        out[:, at] = jnp.dot(flat, wo[:, at], preferred_element_type=F32)[0:1] + mlp[:, at]
        return carry

    lax.fori_loop(0, out.shape[1] // (4 * UNIT), project, 0)


def window_body(layer, size, half, n_pipe, ids, q_ref, new_ref, mlp_ref, wo_hbm, k_own, v_own, near, *refs):
    pipe = refs[:n_pipe]
    k_out, v_out = refs[n_pipe + 3:n_pipe + 5]
    part_ref = refs[n_pipe + 2]
    kv, edge, wo, scores, weights, sems, out_sems, wo_sem = refs[n_pipe + 5:]
    me = ids[0]
    core = lax.rem(me, 2)
    second = me // 2 == 1
    beta = ids[1 + me] - WINDOW
    last = beta // UNIT
    first, count = crossing(beta, second, 2 * half)
    over = jnp.maximum(count - size, 0)
    cut = size - half

    def fetch(w, low, part, dst, sem):
        high = jnp.logical_and(w <= last, jnp.logical_not(low))
        crosses = jnp.logical_xor(high, second)
        at = lanes(lax.rem(w, half))
        local = w // half == core
        idx = jnp.clip(w - first, 0, 2 * half - 1)
        stay = jnp.logical_not(crosses)

        @pl.when(jnp.logical_and(stay, local))
        def _():
            move([((k_own, v_own)[part].at[layer, me, :, :, at], dst, sem)])

        @pl.when(jnp.logical_and(stay, jnp.logical_not(local)))
        def _():
            move([(near.at[part, me, :, :, at], dst, sem)])

        @pl.when(jnp.logical_and(crosses, jnp.logical_and(idx >= cut, idx < size)))
        def _():
            move([(pipe[0].at[part, :, :, lanes(idx - cut)], dst, sem)])

        if cut:
            @pl.when(jnp.logical_and(crosses, idx < cut))
            def _():
                move([(pipe[1].at[part, :, :, lanes(idx)], dst, sem)])

        if size < 2 * half:
            @pl.when(jnp.logical_and(crosses, idx >= size))
            def _():
                move([(pipe[-1].at[part, :, :, lanes(jnp.clip(half - over + idx - size, 0, half - 1))], dst, sem)])

    wo_copy = pltpu.make_async_copy(wo_hbm.at[layer], wo, wo_sem)
    for part in range(2):
        def issue(w, carry, part=part):
            fetch(w, False, part, kv.at[part, :, :, lanes(w)], sems.at[part])
            return carry

        lax.fori_loop(0, 2 * half, issue, 0)
        fetch(last, True, part, edge.at[part], sems.at[part])
    wo_copy.start()

    def ready(part):
        pltpu.make_async_copy(kv.at[part], kv.at[part], sems.at[part]).wait()
        pltpu.make_async_copy(edge.at[part], edge.at[part], sems.at[part]).wait()
        settle(kv.at[part], new_ref[part], beta, lambda old: edge[part].astype(F32), (last, last + 1))

    ready(0)
    weights[...] = softmax_weights(stacked(q_ref), kv.at[0], scores, None)
    k_copy = pltpu.make_async_copy(kv.at[0], k_out.at[layer], out_sems.at[0])
    k_copy.start()
    ready(1)
    wo_copy.wait()
    mix_and_project(weights, kv.at[1], wo, mlp_ref, part_ref)
    v_copy = pltpu.make_async_copy(kv.at[1], v_out.at[layer], out_sems.at[1])
    v_copy.start()
    k_copy.wait()
    v_copy.wait()


def attend_window(layer, size, ids, q, new_kv, mlp, w_out, k_t, v_t, near, pipe, k_buf, v_buf):
    heads, dim, shard = k_t.shape[2:]
    half = shard // UNIT
    n_pipe = len(pipe)
    return pl.pallas_call(
        functools.partial(window_body, layer, size, half, n_pipe),
        in_specs=[SMEM, VMEM, VMEM, VMEM] + [HBM] * (4 + n_pipe + 2),
        out_specs=[VMEM, HBM, HBM],
        out_shape=[jax.ShapeDtypeStruct(mlp.shape, F32), jax.ShapeDtypeStruct(k_buf.shape, BF16), jax.ShapeDtypeStruct(v_buf.shape, BF16)],
        scratch_shapes=[
            pltpu.VMEM((2, heads, dim, 2 * shard), BF16),
            pltpu.VMEM((2, heads, dim, UNIT), BF16),
            pltpu.VMEM(w_out.shape[1:], BF16),
            pltpu.VMEM((q.shape[0] * q.shape[1], 2 * shard), F32),
            pltpu.VMEM((q.shape[0] * q.shape[1], 2 * shard), BF16),
            pltpu.SemaphoreType.DMA((2,)),
            pltpu.SemaphoreType.DMA((2,)),
            pltpu.SemaphoreType.DMA,
        ],
        input_output_aliases={8 + n_pipe: 1, 9 + n_pipe: 2},
        cost_estimate=cost(16 * heads * dim * shard),
        name="attend_window",
    )(ids, q, new_kv, mlp, w_out, k_t, v_t, near, *pipe, k_buf, v_buf)


def fetch_row(layer, me, own, blocks, kv, sem):
    shard = blocks[0].shape[-1]
    for relation in range(4):
        at = pl.ds(pl.multiple_of(jnp.bitwise_xor(me, relation) * shard, UNIT), shard)
        src = own.at[layer, me] if relation == 0 else blocks[relation - 1]
        move([(src, kv.at[:, :, at], sem)])


def scores_body(layer, ids, q_ref, new_ref, own, b1, b2, b3, w_ref, k_out, kv, sem, out_sem, scores):
    me = ids[0]
    length = ids[1 + me]
    fetch_row(layer, me, own, (b1, b2, b3), kv, sem)
    pltpu.make_async_copy(kv, kv, sem).wait()
    settle(kv, new_ref[0], length, jnp.zeros_like, (length // UNIT, kv.shape[-1] // UNIT))
    w_ref[...] = softmax_weights(stacked(q_ref), kv, scores, length)
    copy = pltpu.make_async_copy(kv, k_out, out_sem)
    copy.start()
    copy.wait()


def values_body(layer, ids, w_ref, new_ref, mlp_ref, wo_hbm, own, b1, b2, b3, part_ref, v_out, kv, wo, sem, out_sem, wo_sem):
    me = ids[0]
    length = ids[1 + me]
    fetch_row(layer, me, own, (b1, b2, b3), kv, sem)
    wo_copy = pltpu.make_async_copy(wo_hbm.at[layer], wo, wo_sem)
    wo_copy.start()
    pltpu.make_async_copy(kv, kv, sem).wait()
    settle(kv, new_ref[1], length, jnp.zeros_like, (length // UNIT, kv.shape[-1] // UNIT))
    wo_copy.wait()
    mix_and_project(w_ref, kv, wo, mlp_ref, part_ref)
    copy = pltpu.make_async_copy(kv, v_out, out_sem)
    copy.start()
    copy.wait()


def attend_global(layer, ids, q, new_kv, mlp, w_out, k_t, v_t, k_blocks, v_blocks):
    heads, dim, shard = k_t.shape[2:]
    row = jax.ShapeDtypeStruct((heads, dim, 4 * shard), BF16)
    scratch = [pltpu.VMEM(row.shape, BF16), pltpu.SemaphoreType.DMA, pltpu.SemaphoreType.DMA]
    n_q = q.shape[0] * q.shape[1]
    weights, k_glob = pl.pallas_call(
        functools.partial(scores_body, layer),
        in_specs=[SMEM, VMEM, VMEM] + [HBM] * 4,
        out_specs=[VMEM, HBM],
        out_shape=[jax.ShapeDtypeStruct((n_q, 4 * shard), BF16), row],
        scratch_shapes=scratch + [pltpu.VMEM((n_q, 4 * shard), F32)],
        cost_estimate=cost(16 * heads * dim * shard),
        name="scores",
    )(ids, q, new_kv, k_t, *k_blocks)
    part, v_glob = pl.pallas_call(
        functools.partial(values_body, layer),
        in_specs=[SMEM, VMEM, VMEM, VMEM] + [HBM] * 5,
        out_specs=[VMEM, HBM],
        out_shape=[jax.ShapeDtypeStruct(mlp.shape, F32), row],
        scratch_shapes=scratch[:1] + [pltpu.VMEM(w_out.shape[1:], BF16)] + [pltpu.SemaphoreType.DMA] * 3,
        cost_estimate=cost(16 * heads * dim * shard),
        name="values",
    )(ids, weights, new_kv, mlp, w_out, v_t, *v_blocks)
    return part, k_glob, v_glob


def summed(tp, residual, parts):
    total = residual.astype(F32)
    for t in range(4):
        at = jnp.bitwise_xor(tp, t)
        pick = parts[3][...]
        for r in range(3):
            pick = jnp.where(at == r, parts[r][...], pick)
        total = pick if t == 0 else total + pick
    return (residual.astype(F32) + total).astype(BF16)


def front_body(layer, dim, n_parts, tp_ref, h_ref, *refs):
    parts, (gain, cosine, sine, wq, wk, wv, wg, wu, wd, h_out, q_out, new_out, mlp_out, u, acc) = refs[:n_parts], refs[n_parts:]
    step = pl.program_id(0)

    def turn(proj):
        if cosine is None:
            return proj
        width = proj.shape[1]
        lane = lax.broadcasted_iota(jnp.int32, proj.shape, 1)
        ahead = pltpu.roll(proj, width - dim // 2, 1)
        behind = pltpu.roll(proj, dim // 2, 1)
        swapped = jnp.where(lax.rem(lane, dim) < dim // 2, -ahead, behind)
        return proj * cosine[...] + swapped * sine[...]

    def over_rows(mats):
        depth = 4 * UNIT

        def block(i, sums):
            rows = lanes(i * 4, 4)
            return tuple(t + jnp.dot(u[:, rows], m[0, rows, :], preferred_element_type=F32) for t, m in zip(sums, mats))

        return lax.fori_loop(0, u.shape[1] // depth, block, tuple(jnp.zeros((u.shape[0], m.shape[2]), F32) for m in mats))

    def rounded(proj):
        return proj.astype(BF16).astype(F32)

    @pl.when(step == 0)
    def _():
        h = summed(tp_ref[0], h_ref[...], parts) if n_parts else h_ref[...]
        h_out[...] = h
        rows32 = h.astype(F32)
        centered = rows32 - rows32.mean(axis=-1, keepdims=True)
        variance = (centered * centered).mean(axis=-1, keepdims=True)
        scaled = centered * lax.rsqrt(variance + NORM_EPS) * gain[...].astype(F32)[layer:layer + 1]
        u[...] = jnp.broadcast_to(scaled, u.shape).astype(BF16)
        acc[...] = jnp.zeros_like(acc)
        both = over_rows((wk, wv))
        key_new, value_new = rounded(turn(both[0])), rounded(both[1])
        for part, new in ((0, key_new), (1, value_new)):
            for head in range(new_out.shape[1]):
                new_out[part, head:head + 1, :] = new[0:1, head * dim:(head + 1) * dim]

    query, gate, up = over_rows((wq, wg, wu))
    query = rounded(turn(query))
    for head in range(q_out.shape[1]):
        q_out[0, head:head + 1, :] = query[0:1, head * dim:(head + 1) * dim]
    active = (jax.nn.silu(gate) * up).astype(BF16)

    def down(i, carry):
        at = lanes(i * 4, 4)
        acc[:, at] += jnp.dot(active, wd[0, :, at], preferred_element_type=F32)
        return carry

    lax.fori_loop(0, acc.shape[1] // (4 * UNIT), down, 0)

    @pl.when(step == FFN_STEPS - 1)
    def _():
        mlp_out[...] = acc[0:1, :]


def plain_front_body(layer, dim, n_parts, tp_ref, h_ref, *refs):
    front_body(layer, dim, n_parts, tp_ref, h_ref, *refs[:n_parts + 1], None, None, *refs[n_parts + 1:])


def front(layer, dim, tp, residual, parts, ln_gain, turns, w_query, w_key, w_value, w_gate, w_up, w_down):
    width = residual.shape[1]
    q_width, kv_width, ffn = w_query.shape[2], w_key.shape[2], w_gate.shape[2]
    q_step, ffn_step = q_width // FFN_STEPS, ffn // FFN_STEPS
    whole = lambda *shape: pl.BlockSpec(shape, lambda j: (0,) * len(shape))
    col = lambda rows, cols: pl.BlockSpec((1, rows, cols), lambda j: (layer, 0, j))
    fixed = lambda rows, cols: pl.BlockSpec((1, rows, cols), lambda j: (layer, 0, 0))
    n_parts = len(parts)
    body = front_body if turns else plain_front_body
    return pl.pallas_call(
        functools.partial(body, layer, dim, n_parts),
        grid=(FFN_STEPS,),
        in_specs=[SMEM, whole(1, width)] + [whole(1, width)] * n_parts + [whole(*ln_gain.shape)] + [whole(1, kv_width)] * len(turns)
        + [col(width, q_step), fixed(width, kv_width), fixed(width, kv_width), col(width, ffn_step), col(width, ffn_step), pl.BlockSpec((1, ffn_step, width), lambda j: (layer, j, 0))],
        out_specs=[whole(1, width), pl.BlockSpec((1, q_step // dim, dim), lambda j: (j, 0, 0)), whole(2, kv_width // dim, dim), whole(1, width)],
        out_shape=[
            jax.ShapeDtypeStruct((1, width), BF16),
            jax.ShapeDtypeStruct((FFN_STEPS, q_step // dim, dim), F32),
            jax.ShapeDtypeStruct((2, kv_width // dim, dim), F32),
            jax.ShapeDtypeStruct((1, width), F32),
        ],
        scratch_shapes=[pltpu.VMEM((8, width), BF16), pltpu.VMEM((8, width), F32)],
        compiler_params=pltpu.CompilerParams(dimension_semantics=("arbitrary",)),
        cost_estimate=cost(2 * width * (q_width + 2 * kv_width + 3 * ffn)),
        name="front",
    )(tp, residual, *parts, ln_gain, *turns, w_query, w_key, w_value, w_gate, w_up, w_down)


def close_body(tp_ref, h_ref, p0, p1, p2, p3, out_ref):
    out_ref[...] = summed(tp_ref[0], h_ref[...], (p0, p1, p2, p3))


def close(tp, residual, parts):
    return pl.pallas_call(
        close_body,
        in_specs=[SMEM] + [VMEM] * 5,
        out_specs=VMEM,
        out_shape=jax.ShapeDtypeStruct(residual.shape, BF16),
        name="close",
    )(tp, residual, *parts)


def fresh_body(*refs):
    pass


def fresh_buffers(shapes):
    return pl.pallas_call(fresh_body, out_specs=[HBM] * len(shapes), out_shape=[jax.ShapeDtypeStruct(s, BF16) for s in shapes], name="fresh")()


def solution(mesh):
    cache_spec = P(None, "dp", "tp", "sp", None)
    row_spec = P(("dp", "sp"), None)
    col_spec = P(None, None, "tp")
    inner_spec = P(None, "tp", None)
    window_spec = P(None, ("dp", "sp"), "tp", None, None)
    global_spec = P(("dp", "sp"), "tp", None, None)
    in_specs = (cache_spec, cache_spec, P("dp"), row_spec, P(None, None), col_spec, col_spec, col_spec, inner_spec, col_spec, col_spec, inner_spec)
    out_specs = (row_spec, window_spec, window_spec, global_spec, global_spec)
    n_sp, n_tp = mesh.shape["sp"], mesh.shape["tp"]

    def swap(t, axis, relation):
        return lax.ppermute(t, axis, [(i, i ^ relation) for i in range(n_sp if axis == "sp" else n_tp)])

    def device_step(k_cache, v_cache, lengths, hidden, ln_gain, w_query, w_key, w_value, w_out, w_gate, w_up, w_down):
        n_layers = w_query.shape[0]
        heads, shard, dim = k_cache.shape[2:]
        half = shard // UNIT
        final = n_layers - 1
        me = lax.axis_index("sp").astype(jnp.int32)
        tp = lax.axis_index("tp").astype(jnp.int32)[None]
        ids = jnp.concatenate([me[None], lengths])
        k_t = jnp.swapaxes(k_cache, 3, 4)
        v_t = jnp.swapaxes(v_cache, 3, 4)

        inv_freq = 1.0 / (ROPE_BASE ** (jnp.arange(dim // 2, dtype=F32) * 2.0 / dim))
        angles = lax.dynamic_slice_in_dim(lengths, me, 1).astype(F32)[:, None] * inv_freq[None, :]
        repeat = 2 * w_key.shape[2] // dim
        turns = (jnp.tile(jnp.cos(angles), (1, repeat)), jnp.tile(jnp.sin(angles), (1, repeat)))

        _, counts = crossing(lengths - WINDOW, jnp.arange(n_sp) >= n_sp // 2, 2 * half)
        need = lax.pmax(jnp.max((counts.reshape(2, -1).sum(axis=1) + 1) // 2), "dp")
        choice = sum((need > size).astype(jnp.int32) for size in SIZES[:-1])

        def block(t, relation):
            return lax.dynamic_slice(t, (final, jnp.bitwise_xor(me, relation), 0, 0, 0), (1, 1, heads, dim, shard))[0, 0]

        far_cut = block(k_t, 2)
        k_far = swap(far_cut, "sp", 2)
        first_near = swap(cut(0, after(ids, far_cut), k_t, v_t), "sp", 1)

        def run(size):
            return run_scoped(size)

        def run_scoped(size):
            k_win, v_win = fresh_buffers([(final, heads, dim, WINDOW)] * 2)
            near, pipes = [first_near], []
            for layer in range(final):
                packed = pack(layer, size, ids, k_t, v_t, near[layer])
                pipes.append([swap(p, "sp", 2) for p in packed])
                if layer + 1 < final:
                    near.append(swap(cut(layer + 1, after(ids, packed[0]), k_t, v_t), "sp", 1))
            late = [(k_t, 3), (k_t, 1), (v_t, 2), (v_t, 3), (v_t, 1)]
            cuts = lax.optimization_barrier((packed[0], [block(t, r) for t, r in late]))[1]
            k_cross, k_near, v_far, v_cross, v_near = [swap(c, "sp", r) for c, (_, r) in zip(cuts, late)]
            residual, parts = hidden, ()
            turn = after(tp, *cuts)
            for layer in range(n_layers):
                sliding = layer < final
                residual, q, new_kv, mlp = front(layer, dim, turn, residual, parts, ln_gain, turns if sliding else (), w_query, w_key, w_value, w_gate, w_up, w_down)
                if sliding:
                    if size < 2 * half:
                        pipes[layer].append(swap(after(pipes[layer][0], q), "sp", 1))
                    part, k_win, v_win = attend_window(layer, size, ids, q, new_kv, mlp, w_out, k_t, v_t, near[layer], pipes[layer], k_win, v_win)
                else:
                    part, k_glob, v_glob = attend_global(layer, ids, q, new_kv, mlp, w_out, k_t, v_t, [k_near, k_far, k_cross], [v_near, v_far, v_cross])
                parts = (part,) + tuple(swap(part, "tp", r) for r in (1, 2, 3))
            return close(tp, residual, parts), k_win, v_win, k_glob, v_glob

        if len(SIZES) == 1:
            out, k_win, v_win, k_glob, v_glob = run(SIZES[0])
        else:
            out, k_win, v_win, k_glob, v_glob = lax.switch(choice, [functools.partial(run, size) for size in SIZES])
        back = lambda t: jnp.swapaxes(t, -1, -2)
        return out, back(k_win)[:, None], back(v_win)[:, None], back(k_glob)[None], back(v_glob)[None]

    return jax.shard_map(device_step, mesh=mesh, in_specs=in_specs, out_specs=out_specs, check_vma=False)
```

```python
import functools

import jax
import jax.numpy as jnp
from jax import lax
from jax.experimental import pallas as pl
from jax.experimental.pallas import tpu as pltpu
from jax.sharding import PartitionSpec as P


WINDOW = 4096
ROPE_BASE = 50000
NORM_EPS = 1e-5
UNIT = 128
SIZES = (16, 20, 24, 28, 32)
FFN_STEPS = 4
CHUNK = 16
HBM = pl.BlockSpec(memory_space=pltpu.HBM)
VMEM = pl.BlockSpec(memory_space=pltpu.VMEM)
SMEM = pl.BlockSpec(memory_space=pltpu.SMEM)
F32 = jnp.float32
BF16 = jnp.bfloat16


def cost(n_bytes):
    return pl.CostEstimate(flops=n_bytes, bytes_accessed=n_bytes, transcendentals=0)


def lanes(block, count=1):
    return pl.ds(pl.multiple_of(block * UNIT, UNIT), count * UNIT)


def crossing(beta, on_second_chip, n_units):
    above = (beta + 1) // UNIT
    below = (beta + UNIT - 1) // UNIT
    return jnp.where(on_second_chip, above, 0), jnp.where(on_second_chip, n_units - above, below)


def move(pairs):
    for src, dst, sem in pairs:
        pltpu.make_async_copy(src, dst, sem).start()


def pack_body(layer, size, half, ids, k_own, v_own, near, *refs):
    outs, (buf, sem, out_sem) = refs[:-3], refs[-3:]
    me = ids[0]
    core = lax.rem(me, 2)
    base = (1 - me // 2) * 2
    second = base == 2
    row, other = base + core, base + 1 - core
    first, count = crossing(ids[1 + row] - WINDOW, second, 2 * half)
    other_first, other_count = crossing(ids[1 + other] - WINDOW, second, 2 * half)
    over = jnp.maximum(other_count - size, 0)

    def issue(i, carry):
        mine = i < count
        dest = jnp.where(mine, row, other)
        unit = jnp.where(mine, first + i, other_first + size + i - (size - over))
        unit = jnp.clip(unit, 0, 2 * half - 1)
        at = lanes(lax.rem(unit, half))
        local = unit // half == core

        @pl.when(local)
        def _():
            move([(k_own.at[layer, dest, :, :, at], buf.at[0, :, :, lanes(i)], sem), (v_own.at[layer, dest, :, :, at], buf.at[1, :, :, lanes(i)], sem)])

        @pl.when(jnp.logical_not(local))
        def _():
            move([(near.at[p, dest, :, :, at], buf.at[p, :, :, lanes(i)], sem) for p in range(2)])

        return carry

    lax.fori_loop(0, size, issue, 0)
    pltpu.make_async_copy(buf, buf, sem).wait()
    cut = size - half
    copies = [pltpu.make_async_copy(buf.at[:, :, :, cut * UNIT:], outs[0], out_sem)]
    if cut:
        copies.append(pltpu.make_async_copy(buf.at[:, :, :, :cut * UNIT], outs[1], out_sem))
    for copy in copies:
        copy.start()
    for copy in copies:
        copy.wait()


def pack(layer, size, ids, k_t, v_t, near):
    heads, dim, shard = k_t.shape[2:]
    half = shard // UNIT
    widths = [half] + ([size - half] if size > half else [])
    return pl.pallas_call(
        functools.partial(pack_body, layer, size, half),
        in_specs=[SMEM, HBM, HBM, HBM],
        out_specs=[HBM] * len(widths),
        out_shape=[jax.ShapeDtypeStruct((2, heads, dim, w * UNIT), BF16) for w in widths],
        scratch_shapes=[pltpu.VMEM((2, heads, dim, size * UNIT), BF16), pltpu.SemaphoreType.DMA, pltpu.SemaphoreType.DMA],
        cost_estimate=cost(8 * heads * dim * size * UNIT),
        name="pack",
    )(ids, k_t, v_t, near)


def cut_body(layer, ids, k_own, v_own, out, buf, in_sems, out_sem):
    rows = k_own.shape[1]
    loads = [pltpu.make_async_copy((k_own, v_own)[i // rows].at[layer, i % rows], buf.at[i], in_sems.at[i]) for i in range(2 * rows)]
    stores = [pltpu.make_async_copy(buf.at[i], out.at[i // rows, i % rows], out_sem) for i in range(2 * rows)]
    for load in loads:
        load.start()
    for load, store in zip(loads, stores):
        load.wait()
        store.start()
    for store in stores:
        store.wait()


def cut(layer, ids, k_t, v_t):
    shape = k_t.shape[1:]
    return pl.pallas_call(
        functools.partial(cut_body, layer),
        in_specs=[SMEM, HBM, HBM],
        out_specs=HBM,
        out_shape=jax.ShapeDtypeStruct((2,) + shape, BF16),
        scratch_shapes=[pltpu.VMEM((2 * shape[0],) + shape[1:], BF16), pltpu.SemaphoreType.DMA((2 * shape[0],)), pltpu.SemaphoreType.DMA],
        cost_estimate=cost(8 * k_t.size // k_t.shape[0]),
        name="cut",
    )(ids, k_t, v_t)


def after(value, *others):
    return lax.optimization_barrier((value, others))[0]


def settle(kv, new_rows, beta, rest_of, units):
    fresh = new_rows[:, :, None]
    lane = lax.broadcasted_iota(jnp.int32, (1, 1, UNIT), 2)

    def fix(w, carry):
        pos = lane + w * UNIT
        old = kv[:, :, lanes(w)].astype(F32)
        put = jnp.where(pos < beta, old, jnp.where(pos == beta, fresh, rest_of(old)))
        kv[:, :, lanes(w)] = put.astype(BF16)
        return carry

    lax.fori_loop(*units, fix, 0)


def stacked(q_ref):
    return jnp.concatenate([q_ref[j] for j in range(q_ref.shape[0])], axis=0).astype(BF16)


def softmax_weights(q, keys, scores, beta):
    upper = lax.broadcasted_iota(jnp.int32, (q.shape[0], 1), 0) < q.shape[0] // 2

    def chunk(i, carry):
        at = lanes(i * CHUNK, CHUNK)
        s0 = jnp.dot(q, keys[0, :, at], preferred_element_type=F32)
        s1 = jnp.dot(q, keys[1, :, at], preferred_element_type=F32)
        part = jnp.where(upper, s0, s1) * (q.shape[1] ** -0.5)
        if beta is not None:
            part = jnp.where(lax.broadcasted_iota(jnp.int32, (1, part.shape[1]), 1) + i * CHUNK * UNIT <= beta, part, -1e30)
        scores[:, at] = part
        return carry

    lax.fori_loop(0, keys.shape[-1] // (CHUNK * UNIT), chunk, 0)
    top = scores[...].max(axis=-1, keepdims=True)
    expd = jnp.exp(scores[...] - top)
    return (expd / expd.sum(axis=-1, keepdims=True)).astype(BF16)


def mix_and_project(weights, values, copy, wo, mlp, out):
    rows = weights.shape[0]
    dim = values.shape[1]
    upper = lax.broadcasted_iota(jnp.int32, (rows, 1), 0) < rows // 2
    dims = (((1,), (1,)), ((), ()))

    def chunk(i, carry):
        at = lanes(i * CHUNK, CHUNK)
        return tuple(carry[h] + lax.dot_general(weights[:, at], values[h, :, at], dims, preferred_element_type=F32) for h in range(2))

    m0, m1 = lax.fori_loop(0, values.shape[-1] // (CHUNK * UNIT), chunk, (jnp.zeros((rows, dim), F32),) * 2)
    copy.start()
    mixed = jnp.where(upper, m0, m1).astype(BF16).astype(F32)
    flat = jnp.concatenate([mixed[j:j + 1] for j in range(rows)], axis=1)
    flat = jnp.broadcast_to(flat, (8, flat.shape[1])).astype(BF16)

    def project(i, carry):
        at = lanes(i * 4, 4)
        out[:, at] = jnp.dot(flat, wo[:, at], preferred_element_type=F32)[0:1] + mlp[:, at]
        return carry

    lax.fori_loop(0, out.shape[1] // (4 * UNIT), project, 0)


def window_body(layer, size, half, n_pipe, ids, q_ref, new_ref, mlp_ref, wo_hbm, k_own, v_own, near, *refs):
    pipe = refs[:n_pipe]
    k_out, v_out = refs[n_pipe + 3:n_pipe + 5]
    part_ref = refs[n_pipe + 2]
    kv, edge, wo, scores, weights, sems, out_sems, wo_sem = refs[n_pipe + 5:]
    me = ids[0]
    core = lax.rem(me, 2)
    second = me // 2 == 1
    beta = ids[1 + me] - WINDOW
    last = beta // UNIT
    first, count = crossing(beta, second, 2 * half)
    over = jnp.maximum(count - size, 0)
    cut = size - half

    def fetch(w, low, part, dst, sem):
        high = jnp.logical_and(w <= last, jnp.logical_not(low))
        crosses = jnp.logical_xor(high, second)
        at = lanes(lax.rem(w, half))
        local = w // half == core
        idx = jnp.clip(w - first, 0, 2 * half - 1)
        stay = jnp.logical_not(crosses)

        @pl.when(jnp.logical_and(stay, local))
        def _():
            move([((k_own, v_own)[part].at[layer, me, :, :, at], dst, sem)])

        @pl.when(jnp.logical_and(stay, jnp.logical_not(local)))
        def _():
            move([(near.at[part, me, :, :, at], dst, sem)])

        @pl.when(jnp.logical_and(crosses, jnp.logical_and(idx >= cut, idx < size)))
        def _():
            move([(pipe[0].at[part, :, :, lanes(idx - cut)], dst, sem)])

        if cut:
            @pl.when(jnp.logical_and(crosses, idx < cut))
            def _():
                move([(pipe[1].at[part, :, :, lanes(idx)], dst, sem)])

        if size < 2 * half:
            @pl.when(jnp.logical_and(crosses, idx >= size))
            def _():
                move([(pipe[-1].at[part, :, :, lanes(jnp.clip(half - over + idx - size, 0, half - 1))], dst, sem)])

    wo_copy = pltpu.make_async_copy(wo_hbm.at[layer], wo, wo_sem)
    for part in range(2):
        def issue(w, carry, part=part):
            fetch(w, False, part, kv.at[part, :, :, lanes(w)], sems.at[part])
            return carry

        lax.fori_loop(0, 2 * half, issue, 0)
        fetch(last, True, part, edge.at[part], sems.at[part])
    wo_copy.start()

    def ready(part):
        pltpu.make_async_copy(kv.at[part], kv.at[part], sems.at[part]).wait()
        pltpu.make_async_copy(edge.at[part], edge.at[part], sems.at[part]).wait()
        settle(kv.at[part], new_ref[part], beta, lambda old: edge[part].astype(F32), (last, last + 1))

    ready(0)
    weights[...] = softmax_weights(stacked(q_ref), kv.at[0], scores, None)
    k_copy = pltpu.make_async_copy(kv.at[0], k_out.at[layer], out_sems.at[0])
    k_copy.start()
    ready(1)
    wo_copy.wait()
    v_copy = pltpu.make_async_copy(kv.at[1], v_out.at[layer], out_sems.at[1])
    mix_and_project(weights, kv.at[1], v_copy, wo, mlp_ref, part_ref)
    k_copy.wait()
    v_copy.wait()


def attend_window(layer, size, ids, q, new_kv, mlp, w_out, k_t, v_t, near, pipe, k_buf, v_buf):
    heads, dim, shard = k_t.shape[2:]
    half = shard // UNIT
    n_pipe = len(pipe)
    return pl.pallas_call(
        functools.partial(window_body, layer, size, half, n_pipe),
        in_specs=[SMEM, VMEM, VMEM, VMEM] + [HBM] * (4 + n_pipe + 2),
        out_specs=[VMEM, HBM, HBM],
        out_shape=[jax.ShapeDtypeStruct(mlp.shape, F32), jax.ShapeDtypeStruct(k_buf.shape, BF16), jax.ShapeDtypeStruct(v_buf.shape, BF16)],
        scratch_shapes=[
            pltpu.VMEM((2, heads, dim, 2 * shard), BF16),
            pltpu.VMEM((2, heads, dim, UNIT), BF16),
            pltpu.VMEM(w_out.shape[1:], BF16),
            pltpu.VMEM((q.shape[0] * q.shape[1], 2 * shard), F32),
            pltpu.VMEM((q.shape[0] * q.shape[1], 2 * shard), BF16),
            pltpu.SemaphoreType.DMA((2,)),
            pltpu.SemaphoreType.DMA((2,)),
            pltpu.SemaphoreType.DMA,
        ],
        input_output_aliases={8 + n_pipe: 1, 9 + n_pipe: 2},
        cost_estimate=cost(16 * heads * dim * shard),
        name="attend_window",
    )(ids, q, new_kv, mlp, w_out, k_t, v_t, near, *pipe, k_buf, v_buf)


def fetch_row(layer, me, own, blocks, kv, sem):
    shard = blocks[0].shape[-1]
    for relation in range(4):
        at = pl.ds(pl.multiple_of(jnp.bitwise_xor(me, relation) * shard, UNIT), shard)
        src = own.at[layer, me] if relation == 0 else blocks[relation - 1]
        move([(src, kv.at[:, :, at], sem)])


def scores_body(layer, ids, q_ref, new_ref, own, b1, b2, b3, w_ref, k_out, kv, sem, out_sem, scores):
    me = ids[0]
    length = ids[1 + me]
    fetch_row(layer, me, own, (b1, b2, b3), kv, sem)
    pltpu.make_async_copy(kv, kv, sem).wait()
    settle(kv, new_ref[0], length, jnp.zeros_like, (length // UNIT, kv.shape[-1] // UNIT))
    w_ref[...] = softmax_weights(stacked(q_ref), kv, scores, length)
    copy = pltpu.make_async_copy(kv, k_out, out_sem)
    copy.start()
    copy.wait()


def values_body(layer, ids, w_ref, new_ref, mlp_ref, wo_hbm, own, b1, b2, b3, part_ref, v_out, kv, wo, sem, out_sem, wo_sem):
    me = ids[0]
    length = ids[1 + me]
    fetch_row(layer, me, own, (b1, b2, b3), kv, sem)
    wo_copy = pltpu.make_async_copy(wo_hbm.at[layer], wo, wo_sem)
    wo_copy.start()
    pltpu.make_async_copy(kv, kv, sem).wait()
    settle(kv, new_ref[1], length, jnp.zeros_like, (length // UNIT, kv.shape[-1] // UNIT))
    wo_copy.wait()
    copy = pltpu.make_async_copy(kv, v_out, out_sem)
    mix_and_project(w_ref, kv, copy, wo, mlp_ref, part_ref)
    copy.wait()


def attend_global(layer, ids, q, new_kv, mlp, w_out, k_t, v_t, k_blocks, v_blocks):
    heads, dim, shard = k_t.shape[2:]
    row = jax.ShapeDtypeStruct((heads, dim, 4 * shard), BF16)
    scratch = [pltpu.VMEM(row.shape, BF16), pltpu.SemaphoreType.DMA, pltpu.SemaphoreType.DMA]
    n_q = q.shape[0] * q.shape[1]
    weights, k_glob = pl.pallas_call(
        functools.partial(scores_body, layer),
        in_specs=[SMEM, VMEM, VMEM] + [HBM] * 4,
        out_specs=[VMEM, HBM],
        out_shape=[jax.ShapeDtypeStruct((n_q, 4 * shard), BF16), row],
        scratch_shapes=scratch + [pltpu.VMEM((n_q, 4 * shard), F32)],
        cost_estimate=cost(16 * heads * dim * shard),
        name="scores",
    )(ids, q, new_kv, k_t, *k_blocks)
    part, v_glob = pl.pallas_call(
        functools.partial(values_body, layer),
        in_specs=[SMEM, VMEM, VMEM, VMEM] + [HBM] * 5,
        out_specs=[VMEM, HBM],
        out_shape=[jax.ShapeDtypeStruct(mlp.shape, F32), row],
        scratch_shapes=scratch[:1] + [pltpu.VMEM(w_out.shape[1:], BF16)] + [pltpu.SemaphoreType.DMA] * 3,
        cost_estimate=cost(16 * heads * dim * shard),
        name="values",
    )(ids, weights, new_kv, mlp, w_out, v_t, *v_blocks)
    return part, k_glob, v_glob


def summed(tp, residual, parts):
    total = residual.astype(F32)
    for t in range(4):
        at = jnp.bitwise_xor(tp, t)
        pick = parts[3][...]
        for r in range(3):
            pick = jnp.where(at == r, parts[r][...], pick)
        total = pick if t == 0 else total + pick
    return (residual.astype(F32) + total).astype(BF16)


def front_body(layer, dim, n_parts, tp_ref, h_ref, *refs):
    parts, (gain, cosine, sine, wq, wk, wv, wg, wu, wd, h_out, q_out, new_out, mlp_out, u, acc) = refs[:n_parts], refs[n_parts:]
    step = pl.program_id(0)

    def turn(proj):
        if cosine is None:
            return proj
        width = proj.shape[1]
        lane = lax.broadcasted_iota(jnp.int32, proj.shape, 1)
        ahead = pltpu.roll(proj, width - dim // 2, 1)
        behind = pltpu.roll(proj, dim // 2, 1)
        swapped = jnp.where(lax.rem(lane, dim) < dim // 2, -ahead, behind)
        return proj * cosine[...] + swapped * sine[...]

    def over_rows(mats):
        depth = 8 * UNIT

        def block(i, sums):
            rows = lanes(i * 8, 8)
            return tuple(t + jnp.dot(u[:, rows], m[0, rows, :], preferred_element_type=F32) for t, m in zip(sums, mats))

        return lax.fori_loop(0, u.shape[1] // depth, block, tuple(jnp.zeros((u.shape[0], m.shape[2]), F32) for m in mats))

    def rounded(proj):
        return proj.astype(BF16).astype(F32)

    @pl.when(step == 0)
    def _():
        h = summed(tp_ref[0], h_ref[...], parts) if n_parts else h_ref[...]
        h_out[...] = h
        rows32 = h.astype(F32)
        centered = rows32 - rows32.mean(axis=-1, keepdims=True)
        variance = (centered * centered).mean(axis=-1, keepdims=True)
        scaled = centered * lax.rsqrt(variance + NORM_EPS) * gain[...].astype(F32)[layer:layer + 1]
        u[...] = jnp.broadcast_to(scaled, u.shape).astype(BF16)
        acc[...] = jnp.zeros_like(acc)
        both = over_rows((wk, wv))
        key_new, value_new = rounded(turn(both[0])), rounded(both[1])
        for part, new in ((0, key_new), (1, value_new)):
            for head in range(new_out.shape[1]):
                new_out[part, head:head + 1, :] = new[0:1, head * dim:(head + 1) * dim]

    query, gate, up = over_rows((wq, wg, wu))
    query = rounded(turn(query))
    for head in range(q_out.shape[1]):
        q_out[0, head:head + 1, :] = query[0:1, head * dim:(head + 1) * dim]
    active = (jax.nn.silu(gate) * up).astype(BF16)

    def down(i, carry):
        at = lanes(i * 8, 8)
        acc[:, at] += jnp.dot(active, wd[0, :, at], preferred_element_type=F32)
        return carry

    lax.fori_loop(0, acc.shape[1] // (8 * UNIT), down, 0)

    @pl.when(step == FFN_STEPS - 1)
    def _():
        mlp_out[...] = acc[0:1, :]


def plain_front_body(layer, dim, n_parts, tp_ref, h_ref, *refs):
    front_body(layer, dim, n_parts, tp_ref, h_ref, *refs[:n_parts + 1], None, None, *refs[n_parts + 1:])


def front(layer, dim, tp, residual, parts, ln_gain, turns, w_query, w_key, w_value, w_gate, w_up, w_down):
    width = residual.shape[1]
    q_width, kv_width, ffn = w_query.shape[2], w_key.shape[2], w_gate.shape[2]
    q_step, ffn_step = q_width // FFN_STEPS, ffn // FFN_STEPS
    whole = lambda *shape: pl.BlockSpec(shape, lambda j: (0,) * len(shape))
    col = lambda rows, cols: pl.BlockSpec((1, rows, cols), lambda j: (layer, 0, j))
    fixed = lambda rows, cols: pl.BlockSpec((1, rows, cols), lambda j: (layer, 0, 0))
    n_parts = len(parts)
    body = front_body if turns else plain_front_body
    return pl.pallas_call(
        functools.partial(body, layer, dim, n_parts),
        grid=(FFN_STEPS,),
        in_specs=[SMEM, whole(1, width)] + [whole(1, width)] * n_parts + [whole(*ln_gain.shape)] + [whole(1, kv_width)] * len(turns)
        + [col(width, q_step), fixed(width, kv_width), fixed(width, kv_width), col(width, ffn_step), col(width, ffn_step), pl.BlockSpec((1, ffn_step, width), lambda j: (layer, j, 0))],
        out_specs=[whole(1, width), pl.BlockSpec((1, q_step // dim, dim), lambda j: (j, 0, 0)), whole(2, kv_width // dim, dim), whole(1, width)],
        out_shape=[
            jax.ShapeDtypeStruct((1, width), BF16),
            jax.ShapeDtypeStruct((FFN_STEPS, q_step // dim, dim), F32),
            jax.ShapeDtypeStruct((2, kv_width // dim, dim), F32),
            jax.ShapeDtypeStruct((1, width), F32),
        ],
        scratch_shapes=[pltpu.VMEM((8, width), BF16), pltpu.VMEM((8, width), F32)],
        compiler_params=pltpu.CompilerParams(dimension_semantics=("arbitrary",)),
        cost_estimate=cost(2 * width * (q_width + 2 * kv_width + 3 * ffn)),
        name="front",
    )(tp, residual, *parts, ln_gain, *turns, w_query, w_key, w_value, w_gate, w_up, w_down)


def close_body(tp_ref, h_ref, p0, p1, p2, p3, out_ref):
    out_ref[...] = summed(tp_ref[0], h_ref[...], (p0, p1, p2, p3))


def close(tp, residual, parts):
    return pl.pallas_call(
        close_body,
        in_specs=[SMEM] + [VMEM] * 5,
        out_specs=VMEM,
        out_shape=jax.ShapeDtypeStruct(residual.shape, BF16),
        name="close",
    )(tp, residual, *parts)


def fresh_body(*refs):
    pass


def fresh_buffers(shapes):
    return pl.pallas_call(fresh_body, out_specs=[HBM] * len(shapes), out_shape=[jax.ShapeDtypeStruct(s, BF16) for s in shapes], name="fresh")()


def solution(mesh):
    cache_spec = P(None, "dp", "tp", "sp", None)
    row_spec = P(("dp", "sp"), None)
    col_spec = P(None, None, "tp")
    inner_spec = P(None, "tp", None)
    window_spec = P(None, ("dp", "sp"), "tp", None, None)
    global_spec = P(("dp", "sp"), "tp", None, None)
    in_specs = (cache_spec, cache_spec, P("dp"), row_spec, P(None, None), col_spec, col_spec, col_spec, inner_spec, col_spec, col_spec, inner_spec)
    out_specs = (row_spec, window_spec, window_spec, global_spec, global_spec)
    n_sp, n_tp = mesh.shape["sp"], mesh.shape["tp"]

    def swap(t, axis, relation):
        return lax.ppermute(t, axis, [(i, i ^ relation) for i in range(n_sp if axis == "sp" else n_tp)])

    def device_step(k_cache, v_cache, lengths, hidden, ln_gain, w_query, w_key, w_value, w_out, w_gate, w_up, w_down):
        n_layers = w_query.shape[0]
        heads, shard, dim = k_cache.shape[2:]
        half = shard // UNIT
        final = n_layers - 1
        me = lax.axis_index("sp").astype(jnp.int32)
        tp = lax.axis_index("tp").astype(jnp.int32)[None]
        ids = jnp.concatenate([me[None], lengths])
        k_t = jnp.swapaxes(k_cache, 3, 4)
        v_t = jnp.swapaxes(v_cache, 3, 4)

        inv_freq = 1.0 / (ROPE_BASE ** (jnp.arange(dim // 2, dtype=F32) * 2.0 / dim))
        angles = lax.dynamic_slice_in_dim(lengths, me, 1).astype(F32)[:, None] * inv_freq[None, :]
        repeat = 2 * w_key.shape[2] // dim
        turns = (jnp.tile(jnp.cos(angles), (1, repeat)), jnp.tile(jnp.sin(angles), (1, repeat)))

        _, counts = crossing(lengths - WINDOW, jnp.arange(n_sp) >= n_sp // 2, 2 * half)
        need = lax.pmax(jnp.max((counts.reshape(2, -1).sum(axis=1) + 1) // 2), "dp")
        choice = sum((need > size).astype(jnp.int32) for size in SIZES[:-1])

        def block(t, relation):
            return lax.dynamic_slice(t, (final, jnp.bitwise_xor(me, relation), 0, 0, 0), (1, 1, heads, dim, shard))[0, 0]

        far_cut = block(k_t, 2)
        k_far = swap(far_cut, "sp", 2)
        first_cut = cut(0, ids, k_t, v_t)
        first_near = swap(first_cut, "sp", 1)

        def run(size):
            return run_scoped(size)

        def run_scoped(size):
            k_win, v_win = fresh_buffers([(final, heads, dim, WINDOW)] * 2)
            near, pipes = [first_near], []
            for layer in range(final):
                packed = pack(layer, size, ids, k_t, v_t, near[layer])
                pipes.append([swap(p, "sp", 2) for p in packed])
                if layer + 1 < final:
                    near.append(swap(cut(layer + 1, ids, k_t, v_t), "sp", 1))
            late = [(k_t, 3), (k_t, 1), (v_t, 2), (v_t, 3), (v_t, 1)]
            cuts = lax.optimization_barrier((packed[0], [block(t, r) for t, r in late]))[1]
            k_cross, k_near, v_far, v_cross, v_near = [swap(c, "sp", r) for c, (_, r) in zip(cuts, late)]
            residual, parts = hidden, ()
            turn = after(tp, *cuts)
            for layer in range(n_layers):
                sliding = layer < final
                residual, q, new_kv, mlp = front(layer, dim, turn, residual, parts, ln_gain, turns if sliding else (), w_query, w_key, w_value, w_gate, w_up, w_down)
                if sliding:
                    if size < 2 * half:
                        pipes[layer].append(swap(after(pipes[layer][0], q), "sp", 1))
                    part, k_win, v_win = attend_window(layer, size, ids, q, new_kv, mlp, w_out, k_t, v_t, near[layer], pipes[layer], k_win, v_win)
                else:
                    part, k_glob, v_glob = attend_global(layer, ids, q, new_kv, mlp, w_out, k_t, v_t, [k_near, k_far, k_cross], [v_near, v_far, v_cross])
                parts = (part,) + tuple(swap(part, "tp", r) for r in (1, 2, 3))
            return close(tp, residual, parts), k_win, v_win, k_glob, v_glob

        if len(SIZES) == 1:
            out, k_win, v_win, k_glob, v_glob = run(SIZES[0])
        else:
            out, k_win, v_win, k_glob, v_glob = lax.switch(choice, [functools.partial(run, size) for size in SIZES])
        back = lambda t: jnp.swapaxes(t, -1, -2)
        return out, back(k_win)[:, None], back(v_win)[:, None], back(k_glob)[None], back(v_glob)[None]

    return jax.shard_map(device_step, mesh=mesh, in_specs=in_specs, out_specs=out_specs, check_vma=False)
```

```python
import functools

import jax
import jax.numpy as jnp
from jax import lax
from jax.experimental import pallas as pl
from jax.experimental.pallas import tpu as pltpu
from jax.sharding import PartitionSpec as P


WINDOW = 4096
ROPE_BASE = 50000
NORM_EPS = 1e-5
UNIT = 128
SIZES = (18, 23, 28, 32)
FFN_STEPS = 4
CHUNK = 16
HBM = pl.BlockSpec(memory_space=pltpu.HBM)
VMEM = pl.BlockSpec(memory_space=pltpu.VMEM)
SMEM = pl.BlockSpec(memory_space=pltpu.SMEM)
F32 = jnp.float32
BF16 = jnp.bfloat16


def cost(n_bytes):
    return pl.CostEstimate(flops=n_bytes, bytes_accessed=n_bytes, transcendentals=0)


def lanes(block, count=1):
    return pl.ds(pl.multiple_of(block * UNIT, UNIT), count * UNIT)


def crossing(beta, on_second_chip, n_units):
    above = (beta + 1) // UNIT
    below = (beta + UNIT - 1) // UNIT
    return jnp.where(on_second_chip, above, 0), jnp.where(on_second_chip, n_units - above, below)


def move(pairs):
    for src, dst, sem in pairs:
        pltpu.make_async_copy(src, dst, sem).start()


def pack_body(layer, size, half, ids, k_own, v_own, k_near, v_near, *refs):
    outs, (buf, sem, out_sem) = refs[:-3], refs[-3:]
    me = ids[0]
    core = lax.rem(me, 2)
    base = (1 - me // 2) * 2
    second = base == 2
    row, other = base + core, base + 1 - core
    first, count = crossing(ids[1 + row] - WINDOW, second, 2 * half)
    other_first, other_count = crossing(ids[1 + other] - WINDOW, second, 2 * half)
    over = jnp.maximum(other_count - size, 0)

    def issue(i, carry):
        mine = i < count
        dest = jnp.where(mine, row, other)
        unit = jnp.where(mine, first + i, other_first + size + i - (size - over))
        unit = jnp.clip(unit, 0, 2 * half - 1)
        at = lanes(lax.rem(unit, half))
        local = unit // half == core

        @pl.when(local)
        def _():
            move([(k_own.at[layer, dest, :, :, at], buf.at[0, :, :, lanes(i)], sem), (v_own.at[layer, dest, :, :, at], buf.at[1, :, :, lanes(i)], sem)])

        @pl.when(jnp.logical_not(local))
        def _():
            move([(near.at[layer, dest, :, :, at], buf.at[p, :, :, lanes(i)], sem) for p, near in enumerate((k_near, v_near))])

        return carry

    lax.fori_loop(0, size, issue, 0)
    pltpu.make_async_copy(buf, buf, sem).wait()
    cut = size - half
    copies = [pltpu.make_async_copy(buf.at[:, :, :, cut * UNIT:], outs[0], out_sem)]
    if cut:
        copies.append(pltpu.make_async_copy(buf.at[:, :, :, :cut * UNIT], outs[1], out_sem))
    for copy in copies:
        copy.start()
    for copy in copies:
        copy.wait()


def pack(layer, size, ids, k_t, v_t, nears):
    heads, dim, shard = k_t.shape[2:]
    half = shard // UNIT
    widths = [half] + ([size - half] if size > half else [])
    return pl.pallas_call(
        functools.partial(pack_body, layer, size, half),
        in_specs=[SMEM] + [HBM] * 4,
        out_specs=[HBM] * len(widths),
        out_shape=[jax.ShapeDtypeStruct((2, heads, dim, w * UNIT), BF16) for w in widths],
        scratch_shapes=[pltpu.VMEM((2, heads, dim, size * UNIT), BF16), pltpu.SemaphoreType.DMA, pltpu.SemaphoreType.DMA],
        cost_estimate=cost(8 * heads * dim * size * UNIT),
        name="pack",
    )(ids, k_t, v_t, *nears)


def after(value, *others):
    return lax.optimization_barrier((value, others))[0]


def settle(kv, new_rows, beta, rest_of, units):
    fresh = new_rows[:, :, None]
    lane = lax.broadcasted_iota(jnp.int32, (1, 1, UNIT), 2)

    def fix(w, carry):
        pos = lane + w * UNIT
        old = kv[:, :, lanes(w)].astype(F32)
        put = jnp.where(pos < beta, old, jnp.where(pos == beta, fresh, rest_of(old)))
        kv[:, :, lanes(w)] = put.astype(BF16)
        return carry

    lax.fori_loop(*units, fix, 0)


def stacked(q_ref):
    return jnp.concatenate([q_ref[j] for j in range(q_ref.shape[0])], axis=0).astype(BF16)


def softmax_weights(q, keys, scores, beta):
    upper = lax.broadcasted_iota(jnp.int32, (q.shape[0], 1), 0) < q.shape[0] // 2

    def chunk(i, carry):
        at = lanes(i * CHUNK, CHUNK)
        s0 = jnp.dot(q, keys[0, :, at], preferred_element_type=F32)
        s1 = jnp.dot(q, keys[1, :, at], preferred_element_type=F32)
        part = jnp.where(upper, s0, s1) * (q.shape[1] ** -0.5)
        if beta is not None:
            part = jnp.where(lax.broadcasted_iota(jnp.int32, (1, part.shape[1]), 1) + i * CHUNK * UNIT <= beta, part, -1e30)
        scores[:, at] = part
        return carry

    lax.fori_loop(0, keys.shape[-1] // (CHUNK * UNIT), chunk, 0)
    top = scores[...].max(axis=-1, keepdims=True)
    expd = jnp.exp(scores[...] - top)
    return (expd / expd.sum(axis=-1, keepdims=True)).astype(BF16)


def mix_and_project(weights, values, copy, wo, mlp, out):
    rows = weights.shape[0]
    dim = values.shape[1]
    upper = lax.broadcasted_iota(jnp.int32, (rows, 1), 0) < rows // 2
    dims = (((1,), (1,)), ((), ()))

    def chunk(i, carry):
        at = lanes(i * CHUNK, CHUNK)
        return tuple(carry[h] + lax.dot_general(weights[:, at], values[h, :, at], dims, preferred_element_type=F32) for h in range(2))

    m0, m1 = lax.fori_loop(0, values.shape[-1] // (CHUNK * UNIT), chunk, (jnp.zeros((rows, dim), F32),) * 2)
    copy.start()
    mixed = jnp.where(upper, m0, m1).astype(BF16).astype(F32)
    flat = jnp.concatenate([mixed[j:j + 1] for j in range(rows)], axis=1)
    flat = jnp.broadcast_to(flat, (8, flat.shape[1])).astype(BF16)

    def project(i, carry):
        at = lanes(i * 4, 4)
        out[:, at] = jnp.dot(flat, wo[:, at], preferred_element_type=F32)[0:1] + mlp[:, at]
        return carry

    lax.fori_loop(0, out.shape[1] // (4 * UNIT), project, 0)


def window_body(layer, size, half, n_pipe, ids, q_ref, new_ref, mlp_ref, wo_hbm, k_own, v_own, k_near, v_near, *refs):
    pipe = refs[:n_pipe]
    k_out, v_out = refs[n_pipe + 3:n_pipe + 5]
    part_ref = refs[n_pipe + 2]
    kv, edge, wo, scores, weights, sems, out_sems, wo_sem = refs[n_pipe + 5:]
    me = ids[0]
    core = lax.rem(me, 2)
    second = me // 2 == 1
    beta = ids[1 + me] - WINDOW
    last = beta // UNIT
    first, count = crossing(beta, second, 2 * half)
    direct = size is None
    over = 0 if direct else jnp.maximum(count - size, 0)
    cut = 0 if direct else size - half

    def fetch(w, low, part, dst, sem):
        high = jnp.logical_and(w <= last, jnp.logical_not(low))
        crosses = jnp.logical_xor(high, second)
        at = lanes(lax.rem(w, half))
        local = w // half == core
        idx = jnp.clip(w - first, 0, 2 * half - 1)
        stay = jnp.logical_not(crosses)

        @pl.when(jnp.logical_and(stay, local))
        def _():
            move([((k_own, v_own)[part].at[layer, me, :, :, at], dst, sem)])

        @pl.when(jnp.logical_and(stay, jnp.logical_not(local)))
        def _():
            move([((k_near, v_near)[part].at[layer, me, :, :, at], dst, sem)])

        if direct:
            for here, ref in ((local, pipe[2 * part]), (jnp.logical_not(local), pipe[2 * part + 1])):
                @pl.when(jnp.logical_and(crosses, here))
                def _(ref=ref):
                    move([(ref.at[:, :, at], dst, sem)])
            return

        @pl.when(jnp.logical_and(crosses, jnp.logical_and(idx >= cut, idx < size)))
        def _():
            move([(pipe[0].at[part, :, :, lanes(idx - cut)], dst, sem)])

        if cut:
            @pl.when(jnp.logical_and(crosses, idx < cut))
            def _():
                move([(pipe[1].at[part, :, :, lanes(idx)], dst, sem)])

        if size < 2 * half:
            @pl.when(jnp.logical_and(crosses, idx >= size))
            def _():
                move([(pipe[-1].at[part, :, :, lanes(jnp.clip(half - over + idx - size, 0, half - 1))], dst, sem)])

    wo_copy = pltpu.make_async_copy(wo_hbm.at[layer], wo, wo_sem)
    for part in range(2):
        def issue(w, carry, part=part):
            fetch(w, False, part, kv.at[part, :, :, lanes(w)], sems.at[part])
            return carry

        lax.fori_loop(0, 2 * half, issue, 0)
        fetch(last, True, part, edge.at[part], sems.at[part])
    wo_copy.start()

    def ready(part):
        pltpu.make_async_copy(kv.at[part], kv.at[part], sems.at[part]).wait()
        pltpu.make_async_copy(edge.at[part], edge.at[part], sems.at[part]).wait()
        settle(kv.at[part], new_ref[part], beta, lambda old: edge[part].astype(F32), (last, last + 1))

    ready(0)
    weights[...] = softmax_weights(stacked(q_ref), kv.at[0], scores, None)
    k_copy = pltpu.make_async_copy(kv.at[0], k_out.at[layer], out_sems.at[0])
    k_copy.start()
    ready(1)
    wo_copy.wait()
    v_copy = pltpu.make_async_copy(kv.at[1], v_out.at[layer], out_sems.at[1])
    mix_and_project(weights, kv.at[1], v_copy, wo, mlp_ref, part_ref)
    k_copy.wait()
    v_copy.wait()


def attend_window(layer, size, ids, q, new_kv, mlp, w_out, k_t, v_t, nears, pipe, k_buf, v_buf):
    heads, dim, shard = k_t.shape[2:]
    half = shard // UNIT
    n_pipe = len(pipe)
    return pl.pallas_call(
        functools.partial(window_body, layer, size, half, n_pipe),
        in_specs=[SMEM, VMEM, VMEM, VMEM] + [HBM] * (5 + n_pipe + 2),
        out_specs=[VMEM, HBM, HBM],
        out_shape=[jax.ShapeDtypeStruct(mlp.shape, F32), jax.ShapeDtypeStruct(k_buf.shape, BF16), jax.ShapeDtypeStruct(v_buf.shape, BF16)],
        scratch_shapes=[
            pltpu.VMEM((2, heads, dim, 2 * shard), BF16),
            pltpu.VMEM((2, heads, dim, UNIT), BF16),
            pltpu.VMEM(w_out.shape[1:], BF16),
            pltpu.VMEM((q.shape[0] * q.shape[1], 2 * shard), F32),
            pltpu.VMEM((q.shape[0] * q.shape[1], 2 * shard), BF16),
            pltpu.SemaphoreType.DMA((2,)),
            pltpu.SemaphoreType.DMA((2,)),
            pltpu.SemaphoreType.DMA,
        ],
        input_output_aliases={9 + n_pipe: 1, 10 + n_pipe: 2},
        cost_estimate=cost(16 * heads * dim * shard),
        name="attend_window",
    )(ids, q, new_kv, mlp, w_out, k_t, v_t, *nears, *pipe, k_buf, v_buf)


def fetch_row(layer, me, own, blocks, kv, sem):
    shard = own.shape[-1]
    for relation in range(4):
        at = pl.ds(pl.multiple_of(jnp.bitwise_xor(me, relation) * shard, UNIT), shard)
        src = (own, blocks[0])[relation].at[layer, me] if relation < 2 else blocks[relation - 1]
        move([(src, kv.at[:, :, at], sem)])


def scores_body(layer, ids, q_ref, new_ref, own, b1, b2, b3, w_ref, k_out, kv, sem, out_sem, scores):
    me = ids[0]
    length = ids[1 + me]
    fetch_row(layer, me, own, (b1, b2, b3), kv, sem)
    pltpu.make_async_copy(kv, kv, sem).wait()
    settle(kv, new_ref[0], length, jnp.zeros_like, (length // UNIT, kv.shape[-1] // UNIT))
    w_ref[...] = softmax_weights(stacked(q_ref), kv, scores, length)
    copy = pltpu.make_async_copy(kv, k_out, out_sem)
    copy.start()
    copy.wait()


def values_body(layer, ids, w_ref, new_ref, mlp_ref, wo_hbm, own, b1, b2, b3, part_ref, v_out, kv, wo, sem, out_sem, wo_sem):
    me = ids[0]
    length = ids[1 + me]
    fetch_row(layer, me, own, (b1, b2, b3), kv, sem)
    wo_copy = pltpu.make_async_copy(wo_hbm.at[layer], wo, wo_sem)
    wo_copy.start()
    pltpu.make_async_copy(kv, kv, sem).wait()
    settle(kv, new_ref[1], length, jnp.zeros_like, (length // UNIT, kv.shape[-1] // UNIT))
    wo_copy.wait()
    copy = pltpu.make_async_copy(kv, v_out, out_sem)
    mix_and_project(w_ref, kv, copy, wo, mlp_ref, part_ref)
    copy.wait()


def attend_global(layer, ids, q, new_kv, mlp, w_out, k_t, v_t, k_blocks, v_blocks):
    heads, dim, shard = k_t.shape[2:]
    row = jax.ShapeDtypeStruct((heads, dim, 4 * shard), BF16)
    scratch = [pltpu.VMEM(row.shape, BF16), pltpu.SemaphoreType.DMA, pltpu.SemaphoreType.DMA]
    n_q = q.shape[0] * q.shape[1]
    weights, k_glob = pl.pallas_call(
        functools.partial(scores_body, layer),
        in_specs=[SMEM, VMEM, VMEM] + [HBM] * 4,
        out_specs=[VMEM, HBM],
        out_shape=[jax.ShapeDtypeStruct((n_q, 4 * shard), BF16), row],
        scratch_shapes=scratch + [pltpu.VMEM((n_q, 4 * shard), F32)],
        cost_estimate=cost(16 * heads * dim * shard),
        name="scores",
    )(ids, q, new_kv, k_t, *k_blocks)
    part, v_glob = pl.pallas_call(
        functools.partial(values_body, layer),
        in_specs=[SMEM, VMEM, VMEM, VMEM] + [HBM] * 5,
        out_specs=[VMEM, HBM],
        out_shape=[jax.ShapeDtypeStruct(mlp.shape, F32), row],
        scratch_shapes=scratch[:1] + [pltpu.VMEM(w_out.shape[1:], BF16)] + [pltpu.SemaphoreType.DMA] * 3,
        cost_estimate=cost(16 * heads * dim * shard),
        name="values",
    )(ids, weights, new_kv, mlp, w_out, v_t, *v_blocks)
    return part, k_glob, v_glob


def summed(tp, residual, parts):
    total = residual.astype(F32)
    for t in range(4):
        at = jnp.bitwise_xor(tp, t)
        pick = parts[3][...]
        for r in range(3):
            pick = jnp.where(at == r, parts[r][...], pick)
        total = pick if t == 0 else total + pick
    return (residual.astype(F32) + total).astype(BF16)


def front_body(layer, dim, n_parts, tp_ref, h_ref, *refs):
    parts, (gain, cosine, sine, wq, wk, wv, wg, wu, wd, h_out, q_out, new_out, mlp_out, u, acc) = refs[:n_parts], refs[n_parts:]
    step = pl.program_id(0)

    def turn(proj):
        if cosine is None:
            return proj
        width = proj.shape[1]
        lane = lax.broadcasted_iota(jnp.int32, proj.shape, 1)
        ahead = pltpu.roll(proj, width - dim // 2, 1)
        behind = pltpu.roll(proj, dim // 2, 1)
        swapped = jnp.where(lax.rem(lane, dim) < dim // 2, -ahead, behind)
        return proj * cosine[...] + swapped * sine[...]

    def over_rows(mats):
        depth = 8 * UNIT

        def block(i, sums):
            rows = lanes(i * 8, 8)
            return tuple(t + jnp.dot(u[:, rows], m[0, rows, :], preferred_element_type=F32) for t, m in zip(sums, mats))

        return lax.fori_loop(0, u.shape[1] // depth, block, tuple(jnp.zeros((u.shape[0], m.shape[2]), F32) for m in mats))

    def rounded(proj):
        return proj.astype(BF16).astype(F32)

    @pl.when(step == 0)
    def _():
        h = summed(tp_ref[0], h_ref[...], parts) if n_parts else h_ref[...]
        h_out[...] = h
        rows32 = h.astype(F32)
        centered = rows32 - rows32.mean(axis=-1, keepdims=True)
        variance = (centered * centered).mean(axis=-1, keepdims=True)
        scaled = centered * lax.rsqrt(variance + NORM_EPS) * gain[...].astype(F32)[layer:layer + 1]
        u[...] = jnp.broadcast_to(scaled, u.shape).astype(BF16)
        acc[...] = jnp.zeros_like(acc)
        both = over_rows((wk, wv))
        key_new, value_new = rounded(turn(both[0])), rounded(both[1])
        for part, new in ((0, key_new), (1, value_new)):
            for head in range(new_out.shape[1]):
                new_out[part, head:head + 1, :] = new[0:1, head * dim:(head + 1) * dim]

    query, gate, up = over_rows((wq, wg, wu))
    query = rounded(turn(query))
    for head in range(q_out.shape[1]):
        q_out[0, head:head + 1, :] = query[0:1, head * dim:(head + 1) * dim]
    active = (jax.nn.silu(gate) * up).astype(BF16)

    def down(i, carry):
        at = lanes(i * 8, 8)
        acc[:, at] += jnp.dot(active, wd[0, :, at], preferred_element_type=F32)
        return carry

    lax.fori_loop(0, acc.shape[1] // (8 * UNIT), down, 0)

    @pl.when(step == FFN_STEPS - 1)
    def _():
        mlp_out[...] = acc[0:1, :]


def plain_front_body(layer, dim, n_parts, tp_ref, h_ref, *refs):
    front_body(layer, dim, n_parts, tp_ref, h_ref, *refs[:n_parts + 1], None, None, *refs[n_parts + 1:])


def front(layer, dim, tp, residual, parts, ln_gain, turns, w_query, w_key, w_value, w_gate, w_up, w_down):
    width = residual.shape[1]
    q_width, kv_width, ffn = w_query.shape[2], w_key.shape[2], w_gate.shape[2]
    q_step, ffn_step = q_width // FFN_STEPS, ffn // FFN_STEPS
    whole = lambda *shape: pl.BlockSpec(shape, lambda j: (0,) * len(shape))
    col = lambda rows, cols: pl.BlockSpec((1, rows, cols), lambda j: (layer, 0, j))
    fixed = lambda rows, cols: pl.BlockSpec((1, rows, cols), lambda j: (layer, 0, 0))
    n_parts = len(parts)
    body = front_body if turns else plain_front_body
    return pl.pallas_call(
        functools.partial(body, layer, dim, n_parts),
        grid=(FFN_STEPS,),
        in_specs=[SMEM, whole(1, width)] + [whole(1, width)] * n_parts + [whole(*ln_gain.shape)] + [whole(1, kv_width)] * len(turns)
        + [col(width, q_step), fixed(width, kv_width), fixed(width, kv_width), col(width, ffn_step), col(width, ffn_step), pl.BlockSpec((1, ffn_step, width), lambda j: (layer, j, 0))],
        out_specs=[whole(1, width), pl.BlockSpec((1, q_step // dim, dim), lambda j: (j, 0, 0)), whole(2, kv_width // dim, dim), whole(1, width)],
        out_shape=[
            jax.ShapeDtypeStruct((1, width), BF16),
            jax.ShapeDtypeStruct((FFN_STEPS, q_step // dim, dim), F32),
            jax.ShapeDtypeStruct((2, kv_width // dim, dim), F32),
            jax.ShapeDtypeStruct((1, width), F32),
        ],
        scratch_shapes=[pltpu.VMEM((8, width), BF16), pltpu.VMEM((8, width), F32)],
        compiler_params=pltpu.CompilerParams(dimension_semantics=("arbitrary",)),
        cost_estimate=cost(2 * width * (q_width + 2 * kv_width + 3 * ffn)),
        name="front",
    )(tp, residual, *parts, ln_gain, *turns, w_query, w_key, w_value, w_gate, w_up, w_down)


def close_body(tp_ref, h_ref, p0, p1, p2, p3, out_ref):
    out_ref[...] = summed(tp_ref[0], h_ref[...], (p0, p1, p2, p3))


def close(tp, residual, parts):
    return pl.pallas_call(
        close_body,
        in_specs=[SMEM] + [VMEM] * 5,
        out_specs=VMEM,
        out_shape=jax.ShapeDtypeStruct(residual.shape, BF16),
        name="close",
    )(tp, residual, *parts)


def fresh_body(*refs):
    pass


def fresh_buffers(shapes):
    return pl.pallas_call(fresh_body, out_specs=[HBM] * len(shapes), out_shape=[jax.ShapeDtypeStruct(s, BF16) for s in shapes], name="fresh")()


def solution(mesh):
    cache_spec = P(None, "dp", "tp", "sp", None)
    row_spec = P(("dp", "sp"), None)
    col_spec = P(None, None, "tp")
    inner_spec = P(None, "tp", None)
    window_spec = P(None, ("dp", "sp"), "tp", None, None)
    global_spec = P(("dp", "sp"), "tp", None, None)
    in_specs = (cache_spec, cache_spec, P("dp"), row_spec, P(None, None), col_spec, col_spec, col_spec, inner_spec, col_spec, col_spec, inner_spec)
    out_specs = (row_spec, window_spec, window_spec, global_spec, global_spec)
    n_sp, n_tp = mesh.shape["sp"], mesh.shape["tp"]

    def swap(t, axis, relation):
        return lax.ppermute(t, axis, [(i, i ^ relation) for i in range(n_sp if axis == "sp" else n_tp)])

    def device_step(k_cache, v_cache, lengths, hidden, ln_gain, w_query, w_key, w_value, w_out, w_gate, w_up, w_down):
        n_layers = w_query.shape[0]
        heads, shard, dim = k_cache.shape[2:]
        half = shard // UNIT
        final = n_layers - 1
        me = lax.axis_index("sp").astype(jnp.int32)
        tp = lax.axis_index("tp").astype(jnp.int32)[None]
        ids = jnp.concatenate([me[None], lengths])
        k_t = jnp.swapaxes(k_cache, 3, 4)
        v_t = jnp.swapaxes(v_cache, 3, 4)

        inv_freq = 1.0 / (ROPE_BASE ** (jnp.arange(dim // 2, dtype=F32) * 2.0 / dim))
        angles = lax.dynamic_slice_in_dim(lengths, me, 1).astype(F32)[:, None] * inv_freq[None, :]
        repeat = 2 * w_key.shape[2] // dim
        turns = (jnp.tile(jnp.cos(angles), (1, repeat)), jnp.tile(jnp.sin(angles), (1, repeat)))

        _, counts = crossing(lengths - WINDOW, jnp.arange(n_sp) >= n_sp // 2, 2 * half)
        need = lax.pmax(jnp.max((counts.reshape(2, -1).sum(axis=1) + 1) // 2), "dp")
        choice = sum((need > size).astype(jnp.int32) for size in SIZES[:-1])

        def block(t, layer, relation):
            return lax.dynamic_slice(t, (layer, jnp.bitwise_xor(me, relation), 0, 0, 0), (1, 1, heads, dim, shard))[0, 0]

        weights = (w_query, w_key, w_value, w_gate, w_up, w_down)
        k_first = [swap(block(k_t, 0, r), "sp", r) for r in (2, 3)]
        nears = [swap(k_t, "sp", 1), swap(v_t, "sp", 1)]
        begun = front(0, dim, tp, hidden, (), ln_gain, turns, *weights)

        def run(size):
            return run_scoped(size)

        def run_scoped(size):
            k_win, v_win = fresh_buffers([(final, heads, dim, WINDOW)] * 2)
            pipes = [k_first + [swap(block(v_t, 0, r), "sp", r) for r in (2, 3)]]
            for layer in range(1, final):
                packed = pack(layer, size, ids, k_t, v_t, nears)
                pipes.append([swap(p, "sp", 2) for p in packed])
            residual, q, new_kv, mlp = begun
            for layer in range(n_layers):
                sliding = layer < final
                if layer:
                    residual, q, new_kv, mlp = front(layer, dim, tp, residual, parts, ln_gain, turns if sliding else (), *weights)
                if layer == 1:
                    cuts = after([block(t, final, r) for t in (k_t, v_t) for r in (2, 3)], q)
                    late = [swap(c, "sp", 2 + i % 2) for i, c in enumerate(cuts)]
                if sliding:
                    if layer and size < 2 * half:
                        pipes[layer].append(swap(after(pipes[layer][0], q), "sp", 1))
                    part, k_win, v_win = attend_window(layer, size if layer else None, ids, q, new_kv, mlp, w_out, k_t, v_t, nears, pipes[layer], k_win, v_win)
                else:
                    part, k_glob, v_glob = attend_global(layer, ids, q, new_kv, mlp, w_out, k_t, v_t, [nears[0]] + late[:2], [nears[1]] + late[2:])
                parts = (part,) + tuple(swap(part, "tp", r) for r in (1, 2, 3))
            return close(tp, residual, parts), k_win, v_win, k_glob, v_glob

        if len(SIZES) == 1:
            out, k_win, v_win, k_glob, v_glob = run(SIZES[0])
        else:
            out, k_win, v_win, k_glob, v_glob = lax.switch(choice, [functools.partial(run, size) for size in SIZES])
        back = lambda t: jnp.swapaxes(t, -1, -2)
        return out, back(k_win)[:, None], back(v_win)[:, None], back(k_glob)[None], back(v_glob)[None]


    return jax.shard_map(device_step, mesh=mesh, in_specs=in_specs, out_specs=out_specs, check_vma=False)
```

```python
import functools

import jax
import jax.numpy as jnp
from jax import lax
from jax.experimental import pallas as pl
from jax.experimental.pallas import tpu as pltpu
from jax.sharding import PartitionSpec as P


WINDOW = 4096
ROPE_BASE = 50000
NORM_EPS = 1e-5
UNIT = 128
SIZES = (18, 23, 28, 32)
FFN_STEPS = 4
CHUNK = 16
HBM = pl.BlockSpec(memory_space=pltpu.HBM)
VMEM = pl.BlockSpec(memory_space=pltpu.VMEM)
SMEM = pl.BlockSpec(memory_space=pltpu.SMEM)
F32 = jnp.float32
BF16 = jnp.bfloat16


def cost(n_bytes):
    return pl.CostEstimate(flops=n_bytes, bytes_accessed=n_bytes, transcendentals=0)


def lanes(block, count=1):
    return pl.ds(pl.multiple_of(block * UNIT, UNIT), count * UNIT)


def crossing(beta, on_second_chip, n_units):
    above = (beta + 1) // UNIT
    below = (beta + UNIT - 1) // UNIT
    return jnp.where(on_second_chip, above, 0), jnp.where(on_second_chip, n_units - above, below)


def move(pairs):
    for src, dst, sem in pairs:
        pltpu.make_async_copy(src, dst, sem).start()


def pack_body(layer, size, half, ids, k_own, v_own, k_near, v_near, *refs):
    outs, (buf, sem, out_sem) = refs[:-3], refs[-3:]
    me = ids[0]
    core = lax.rem(me, 2)
    base = (1 - me // 2) * 2
    second = base == 2
    row, other = base + core, base + 1 - core
    first, count = crossing(ids[1 + row] - WINDOW, second, 2 * half)
    other_first, other_count = crossing(ids[1 + other] - WINDOW, second, 2 * half)
    over = jnp.maximum(other_count - size, 0)

    def issue(i, carry):
        mine = i < count
        dest = jnp.where(mine, row, other)
        unit = jnp.where(mine, first + i, other_first + size + i - (size - over))
        unit = jnp.clip(unit, 0, 2 * half - 1)
        at = lanes(lax.rem(unit, half))
        local = unit // half == core

        @pl.when(local)
        def _():
            move([(k_own.at[layer, dest, :, :, at], buf.at[0, :, :, lanes(i)], sem), (v_own.at[layer, dest, :, :, at], buf.at[1, :, :, lanes(i)], sem)])

        @pl.when(jnp.logical_not(local))
        def _():
            move([(near.at[layer, dest, :, :, at], buf.at[p, :, :, lanes(i)], sem) for p, near in enumerate((k_near, v_near))])

        return carry

    lax.fori_loop(0, size, issue, 0)
    pltpu.make_async_copy(buf, buf, sem).wait()
    cut = size - half
    copies = [pltpu.make_async_copy(buf.at[:, :, :, cut * UNIT:], outs[0], out_sem)]
    if cut:
        copies.append(pltpu.make_async_copy(buf.at[:, :, :, :cut * UNIT], outs[1], out_sem))
    for copy in copies:
        copy.start()
    for copy in copies:
        copy.wait()


def pack(layer, size, ids, k_t, v_t, nears):
    heads, dim, shard = k_t.shape[2:]
    half = shard // UNIT
    widths = [half] + ([size - half] if size > half else [])
    return pl.pallas_call(
        functools.partial(pack_body, layer, size, half),
        in_specs=[SMEM] + [HBM] * 4,
        out_specs=[HBM] * len(widths),
        out_shape=[jax.ShapeDtypeStruct((2, heads, dim, w * UNIT), BF16) for w in widths],
        scratch_shapes=[pltpu.VMEM((2, heads, dim, size * UNIT), BF16), pltpu.SemaphoreType.DMA, pltpu.SemaphoreType.DMA],
        cost_estimate=cost(8 * heads * dim * size * UNIT),
        name="pack",
    )(ids, k_t, v_t, *nears)


def after(value, *others):
    return lax.optimization_barrier((value, others))[0]


def settle(kv, new_rows, beta, rest_of, units):
    fresh = new_rows[:, :, None]
    lane = lax.broadcasted_iota(jnp.int32, (1, 1, UNIT), 2)

    def fix(w, carry):
        pos = lane + w * UNIT
        old = kv[:, :, lanes(w)].astype(F32)
        put = jnp.where(pos < beta, old, jnp.where(pos == beta, fresh, rest_of(old)))
        kv[:, :, lanes(w)] = put.astype(BF16)
        return carry

    lax.fori_loop(*units, fix, 0)


def stacked(q_ref):
    return jnp.concatenate([q_ref[j] for j in range(q_ref.shape[0])], axis=0).astype(BF16)


def softmax_weights(q, keys, scores, beta):
    upper = lax.broadcasted_iota(jnp.int32, (q.shape[0], 1), 0) < q.shape[0] // 2

    def chunk(i, carry):
        at = lanes(i * CHUNK, CHUNK)
        s0 = jnp.dot(q, keys[0, :, at], preferred_element_type=F32)
        s1 = jnp.dot(q, keys[1, :, at], preferred_element_type=F32)
        part = jnp.where(upper, s0, s1) * (q.shape[1] ** -0.5)
        if beta is not None:
            part = jnp.where(lax.broadcasted_iota(jnp.int32, (1, part.shape[1]), 1) + i * CHUNK * UNIT <= beta, part, -1e30)
        scores[:, at] = part
        return carry

    lax.fori_loop(0, keys.shape[-1] // (CHUNK * UNIT), chunk, 0)
    top = scores[...].max(axis=-1, keepdims=True)
    expd = jnp.exp(scores[...] - top)
    return (expd / expd.sum(axis=-1, keepdims=True)).astype(BF16)


def mix_and_project(weights, values, copy, wo, mlp, out):
    rows = weights.shape[0]
    dim = values.shape[1]
    upper = lax.broadcasted_iota(jnp.int32, (rows, 1), 0) < rows // 2
    dims = (((1,), (1,)), ((), ()))

    def chunk(i, carry):
        at = lanes(i * CHUNK, CHUNK)
        return tuple(carry[h] + lax.dot_general(weights[:, at], values[h, :, at], dims, preferred_element_type=F32) for h in range(2))

    m0, m1 = lax.fori_loop(0, values.shape[-1] // (CHUNK * UNIT), chunk, (jnp.zeros((rows, dim), F32),) * 2)
    copy.start()
    mixed = jnp.where(upper, m0, m1).astype(BF16).astype(F32)
    flat = jnp.concatenate([mixed[j:j + 1] for j in range(rows)], axis=1)
    flat = jnp.broadcast_to(flat, (8, flat.shape[1])).astype(BF16)

    def project(i, carry):
        at = lanes(i * 4, 4)
        out[:, at] = jnp.dot(flat, wo[:, at], preferred_element_type=F32)[0:1] + mlp[:, at]
        return carry

    lax.fori_loop(0, out.shape[1] // (4 * UNIT), project, 0)


def window_body(layer, size, half, n_pipe, ids, q_ref, new_ref, mlp_ref, wo_hbm, k_own, v_own, k_near, v_near, *refs):
    pipe = refs[:n_pipe]
    k_out, v_out = refs[n_pipe + 3:n_pipe + 5]
    part_ref = refs[n_pipe + 2]
    kv, edge, wo, scores, weights, sems, out_sems, wo_sem = refs[n_pipe + 5:]
    me = ids[0]
    core = lax.rem(me, 2)
    second = me // 2 == 1
    beta = ids[1 + me] - WINDOW
    last = beta // UNIT
    first, count = crossing(beta, second, 2 * half)
    direct = size is None
    over = 0 if direct else jnp.maximum(count - size, 0)
    cut = 0 if direct else size - half

    def fetch(w, low, part, dst, sem):
        high = jnp.logical_and(w <= last, jnp.logical_not(low))
        crosses = jnp.logical_xor(high, second)
        at = lanes(lax.rem(w, half))
        local = w // half == core
        idx = jnp.clip(w - first, 0, 2 * half - 1)
        stay = jnp.logical_not(crosses)

        @pl.when(jnp.logical_and(stay, local))
        def _():
            move([((k_own, v_own)[part].at[layer, me, :, :, at], dst, sem)])

        @pl.when(jnp.logical_and(stay, jnp.logical_not(local)))
        def _():
            move([((k_near, v_near)[part].at[layer, me, :, :, at], dst, sem)])

        if direct:
            for here, ref in ((local, pipe[2 * part]), (jnp.logical_not(local), pipe[2 * part + 1])):
                @pl.when(jnp.logical_and(crosses, here))
                def _(ref=ref):
                    move([(ref.at[:, :, at], dst, sem)])
            return

        @pl.when(jnp.logical_and(crosses, jnp.logical_and(idx >= cut, idx < size)))
        def _():
            move([(pipe[0].at[part, :, :, lanes(idx - cut)], dst, sem)])

        if cut:
            @pl.when(jnp.logical_and(crosses, idx < cut))
            def _():
                move([(pipe[1].at[part, :, :, lanes(idx)], dst, sem)])

        if size < 2 * half:
            @pl.when(jnp.logical_and(crosses, idx >= size))
            def _():
                move([(pipe[-1].at[part, :, :, lanes(jnp.clip(half - over + idx - size, 0, half - 1))], dst, sem)])

    wo_copy = pltpu.make_async_copy(wo_hbm.at[layer], wo, wo_sem)
    for part in range(2):
        def issue(w, carry, part=part):
            fetch(w, False, part, kv.at[part, :, :, lanes(w)], sems.at[part])
            return carry

        lax.fori_loop(0, 2 * half, issue, 0)
        fetch(last, True, part, edge.at[part], sems.at[part])
    wo_copy.start()

    def ready(part):
        pltpu.make_async_copy(kv.at[part], kv.at[part], sems.at[part]).wait()
        pltpu.make_async_copy(edge.at[part], edge.at[part], sems.at[part]).wait()
        settle(kv.at[part], new_ref[part], beta, lambda old: edge[part].astype(F32), (last, last + 1))

    ready(0)
    weights[...] = softmax_weights(stacked(q_ref), kv.at[0], scores, None)
    k_copy = pltpu.make_async_copy(kv.at[0], k_out.at[layer], out_sems.at[0])
    k_copy.start()
    ready(1)
    wo_copy.wait()
    v_copy = pltpu.make_async_copy(kv.at[1], v_out.at[layer], out_sems.at[1])
    mix_and_project(weights, kv.at[1], v_copy, wo, mlp_ref, part_ref)
    k_copy.wait()
    v_copy.wait()


def attend_window(layer, size, ids, q, new_kv, mlp, w_out, k_t, v_t, nears, pipe, k_buf, v_buf):
    heads, dim, shard = k_t.shape[2:]
    half = shard // UNIT
    n_pipe = len(pipe)
    return pl.pallas_call(
        functools.partial(window_body, layer, size, half, n_pipe),
        in_specs=[SMEM, VMEM, VMEM, VMEM] + [HBM] * (5 + n_pipe + 2),
        out_specs=[VMEM, HBM, HBM],
        out_shape=[jax.ShapeDtypeStruct(mlp.shape, F32), jax.ShapeDtypeStruct(k_buf.shape, BF16), jax.ShapeDtypeStruct(v_buf.shape, BF16)],
        scratch_shapes=[
            pltpu.VMEM((2, heads, dim, 2 * shard), BF16),
            pltpu.VMEM((2, heads, dim, UNIT), BF16),
            pltpu.VMEM(w_out.shape[1:], BF16),
            pltpu.VMEM((q.shape[0] * q.shape[1], 2 * shard), F32),
            pltpu.VMEM((q.shape[0] * q.shape[1], 2 * shard), BF16),
            pltpu.SemaphoreType.DMA((2,)),
            pltpu.SemaphoreType.DMA((2,)),
            pltpu.SemaphoreType.DMA,
        ],
        input_output_aliases={9 + n_pipe: 1, 10 + n_pipe: 2},
        cost_estimate=cost(16 * heads * dim * shard),
        name="attend_window",
    )(ids, q, new_kv, mlp, w_out, k_t, v_t, *nears, *pipe, k_buf, v_buf)


def fetch_row(layer, me, own, blocks, kv, sem):
    shard = own.shape[-1]
    for relation in range(4):
        at = pl.ds(pl.multiple_of(jnp.bitwise_xor(me, relation) * shard, UNIT), shard)
        src = (own, blocks[0])[relation].at[layer, me] if relation < 2 else blocks[relation - 1]
        move([(src, kv.at[:, :, at], sem)])


def scores_body(layer, ids, q_ref, new_ref, own, b1, b2, b3, w_ref, k_out, kv, sem, out_sem, scores):
    me = ids[0]
    length = ids[1 + me]
    fetch_row(layer, me, own, (b1, b2, b3), kv, sem)
    pltpu.make_async_copy(kv, kv, sem).wait()
    settle(kv, new_ref[0], length, jnp.zeros_like, (length // UNIT, kv.shape[-1] // UNIT))
    w_ref[...] = softmax_weights(stacked(q_ref), kv, scores, length)
    copy = pltpu.make_async_copy(kv, k_out, out_sem)
    copy.start()
    copy.wait()


def values_body(layer, ids, w_ref, new_ref, mlp_ref, wo_hbm, own, b1, b2, b3, part_ref, v_out, kv, wo, sem, out_sem, wo_sem):
    me = ids[0]
    length = ids[1 + me]
    fetch_row(layer, me, own, (b1, b2, b3), kv, sem)
    wo_copy = pltpu.make_async_copy(wo_hbm.at[layer], wo, wo_sem)
    wo_copy.start()
    pltpu.make_async_copy(kv, kv, sem).wait()
    settle(kv, new_ref[1], length, jnp.zeros_like, (length // UNIT, kv.shape[-1] // UNIT))
    wo_copy.wait()
    copy = pltpu.make_async_copy(kv, v_out, out_sem)
    mix_and_project(w_ref, kv, copy, wo, mlp_ref, part_ref)
    copy.wait()


def attend_global(layer, ids, q, new_kv, mlp, w_out, k_t, v_t, k_blocks, v_blocks):
    heads, dim, shard = k_t.shape[2:]
    row = jax.ShapeDtypeStruct((heads, dim, 4 * shard), BF16)
    scratch = [pltpu.VMEM(row.shape, BF16), pltpu.SemaphoreType.DMA, pltpu.SemaphoreType.DMA]
    n_q = q.shape[0] * q.shape[1]
    weights, k_glob = pl.pallas_call(
        functools.partial(scores_body, layer),
        in_specs=[SMEM, VMEM, VMEM] + [HBM] * 4,
        out_specs=[VMEM, HBM],
        out_shape=[jax.ShapeDtypeStruct((n_q, 4 * shard), BF16), row],
        scratch_shapes=scratch + [pltpu.VMEM((n_q, 4 * shard), F32)],
        cost_estimate=cost(16 * heads * dim * shard),
        name="scores",
    )(ids, q, new_kv, k_t, *k_blocks)
    part, v_glob = pl.pallas_call(
        functools.partial(values_body, layer),
        in_specs=[SMEM, VMEM, VMEM, VMEM] + [HBM] * 5,
        out_specs=[VMEM, HBM],
        out_shape=[jax.ShapeDtypeStruct(mlp.shape, F32), row],
        scratch_shapes=scratch[:1] + [pltpu.VMEM(w_out.shape[1:], BF16)] + [pltpu.SemaphoreType.DMA] * 3,
        cost_estimate=cost(16 * heads * dim * shard),
        name="values",
    )(ids, weights, new_kv, mlp, w_out, v_t, *v_blocks)
    return part, k_glob, v_glob


def tp_sum_body(part_ref, h_ref, out_ref, slots, send_sems, recv_sems):
    tp = lax.axis_index("tp")
    barrier = pltpu.get_barrier_semaphore()
    peers = [{"tp": jnp.bitwise_xor(tp, r)} for r in (1, 2, 3)]
    for peer in peers:
        pl.semaphore_signal(barrier, inc=1, device_id=peer, device_id_type=pl.DeviceIdType.MESH)
    pl.semaphore_wait(barrier, 3)
    copies = [
        pltpu.make_async_remote_copy(part_ref, slots.at[i], send_sems.at[i], recv_sems.at[i], device_id=peer, device_id_type=pl.DeviceIdType.MESH)
        for i, peer in enumerate(peers)
    ]
    for copy in copies:
        copy.start()
    for copy in copies:
        copy.wait()
    parts = [part_ref[...]] + [slots[i] for i in range(3)]
    for t in range(4):
        at = jnp.bitwise_xor(tp, t)
        pick = parts[3]
        for r in range(3):
            pick = jnp.where(at == r, parts[r], pick)
        total = pick if t == 0 else total + pick
    out_ref[...] = (h_ref[...].astype(F32) + total).astype(BF16)


def tp_sum(layer, part, residual):
    return pl.pallas_call(
        tp_sum_body,
        in_specs=[VMEM, VMEM],
        out_specs=VMEM,
        out_shape=jax.ShapeDtypeStruct(residual.shape, BF16),
        scratch_shapes=[pltpu.VMEM((3,) + part.shape, F32), pltpu.SemaphoreType.DMA((3,)), pltpu.SemaphoreType.DMA((3,))],
        compiler_params=pltpu.CompilerParams(collective_id=layer, has_side_effects=True),
        cost_estimate=cost(12 * part.size),
        name="tp_sum",
    )(part, residual)


def front_body(layer, dim, h_ref, gain, cosine, sine, wq, wk, wv, wg, wu, wd, q_out, new_out, mlp_out, u, acc):
    step = pl.program_id(0)

    def turn(proj):
        if cosine is None:
            return proj
        width = proj.shape[1]
        lane = lax.broadcasted_iota(jnp.int32, proj.shape, 1)
        ahead = pltpu.roll(proj, width - dim // 2, 1)
        behind = pltpu.roll(proj, dim // 2, 1)
        swapped = jnp.where(lax.rem(lane, dim) < dim // 2, -ahead, behind)
        return proj * cosine[...] + swapped * sine[...]

    def over_rows(mats):
        depth = 8 * UNIT

        def block(i, sums):
            rows = lanes(i * 8, 8)
            return tuple(t + jnp.dot(u[:, rows], m[0, rows, :], preferred_element_type=F32) for t, m in zip(sums, mats))

        return lax.fori_loop(0, u.shape[1] // depth, block, tuple(jnp.zeros((u.shape[0], m.shape[2]), F32) for m in mats))

    def rounded(proj):
        return proj.astype(BF16).astype(F32)

    @pl.when(step == 0)
    def _():
        rows32 = h_ref[...].astype(F32)
        centered = rows32 - rows32.mean(axis=-1, keepdims=True)
        variance = (centered * centered).mean(axis=-1, keepdims=True)
        scaled = centered * lax.rsqrt(variance + NORM_EPS) * gain[...].astype(F32)[layer:layer + 1]
        u[...] = jnp.broadcast_to(scaled, u.shape).astype(BF16)
        acc[...] = jnp.zeros_like(acc)
        both = over_rows((wk, wv))
        key_new, value_new = rounded(turn(both[0])), rounded(both[1])
        for part, new in ((0, key_new), (1, value_new)):
            for head in range(new_out.shape[1]):
                new_out[part, head:head + 1, :] = new[0:1, head * dim:(head + 1) * dim]

    query, gate, up = over_rows((wq, wg, wu))
    query = rounded(turn(query))
    for head in range(q_out.shape[1]):
        q_out[0, head:head + 1, :] = query[0:1, head * dim:(head + 1) * dim]
    active = (jax.nn.silu(gate) * up).astype(BF16)

    def down(i, carry):
        at = lanes(i * 8, 8)
        acc[:, at] += jnp.dot(active, wd[0, :, at], preferred_element_type=F32)
        return carry

    lax.fori_loop(0, acc.shape[1] // (8 * UNIT), down, 0)

    @pl.when(step == FFN_STEPS - 1)
    def _():
        mlp_out[...] = acc[0:1, :]


def plain_front_body(layer, dim, h_ref, gain, *refs):
    front_body(layer, dim, h_ref, gain, None, None, *refs)


def front(layer, dim, residual, ln_gain, turns, w_query, w_key, w_value, w_gate, w_up, w_down):
    width = residual.shape[1]
    q_width, kv_width, ffn = w_query.shape[2], w_key.shape[2], w_gate.shape[2]
    q_step, ffn_step = q_width // FFN_STEPS, ffn // FFN_STEPS
    whole = lambda *shape: pl.BlockSpec(shape, lambda j: (0,) * len(shape))
    col = lambda rows, cols: pl.BlockSpec((1, rows, cols), lambda j: (layer, 0, j))
    fixed = lambda rows, cols: pl.BlockSpec((1, rows, cols), lambda j: (layer, 0, 0))
    body = front_body if turns else plain_front_body
    return pl.pallas_call(
        functools.partial(body, layer, dim),
        grid=(FFN_STEPS,),
        in_specs=[whole(1, width), whole(*ln_gain.shape)] + [whole(1, kv_width)] * len(turns)
        + [col(width, q_step), fixed(width, kv_width), fixed(width, kv_width), col(width, ffn_step), col(width, ffn_step), pl.BlockSpec((1, ffn_step, width), lambda j: (layer, j, 0))],
        out_specs=[pl.BlockSpec((1, q_step // dim, dim), lambda j: (j, 0, 0)), whole(2, kv_width // dim, dim), whole(1, width)],
        out_shape=[
            jax.ShapeDtypeStruct((FFN_STEPS, q_step // dim, dim), F32),
            jax.ShapeDtypeStruct((2, kv_width // dim, dim), F32),
            jax.ShapeDtypeStruct((1, width), F32),
        ],
        scratch_shapes=[pltpu.VMEM((8, width), BF16), pltpu.VMEM((8, width), F32)],
        compiler_params=pltpu.CompilerParams(dimension_semantics=("arbitrary",)),
        cost_estimate=cost(2 * width * (q_width + 2 * kv_width + 3 * ffn)),
        name="front",
    )(residual, ln_gain, *turns, w_query, w_key, w_value, w_gate, w_up, w_down)


def fresh_body(*refs):
    pass


def fresh_buffers(shapes):
    return pl.pallas_call(fresh_body, out_specs=[HBM] * len(shapes), out_shape=[jax.ShapeDtypeStruct(s, BF16) for s in shapes], name="fresh")()


def solution(mesh):
    cache_spec = P(None, "dp", "tp", "sp", None)
    row_spec = P(("dp", "sp"), None)
    col_spec = P(None, None, "tp")
    inner_spec = P(None, "tp", None)
    window_spec = P(None, ("dp", "sp"), "tp", None, None)
    global_spec = P(("dp", "sp"), "tp", None, None)
    in_specs = (cache_spec, cache_spec, P("dp"), row_spec, P(None, None), col_spec, col_spec, col_spec, inner_spec, col_spec, col_spec, inner_spec)
    out_specs = (row_spec, window_spec, window_spec, global_spec, global_spec)
    n_sp = mesh.shape["sp"]

    def swap(t, axis, relation):
        return lax.ppermute(t, axis, [(i, i ^ relation) for i in range(n_sp)])

    def device_step(k_cache, v_cache, lengths, hidden, ln_gain, w_query, w_key, w_value, w_out, w_gate, w_up, w_down):
        n_layers = w_query.shape[0]
        heads, shard, dim = k_cache.shape[2:]
        half = shard // UNIT
        final = n_layers - 1
        me = lax.axis_index("sp").astype(jnp.int32)
        ids = jnp.concatenate([me[None], lengths])
        k_t = jnp.swapaxes(k_cache, 3, 4)
        v_t = jnp.swapaxes(v_cache, 3, 4)

        inv_freq = 1.0 / (ROPE_BASE ** (jnp.arange(dim // 2, dtype=F32) * 2.0 / dim))
        angles = lax.dynamic_slice_in_dim(lengths, me, 1).astype(F32)[:, None] * inv_freq[None, :]
        repeat = 2 * w_key.shape[2] // dim
        turns = (jnp.tile(jnp.cos(angles), (1, repeat)), jnp.tile(jnp.sin(angles), (1, repeat)))

        _, counts = crossing(lengths - WINDOW, jnp.arange(n_sp) >= n_sp // 2, 2 * half)
        need = lax.pmax(jnp.max((counts.reshape(2, -1).sum(axis=1) + 1) // 2), "dp")
        choice = sum((need > size).astype(jnp.int32) for size in SIZES[:-1])

        def block(t, layer, relation):
            return lax.dynamic_slice(t, (layer, jnp.bitwise_xor(me, relation), 0, 0, 0), (1, 1, heads, dim, shard))[0, 0]

        weights = (w_query, w_key, w_value, w_gate, w_up, w_down)
        k_first = [swap(block(k_t, 0, r), "sp", r) for r in (2, 3)]
        v_far = swap(block(v_t, 0, 2), "sp", 2)
        nears = [swap(k_t, "sp", 1), swap(v_t, "sp", 1)]
        begun = front(0, dim, hidden, ln_gain, turns, *weights)

        def run(size):
            return run_scoped(size)

        def run_scoped(size):
            k_win, v_win = fresh_buffers([(final, heads, dim, WINDOW)] * 2)
            pipes = [k_first + [v_far, swap(block(v_t, 0, 3), "sp", 3)]]
            for layer in range(1, final):
                packed = pack(layer, size, ids, k_t, v_t, nears)
                pipes.append([swap(p, "sp", 2) for p in packed])
            residual, (q, new_kv, mlp) = hidden, begun
            for layer in range(n_layers):
                sliding = layer < final
                if layer:
                    q, new_kv, mlp = front(layer, dim, residual, ln_gain, turns if sliding else (), *weights)
                if layer == 1:
                    cuts = after([block(t, final, r) for t in (k_t, v_t) for r in (2, 3)], q)
                    late = [swap(c, "sp", 2 + i % 2) for i, c in enumerate(cuts)]
                if sliding:
                    if layer and size < 2 * half:
                        pipes[layer].append(swap(after(pipes[layer][0], q), "sp", 1))
                    part, k_win, v_win = attend_window(layer, size if layer else None, ids, q, new_kv, mlp, w_out, k_t, v_t, nears, pipes[layer], k_win, v_win)
                else:
                    part, k_glob, v_glob = attend_global(layer, ids, q, new_kv, mlp, w_out, k_t, v_t, [nears[0]] + late[:2], [nears[1]] + late[2:])
                residual = tp_sum(layer, part, residual)
            return residual, k_win, v_win, k_glob, v_glob

        if len(SIZES) == 1:
            out, k_win, v_win, k_glob, v_glob = run(SIZES[0])
        else:
            out, k_win, v_win, k_glob, v_glob = lax.switch(choice, [functools.partial(run, size) for size in SIZES])
        back = lambda t: jnp.swapaxes(t, -1, -2)
        return out, back(k_win)[:, None], back(v_win)[:, None], back(k_glob)[None], back(v_glob)[None]


    return jax.shard_map(device_step, mesh=mesh, in_specs=in_specs, out_specs=out_specs, check_vma=False)
```

```python
import functools

import jax
import jax.numpy as jnp
from jax import lax
from jax.experimental import pallas as pl
from jax.experimental.pallas import tpu as pltpu
from jax.sharding import PartitionSpec as P


WINDOW = 4096
ROPE_BASE = 50000
NORM_EPS = 1e-5
UNIT = 128
SIZES = (18, 23, 28, 32)
FFN_STEPS = 4
PEERS = (1, 2, 3)
CHUNK = 16
HBM = pl.BlockSpec(memory_space=pltpu.HBM)
VMEM = pl.BlockSpec(memory_space=pltpu.VMEM)
SMEM = pl.BlockSpec(memory_space=pltpu.SMEM)
F32 = jnp.float32
BF16 = jnp.bfloat16


def cost(n_bytes):
    return pl.CostEstimate(flops=n_bytes, bytes_accessed=n_bytes, transcendentals=0)


def lanes(block, count=1):
    return pl.ds(pl.multiple_of(block * UNIT, UNIT), count * UNIT)


def crossing(beta, on_second_chip, n_units):
    above = (beta + 1) // UNIT
    below = (beta + UNIT - 1) // UNIT
    return jnp.where(on_second_chip, above, 0), jnp.where(on_second_chip, n_units - above, below)


def move(pairs):
    for src, dst, sem in pairs:
        pltpu.make_async_copy(src, dst, sem).start()


def pack_body(layer, size, half, ids, k_own, v_own, k_near, v_near, *refs):
    outs, (buf, sem, out_sem) = refs[:-3], refs[-3:]
    me = ids[0]
    core = lax.rem(me, 2)
    base = (1 - me // 2) * 2
    second = base == 2
    row, other = base + core, base + 1 - core
    first, count = crossing(ids[1 + row] - WINDOW, second, 2 * half)
    other_first, other_count = crossing(ids[1 + other] - WINDOW, second, 2 * half)
    over = jnp.maximum(other_count - size, 0)

    def issue(i, carry):
        mine = i < count
        dest = jnp.where(mine, row, other)
        unit = jnp.where(mine, first + i, other_first + size + i - (size - over))
        unit = jnp.clip(unit, 0, 2 * half - 1)
        at = lanes(lax.rem(unit, half))
        local = unit // half == core

        @pl.when(local)
        def _():
            move([(k_own.at[layer, dest, :, :, at], buf.at[0, :, :, lanes(i)], sem), (v_own.at[layer, dest, :, :, at], buf.at[1, :, :, lanes(i)], sem)])

        @pl.when(jnp.logical_not(local))
        def _():
            move([(near.at[layer, dest, :, :, at], buf.at[p, :, :, lanes(i)], sem) for p, near in enumerate((k_near, v_near))])

        return carry

    lax.fori_loop(0, size, issue, 0)
    pltpu.make_async_copy(buf, buf, sem).wait()
    cut = size - half
    copies = [pltpu.make_async_copy(buf.at[:, :, :, cut * UNIT:], outs[0], out_sem)]
    if cut:
        copies.append(pltpu.make_async_copy(buf.at[:, :, :, :cut * UNIT], outs[1], out_sem))
    for copy in copies:
        copy.start()
    for copy in copies:
        copy.wait()


def pack(layer, size, ids, k_t, v_t, nears):
    heads, dim, shard = k_t.shape[2:]
    half = shard // UNIT
    widths = [half] + ([size - half] if size > half else [])
    return pl.pallas_call(
        functools.partial(pack_body, layer, size, half),
        in_specs=[SMEM] + [HBM] * 4,
        out_specs=[HBM] * len(widths),
        out_shape=[jax.ShapeDtypeStruct((2, heads, dim, w * UNIT), BF16) for w in widths],
        scratch_shapes=[pltpu.VMEM((2, heads, dim, size * UNIT), BF16), pltpu.SemaphoreType.DMA, pltpu.SemaphoreType.DMA],
        cost_estimate=cost(8 * heads * dim * size * UNIT),
        name="pack",
    )(ids, k_t, v_t, *nears)


def after(value, *others):
    return lax.optimization_barrier((value, others))[0]


def settle(kv, new_rows, beta, rest_of, units):
    fresh = new_rows[:, :, None]
    lane = lax.broadcasted_iota(jnp.int32, (1, 1, UNIT), 2)

    def fix(w, carry):
        pos = lane + w * UNIT
        old = kv[:, :, lanes(w)].astype(F32)
        put = jnp.where(pos < beta, old, jnp.where(pos == beta, fresh, rest_of(old)))
        kv[:, :, lanes(w)] = put.astype(BF16)
        return carry

    lax.fori_loop(*units, fix, 0)


def stacked(q_ref):
    return jnp.concatenate([q_ref[j] for j in range(q_ref.shape[0])], axis=0).astype(BF16)


def softmax_weights(q, keys, scores, beta):
    upper = lax.broadcasted_iota(jnp.int32, (q.shape[0], 1), 0) < q.shape[0] // 2

    def chunk(i, carry):
        at = lanes(i * CHUNK, CHUNK)
        s0 = jnp.dot(q, keys[0, :, at], preferred_element_type=F32)
        s1 = jnp.dot(q, keys[1, :, at], preferred_element_type=F32)
        part = jnp.where(upper, s0, s1) * (q.shape[1] ** -0.5)
        if beta is not None:
            part = jnp.where(lax.broadcasted_iota(jnp.int32, (1, part.shape[1]), 1) + i * CHUNK * UNIT <= beta, part, -1e30)
        scores[:, at] = part
        return carry

    lax.fori_loop(0, keys.shape[-1] // (CHUNK * UNIT), chunk, 0)
    top = scores[...].max(axis=-1, keepdims=True)
    expd = jnp.exp(scores[...] - top)
    return (expd / expd.sum(axis=-1, keepdims=True)).astype(BF16)


def mix_and_project(weights, values, copy, wo, mlp, out):
    rows = weights.shape[0]
    dim = values.shape[1]
    upper = lax.broadcasted_iota(jnp.int32, (rows, 1), 0) < rows // 2
    dims = (((1,), (1,)), ((), ()))

    def chunk(i, carry):
        at = lanes(i * CHUNK, CHUNK)
        return tuple(carry[h] + lax.dot_general(weights[:, at], values[h, :, at], dims, preferred_element_type=F32) for h in range(2))

    m0, m1 = lax.fori_loop(0, values.shape[-1] // (CHUNK * UNIT), chunk, (jnp.zeros((rows, dim), F32),) * 2)
    copy.start()
    mixed = jnp.where(upper, m0, m1).astype(BF16).astype(F32)
    flat = jnp.concatenate([mixed[j:j + 1] for j in range(rows)], axis=1)
    flat = jnp.broadcast_to(flat, (8, flat.shape[1])).astype(BF16)

    def project(i, carry):
        at = lanes(i * 4, 4)
        out[:, at] = jnp.dot(flat, wo[:, at], preferred_element_type=F32)[0:1] + mlp[:, at]
        return carry

    lax.fori_loop(0, out.shape[1] // (4 * UNIT), project, 0)


def window_body(layer, size, half, n_pipe, ids, q_ref, new_ref, mlp_ref, wo_hbm, k_own, v_own, k_near, v_near, *refs):
    pipe = refs[:n_pipe]
    k_out, v_out = refs[n_pipe + 3:n_pipe + 5]
    part_ref = refs[n_pipe + 2]
    kv, edge, wo, scores, weights, sems, out_sems, wo_sem = refs[n_pipe + 5:]
    me = ids[0]
    core = lax.rem(me, 2)
    second = me // 2 == 1
    beta = ids[1 + me] - WINDOW
    last = beta // UNIT
    first, count = crossing(beta, second, 2 * half)
    direct = size is None
    over = 0 if direct else jnp.maximum(count - size, 0)
    cut = 0 if direct else size - half

    def fetch(w, low, part, dst, sem):
        high = jnp.logical_and(w <= last, jnp.logical_not(low))
        crosses = jnp.logical_xor(high, second)
        at = lanes(lax.rem(w, half))
        local = w // half == core
        idx = jnp.clip(w - first, 0, 2 * half - 1)
        stay = jnp.logical_not(crosses)

        @pl.when(jnp.logical_and(stay, local))
        def _():
            move([((k_own, v_own)[part].at[layer, me, :, :, at], dst, sem)])

        @pl.when(jnp.logical_and(stay, jnp.logical_not(local)))
        def _():
            move([((k_near, v_near)[part].at[layer, me, :, :, at], dst, sem)])

        if direct:
            for here, ref in ((local, pipe[2 * part]), (jnp.logical_not(local), pipe[2 * part + 1])):
                @pl.when(jnp.logical_and(crosses, here))
                def _(ref=ref):
                    move([(ref.at[:, :, at], dst, sem)])
            return

        @pl.when(jnp.logical_and(crosses, jnp.logical_and(idx >= cut, idx < size)))
        def _():
            move([(pipe[0].at[part, :, :, lanes(idx - cut)], dst, sem)])

        if cut:
            @pl.when(jnp.logical_and(crosses, idx < cut))
            def _():
                move([(pipe[1].at[part, :, :, lanes(idx)], dst, sem)])

        if size < 2 * half:
            @pl.when(jnp.logical_and(crosses, idx >= size))
            def _():
                move([(pipe[-1].at[part, :, :, lanes(jnp.clip(half - over + idx - size, 0, half - 1))], dst, sem)])

    wo_copy = pltpu.make_async_copy(wo_hbm.at[layer], wo, wo_sem)
    for part in range(2):
        def issue(w, carry, part=part):
            fetch(w, False, part, kv.at[part, :, :, lanes(w)], sems.at[part])
            return carry

        lax.fori_loop(0, 2 * half, issue, 0)
        fetch(last, True, part, edge.at[part], sems.at[part])
    wo_copy.start()

    def ready(part):
        pltpu.make_async_copy(kv.at[part], kv.at[part], sems.at[part]).wait()
        pltpu.make_async_copy(edge.at[part], edge.at[part], sems.at[part]).wait()
        settle(kv.at[part], new_ref[part], beta, lambda old: edge[part].astype(F32), (last, last + 1))

    ready(0)
    weights[...] = softmax_weights(stacked(q_ref), kv.at[0], scores, None)
    k_copy = pltpu.make_async_copy(kv.at[0], k_out.at[layer], out_sems.at[0])
    k_copy.start()
    ready(1)
    wo_copy.wait()
    v_copy = pltpu.make_async_copy(kv.at[1], v_out.at[layer], out_sems.at[1])
    mix_and_project(weights, kv.at[1], v_copy, wo, mlp_ref, part_ref)
    k_copy.wait()
    v_copy.wait()


def attend_window(layer, size, ids, q, new_kv, mlp, w_out, k_t, v_t, nears, pipe, k_buf, v_buf):
    heads, dim, shard = k_t.shape[2:]
    half = shard // UNIT
    n_pipe = len(pipe)
    return pl.pallas_call(
        functools.partial(window_body, layer, size, half, n_pipe),
        in_specs=[SMEM, VMEM, VMEM, VMEM] + [HBM] * (5 + n_pipe + 2),
        out_specs=[VMEM, HBM, HBM],
        out_shape=[jax.ShapeDtypeStruct(mlp.shape, F32), jax.ShapeDtypeStruct(k_buf.shape, BF16), jax.ShapeDtypeStruct(v_buf.shape, BF16)],
        scratch_shapes=[
            pltpu.VMEM((2, heads, dim, 2 * shard), BF16),
            pltpu.VMEM((2, heads, dim, UNIT), BF16),
            pltpu.VMEM(w_out.shape[1:], BF16),
            pltpu.VMEM((q.shape[0] * q.shape[1], 2 * shard), F32),
            pltpu.VMEM((q.shape[0] * q.shape[1], 2 * shard), BF16),
            pltpu.SemaphoreType.DMA((2,)),
            pltpu.SemaphoreType.DMA((2,)),
            pltpu.SemaphoreType.DMA,
        ],
        input_output_aliases={9 + n_pipe: 1, 10 + n_pipe: 2},
        cost_estimate=cost(16 * heads * dim * shard),
        name="attend_window",
    )(ids, q, new_kv, mlp, w_out, k_t, v_t, *nears, *pipe, k_buf, v_buf)


def place_body(layer, part, relations, ids, new_ref, own, near, *refs):
    blocks = {1: near}
    blocks.update(zip([r for r in relations if r > 1], refs))
    out, kv, sems, out_sem = refs[-4:]
    me = ids[0]
    length = ids[1 + me]
    shard = own.shape[-1]
    units = shard // UNIT
    spans = {r: pl.ds(pl.multiple_of(jnp.bitwise_xor(me, r) * shard, UNIT), shard) for r in relations}
    for i, r in enumerate(relations):
        src = (own, near)[r].at[layer, me] if r < 2 else blocks[r]
        move([(src, kv.at[:, :, spans[r]], sems.at[i])])
    stores = []
    for i, r in enumerate(relations):
        view = kv.at[:, :, spans[r]]
        pltpu.make_async_copy(view, view, sems.at[i]).wait()
        first = jnp.bitwise_xor(me, r) * units
        settle(kv, new_ref[part], length, jnp.zeros_like, (jnp.maximum(first, length // UNIT), first + units))
        stores.append(pltpu.make_async_copy(view, out.at[:, :, spans[r]], out_sem))
        stores[-1].start()
    for store in stores:
        store.wait()


def place(layer, part, relations, ids, new_kv, own, near, blocks, buf):
    heads, dim, shard = own.shape[2:]
    n_in = 4 + len(blocks)
    return pl.pallas_call(
        functools.partial(place_body, layer, part, relations),
        in_specs=[SMEM, VMEM] + [HBM] * (3 + len(blocks)),
        out_specs=HBM,
        out_shape=jax.ShapeDtypeStruct(buf.shape, BF16),
        scratch_shapes=[pltpu.VMEM(buf.shape, BF16), pltpu.SemaphoreType.DMA((len(relations),)), pltpu.SemaphoreType.DMA],
        input_output_aliases={n_in: 0},
        cost_estimate=cost(4 * heads * dim * shard * len(relations)),
        name="place",
    )(ids, new_kv, own, near, *blocks, buf)


def spread_body(layer, ids, q_ref, new_ref, mlp_ref, h_ref, wo_hbm, k_own, v_own, out_ref, k_all, v_all, wo, q_all, stats, mixes, part_ref, slots, expd, sems, send_sems, recv_sems):
    me = lax.axis_index("sp")
    tp = lax.axis_index("tp")
    barrier = pltpu.get_barrier_semaphore()
    sp_peers = [{"sp": jnp.bitwise_xor(me, r)} for r in PEERS]
    tp_peers = [{"tp": jnp.bitwise_xor(tp, r)} for r in PEERS]
    for peer in sp_peers + tp_peers:
        pl.semaphore_signal(barrier, inc=1, device_id=peer, device_id_type=pl.DeviceIdType.MESH)
    loads = [pltpu.make_async_copy(k_own.at[layer], k_all, sems.at[0]), pltpu.make_async_copy(v_own.at[layer], v_all, sems.at[1]), pltpu.make_async_copy(wo_hbm.at[layer], wo, sems.at[2])]
    for load in loads:
        load.start()

    def exchange(stage, peers, pairs):
        copies = [
            pltpu.make_async_remote_copy(src, dst, send_sems.at[stage, i], recv_sems.at[stage, i], device_id=peer, device_id_type=pl.DeviceIdType.MESH)
            for i, (peer, (src, dst)) in enumerate(zip(peers, pairs))
        ]
        for copy in copies:
            copy.start()
        return copies

    def done(copies):
        for copy in copies:
            copy.wait()

    pl.semaphore_wait(barrier, 6)
    queries = exchange(0, sp_peers, [(q_ref, q_all.at[i]) for i in range(3)])
    n_q = q_ref.shape[0] * q_ref.shape[1]
    dim = q_ref.shape[2]
    shard = k_all.shape[-1]
    upper = lax.broadcasted_iota(jnp.int32, (n_q, 1), 0) < n_q // 2
    lane = lax.broadcasted_iota(jnp.int32, (1, UNIT), 1)
    position = lax.broadcasted_iota(jnp.int32, (1, shard), 1) + me * shard
    q_own = jnp.concatenate([q_ref[j] for j in range(q_ref.shape[0])], axis=0)
    new_k = jnp.where(upper, new_ref[0, 0:1], new_ref[0, 1:2])
    new_v = jnp.where(upper, new_ref[1, 0:1], new_ref[1, 1:2])
    new_score = (q_own * new_k).sum(axis=-1, keepdims=True) * (dim ** -0.5)

    def score(r):
        row = jnp.bitwise_xor(me, r)
        q = q_own if r == 0 else jnp.concatenate([q_all[r - 1, j] for j in range(q_ref.shape[0])], axis=0)
        q = q.astype(BF16)
        s0 = jnp.dot(q, k_all[row, 0], preferred_element_type=F32)
        s1 = jnp.dot(q, k_all[row, 1], preferred_element_type=F32)
        scores = jnp.where(position < ids[1 + row], jnp.where(upper, s0, s1) * (dim ** -0.5), -1e30)
        top = scores.max(axis=-1, keepdims=True)
        e = jnp.exp(scores - top)
        expd[r] = e
        stats[0, r] = jnp.where(lane == 0, top, jnp.where(lane == 1, e.sum(axis=-1, keepdims=True), new_score))

    loads[0].wait()
    score(0)
    done(queries)
    for r in PEERS:
        score(r)
    done(exchange(1, sp_peers, [(stats.at[0], stats.at[r]) for r in PEERS]))
    loads[1].wait()
    dims = (((1,), (1,)), ((), ()))
    for r in (1, 2, 3, 0):
        row = jnp.bitwise_xor(me, r)
        seen = [stats[other, other ^ r] for other in range(4)]
        fresh = stats[r, 0][:, 2:3]
        top = fresh
        for one in seen:
            top = jnp.maximum(top, one[:, 0:1])
        total = jnp.exp(fresh - top)
        for one in seen:
            total = total + one[:, 1:2] * jnp.exp(one[:, 0:1] - top)
        weights = (expd[r] * (jnp.exp(stats[0, r][:, 0:1] - top) / total)).astype(BF16)
        m0 = lax.dot_general(weights, v_all[row, 0], dims, preferred_element_type=F32)
        m1 = lax.dot_general(weights, v_all[row, 1], dims, preferred_element_type=F32)
        mixed = jnp.where(upper, m0, m1)
        if r == 0:
            mixed = mixed + (jnp.exp(fresh - top) / total).astype(BF16).astype(F32) * new_v
        mixes[0, r] = mixed
    done(exchange(2, sp_peers, [(mixes.at[0, r], mixes.at[1, r]) for r in PEERS]))
    mixed = mixes[0, 0] + mixes[1, 1] + mixes[1, 2] + mixes[1, 3]
    mixed = mixed.astype(BF16).astype(F32)
    flat = jnp.concatenate([mixed[j:j + 1] for j in range(n_q)], axis=1)
    flat = jnp.broadcast_to(flat, (8, flat.shape[1])).astype(BF16)
    loads[2].wait()
    part_ref[...] = jnp.dot(flat, wo[...], preferred_element_type=F32)[0:1] + mlp_ref[...]
    done(exchange(3, tp_peers, [(part_ref, slots.at[i]) for i in range(3)]))
    out_ref[...] = in_tp_order(tp, [part_ref[...]] + [slots[i] for i in range(3)], h_ref[...])


def spread(layer, ids, q, new_kv, mlp, residual, w_out, k_t, v_t):
    rows, heads, dim, shard = k_t.shape[1:]
    n_q = q.shape[0] * q.shape[1]
    return pl.pallas_call(
        functools.partial(spread_body, layer),
        in_specs=[SMEM, VMEM, VMEM, VMEM, VMEM, HBM, HBM, HBM],
        out_specs=VMEM,
        out_shape=jax.ShapeDtypeStruct(residual.shape, BF16),
        scratch_shapes=[
            pltpu.VMEM((rows, heads, dim, shard), BF16),
            pltpu.VMEM((rows, heads, dim, shard), BF16),
            pltpu.VMEM(w_out.shape[1:], BF16),
            pltpu.VMEM((3,) + q.shape, F32),
            pltpu.VMEM((4, 4, n_q, UNIT), F32),
            pltpu.VMEM((2, 4, n_q, dim), F32),
            pltpu.VMEM(mlp.shape, F32),
            pltpu.VMEM((3,) + mlp.shape, F32),
            pltpu.VMEM((4, n_q, shard), F32),
            pltpu.SemaphoreType.DMA((3,)),
            pltpu.SemaphoreType.DMA((4, 3)),
            pltpu.SemaphoreType.DMA((4, 3)),
        ],
        compiler_params=pltpu.CompilerParams(collective_id=layer, has_side_effects=True),
        cost_estimate=cost(16 * heads * dim * shard),
        name="spread",
    )(ids, q, new_kv, mlp, residual, w_out, k_t, v_t)


def in_tp_order(tp, parts, residual):
    for t in range(4):
        at = jnp.bitwise_xor(tp, t)
        pick = parts[3]
        for r in range(3):
            pick = jnp.where(at == r, parts[r], pick)
        total = pick if t == 0 else total + pick
    return (residual.astype(F32) + total).astype(BF16)


def tp_sum_body(part_ref, h_ref, out_ref, slots, send_sems, recv_sems):
    tp = lax.axis_index("tp")
    barrier = pltpu.get_barrier_semaphore()
    peers = [{"tp": jnp.bitwise_xor(tp, r)} for r in PEERS]
    for peer in peers:
        pl.semaphore_signal(barrier, inc=1, device_id=peer, device_id_type=pl.DeviceIdType.MESH)
    pl.semaphore_wait(barrier, 3)
    copies = [
        pltpu.make_async_remote_copy(part_ref, slots.at[i], send_sems.at[i], recv_sems.at[i], device_id=peer, device_id_type=pl.DeviceIdType.MESH)
        for i, peer in enumerate(peers)
    ]
    for copy in copies:
        copy.start()
    for copy in copies:
        copy.wait()
    out_ref[...] = in_tp_order(tp, [part_ref[...]] + [slots[i] for i in range(3)], h_ref[...])


def tp_sum(layer, part, residual):
    return pl.pallas_call(
        tp_sum_body,
        in_specs=[VMEM, VMEM],
        out_specs=VMEM,
        out_shape=jax.ShapeDtypeStruct(residual.shape, BF16),
        scratch_shapes=[pltpu.VMEM((3,) + part.shape, F32), pltpu.SemaphoreType.DMA((3,)), pltpu.SemaphoreType.DMA((3,))],
        compiler_params=pltpu.CompilerParams(collective_id=layer, has_side_effects=True),
        cost_estimate=cost(12 * part.size),
        name="tp_sum",
    )(part, residual)


def front_body(layer, dim, h_ref, gain, cosine, sine, wq, wk, wv, wg, wu, wd, q_out, new_out, mlp_out, u, acc):
    step = pl.program_id(0)

    def turn(proj):
        if cosine is None:
            return proj
        width = proj.shape[1]
        lane = lax.broadcasted_iota(jnp.int32, proj.shape, 1)
        ahead = pltpu.roll(proj, width - dim // 2, 1)
        behind = pltpu.roll(proj, dim // 2, 1)
        swapped = jnp.where(lax.rem(lane, dim) < dim // 2, -ahead, behind)
        return proj * cosine[...] + swapped * sine[...]

    def over_rows(mats):
        depth = 8 * UNIT

        def block(i, sums):
            rows = lanes(i * 8, 8)
            return tuple(t + jnp.dot(u[:, rows], m[0, rows, :], preferred_element_type=F32) for t, m in zip(sums, mats))

        return lax.fori_loop(0, u.shape[1] // depth, block, tuple(jnp.zeros((u.shape[0], m.shape[2]), F32) for m in mats))

    def rounded(proj):
        return proj.astype(BF16).astype(F32)

    @pl.when(step == 0)
    def _():
        rows32 = h_ref[...].astype(F32)
        centered = rows32 - rows32.mean(axis=-1, keepdims=True)
        variance = (centered * centered).mean(axis=-1, keepdims=True)
        scaled = centered * lax.rsqrt(variance + NORM_EPS) * gain[...].astype(F32)[layer:layer + 1]
        u[...] = jnp.broadcast_to(scaled, u.shape).astype(BF16)
        acc[...] = jnp.zeros_like(acc)
        both = over_rows((wk, wv))
        key_new, value_new = rounded(turn(both[0])), rounded(both[1])
        for part, new in ((0, key_new), (1, value_new)):
            for head in range(new_out.shape[1]):
                new_out[part, head:head + 1, :] = new[0:1, head * dim:(head + 1) * dim]

    query, gate, up = over_rows((wq, wg, wu))
    query = rounded(turn(query))
    for head in range(q_out.shape[1]):
        q_out[0, head:head + 1, :] = query[0:1, head * dim:(head + 1) * dim]
    active = (jax.nn.silu(gate) * up).astype(BF16)

    def down(i, carry):
        at = lanes(i * 8, 8)
        acc[:, at] += jnp.dot(active, wd[0, :, at], preferred_element_type=F32)
        return carry

    lax.fori_loop(0, acc.shape[1] // (8 * UNIT), down, 0)

    @pl.when(step == FFN_STEPS - 1)
    def _():
        mlp_out[...] = acc[0:1, :]


def plain_front_body(layer, dim, h_ref, gain, *refs):
    front_body(layer, dim, h_ref, gain, None, None, *refs)


def front(layer, dim, residual, ln_gain, turns, w_query, w_key, w_value, w_gate, w_up, w_down):
    width = residual.shape[1]
    q_width, kv_width, ffn = w_query.shape[2], w_key.shape[2], w_gate.shape[2]
    q_step, ffn_step = q_width // FFN_STEPS, ffn // FFN_STEPS
    whole = lambda *shape: pl.BlockSpec(shape, lambda j: (0,) * len(shape))
    col = lambda rows, cols: pl.BlockSpec((1, rows, cols), lambda j: (layer, 0, j))
    fixed = lambda rows, cols: pl.BlockSpec((1, rows, cols), lambda j: (layer, 0, 0))
    body = front_body if turns else plain_front_body
    return pl.pallas_call(
        functools.partial(body, layer, dim),
        grid=(FFN_STEPS,),
        in_specs=[whole(1, width), whole(*ln_gain.shape)] + [whole(1, kv_width)] * len(turns)
        + [col(width, q_step), fixed(width, kv_width), fixed(width, kv_width), col(width, ffn_step), col(width, ffn_step), pl.BlockSpec((1, ffn_step, width), lambda j: (layer, j, 0))],
        out_specs=[pl.BlockSpec((1, q_step // dim, dim), lambda j: (j, 0, 0)), whole(2, kv_width // dim, dim), whole(1, width)],
        out_shape=[
            jax.ShapeDtypeStruct((FFN_STEPS, q_step // dim, dim), F32),
            jax.ShapeDtypeStruct((2, kv_width // dim, dim), F32),
            jax.ShapeDtypeStruct((1, width), F32),
        ],
        scratch_shapes=[pltpu.VMEM((8, width), BF16), pltpu.VMEM((8, width), F32)],
        compiler_params=pltpu.CompilerParams(dimension_semantics=("arbitrary",)),
        cost_estimate=cost(2 * width * (q_width + 2 * kv_width + 3 * ffn)),
        name="front",
    )(residual, ln_gain, *turns, w_query, w_key, w_value, w_gate, w_up, w_down)


def fresh_body(*refs):
    pass


def fresh_buffers(shapes):
    return pl.pallas_call(fresh_body, out_specs=[HBM] * len(shapes), out_shape=[jax.ShapeDtypeStruct(s, BF16) for s in shapes], name="fresh")()


def solution(mesh):
    cache_spec = P(None, "dp", "tp", "sp", None)
    row_spec = P(("dp", "sp"), None)
    col_spec = P(None, None, "tp")
    inner_spec = P(None, "tp", None)
    window_spec = P(None, ("dp", "sp"), "tp", None, None)
    global_spec = P(("dp", "sp"), "tp", None, None)
    in_specs = (cache_spec, cache_spec, P("dp"), row_spec, P(None, None), col_spec, col_spec, col_spec, inner_spec, col_spec, col_spec, inner_spec)
    out_specs = (row_spec, window_spec, window_spec, global_spec, global_spec)
    n_sp = mesh.shape["sp"]

    def swap(t, axis, relation):
        return lax.ppermute(t, axis, [(i, i ^ relation) for i in range(n_sp)])

    def device_step(k_cache, v_cache, lengths, hidden, ln_gain, w_query, w_key, w_value, w_out, w_gate, w_up, w_down):
        n_layers = w_query.shape[0]
        heads, shard, dim = k_cache.shape[2:]
        half = shard // UNIT
        final = n_layers - 1
        me = lax.axis_index("sp").astype(jnp.int32)
        ids = jnp.concatenate([me[None], lengths])
        k_t = jnp.swapaxes(k_cache, 3, 4)
        v_t = jnp.swapaxes(v_cache, 3, 4)

        inv_freq = 1.0 / (ROPE_BASE ** (jnp.arange(dim // 2, dtype=F32) * 2.0 / dim))
        angles = lax.dynamic_slice_in_dim(lengths, me, 1).astype(F32)[:, None] * inv_freq[None, :]
        repeat = 2 * w_key.shape[2] // dim
        turns = (jnp.tile(jnp.cos(angles), (1, repeat)), jnp.tile(jnp.sin(angles), (1, repeat)))

        _, counts = crossing(lengths - WINDOW, jnp.arange(n_sp) >= n_sp // 2, 2 * half)
        need = lax.pmax(jnp.max((counts.reshape(2, -1).sum(axis=1) + 1) // 2), "dp")
        choice = sum((need > size).astype(jnp.int32) for size in SIZES[:-1])

        def block(t, layer, relation):
            return lax.dynamic_slice(t, (layer, jnp.bitwise_xor(me, relation), 0, 0, 0), (1, 1, heads, dim, shard))[0, 0]

        weights = (w_query, w_key, w_value, w_gate, w_up, w_down)
        k_first = [swap(block(k_t, 0, r), "sp", r) for r in (2, 3)]
        v_far = swap(block(v_t, 0, 2), "sp", 2)
        v_cut = block(v_t, 0, 3)
        nears = [swap(k_t, "sp", 1), swap(v_t, "sp", 1)]
        begun = front(0, dim, hidden, ln_gain, turns, *weights)

        def run(size):
            return run_scoped(size)

        def run_scoped(size, ids=ids):
            k_win, v_win = fresh_buffers([(final, heads, dim, WINDOW)] * 2)
            pipes = [k_first + [v_far, swap(v_cut, "sp", 3)]]
            for layer in range(1, final):
                packed = pack(layer, size, ids, k_t, v_t, nears)
                pipes.append([swap(p, "sp", 2) for p in packed])
            residual, (q, new_kv, mlp) = hidden, begun
            for layer in range(n_layers):
                sliding = layer < final
                if layer:
                    q, new_kv, mlp = front(layer, dim, residual, ln_gain, turns if sliding else (), *weights)
                if layer == 1:
                    cuts = after([block(t, final, r) for t in (k_t, v_t) for r in (2, 3)], q)
                    late = [swap(c, "sp", 2 + i % 2) for i, c in enumerate(cuts)]
                if sliding:
                    if layer and size < 2 * half:
                        pipes[layer].append(swap(after(pipes[layer][0], q), "sp", 1))
                    part, k_win, v_win = attend_window(layer, size if layer else None, ids, q, new_kv, mlp, w_out, k_t, v_t, nears, pipes[layer], k_win, v_win)
                    residual = tp_sum(layer, part, residual)
                else:
                    k_glob, v_glob = fresh_buffers([(heads, dim, n_sp * shard)] * 2)
                    residual = spread(layer, ids, q, new_kv, mlp, residual, w_out, k_t, v_t)
                    k_glob = place(final, 0, (0,) + PEERS, ids, new_kv, k_t, nears[0], late[:2], k_glob)
                    ids = after(ids, k_glob)
                    v_glob = place(final, 1, (0, 1, 2), ids, new_kv, v_t, nears[1], late[2:3], v_glob)
                    v_glob = place(final, 1, (3,), ids, new_kv, v_t, nears[1], late[3:], v_glob)
            return residual, k_win, v_win, k_glob, v_glob

        if len(SIZES) == 1:
            out, k_win, v_win, k_glob, v_glob = run(SIZES[0])
        else:
            out, k_win, v_win, k_glob, v_glob = lax.switch(choice, [functools.partial(run, size) for size in SIZES])
        back = lambda t: jnp.swapaxes(t, -1, -2)
        return out, back(k_win)[:, None], back(v_win)[:, None], back(k_glob)[None], back(v_glob)[None]


    return jax.shard_map(device_step, mesh=mesh, in_specs=in_specs, out_specs=out_specs, check_vma=False)
```

```python
import functools

import jax
import jax.numpy as jnp
from jax import lax
from jax.experimental import pallas as pl
from jax.experimental.pallas import tpu as pltpu
from jax.sharding import PartitionSpec as P


WINDOW = 4096
ROPE_BASE = 50000
NORM_EPS = 1e-5
UNIT = 128
SIZES = (18, 23, 28, 32)
FFN_STEPS = 4
PEERS = (1, 2, 3)
CHUNK = 16
HBM = pl.BlockSpec(memory_space=pltpu.HBM)
VMEM = pl.BlockSpec(memory_space=pltpu.VMEM)
SMEM = pl.BlockSpec(memory_space=pltpu.SMEM)
F32 = jnp.float32
BF16 = jnp.bfloat16


def cost(n_bytes):
    return pl.CostEstimate(flops=n_bytes, bytes_accessed=n_bytes, transcendentals=0)


def lanes(block, count=1):
    return pl.ds(pl.multiple_of(block * UNIT, UNIT), count * UNIT)


def crossing(beta, on_second_chip, n_units):
    above = (beta + 1) // UNIT
    below = (beta + UNIT - 1) // UNIT
    return jnp.where(on_second_chip, above, 0), jnp.where(on_second_chip, n_units - above, below)


def move(pairs):
    for src, dst, sem in pairs:
        pltpu.make_async_copy(src, dst, sem).start()


def pack_body(layer, size, half, ids, k_own, v_own, k_near, v_near, *refs):
    outs, (buf, sem, out_sem) = refs[:-3], refs[-3:]
    me = ids[0]
    core = lax.rem(me, 2)
    base = (1 - me // 2) * 2
    second = base == 2
    row, other = base + core, base + 1 - core
    first, count = crossing(ids[1 + row] - WINDOW, second, 2 * half)
    other_first, other_count = crossing(ids[1 + other] - WINDOW, second, 2 * half)
    over = jnp.maximum(other_count - size, 0)

    def issue(i, carry):
        mine = i < count
        dest = jnp.where(mine, row, other)
        unit = jnp.where(mine, first + i, other_first + size + i - (size - over))
        unit = jnp.clip(unit, 0, 2 * half - 1)
        at = lanes(lax.rem(unit, half))
        local = unit // half == core

        @pl.when(local)
        def _():
            move([(k_own.at[layer, dest, :, :, at], buf.at[0, :, :, lanes(i)], sem), (v_own.at[layer, dest, :, :, at], buf.at[1, :, :, lanes(i)], sem)])

        @pl.when(jnp.logical_not(local))
        def _():
            move([(near.at[layer, dest, :, :, at], buf.at[p, :, :, lanes(i)], sem) for p, near in enumerate((k_near, v_near))])

        return carry

    lax.fori_loop(0, size, issue, 0)
    pltpu.make_async_copy(buf, buf, sem).wait()
    cut = size - half
    copies = [pltpu.make_async_copy(buf.at[:, :, :, cut * UNIT:], outs[0], out_sem)]
    if cut:
        copies.append(pltpu.make_async_copy(buf.at[:, :, :, :cut * UNIT], outs[1], out_sem))
    for copy in copies:
        copy.start()
    for copy in copies:
        copy.wait()


def pack(layer, size, ids, k_t, v_t, nears):
    heads, dim, shard = k_t.shape[2:]
    half = shard // UNIT
    widths = [half] + ([size - half] if size > half else [])
    return pl.pallas_call(
        functools.partial(pack_body, layer, size, half),
        in_specs=[SMEM] + [HBM] * 4,
        out_specs=[HBM] * len(widths),
        out_shape=[jax.ShapeDtypeStruct((2, heads, dim, w * UNIT), BF16) for w in widths],
        scratch_shapes=[pltpu.VMEM((2, heads, dim, size * UNIT), BF16), pltpu.SemaphoreType.DMA, pltpu.SemaphoreType.DMA],
        cost_estimate=cost(8 * heads * dim * size * UNIT),
        name="pack",
    )(ids, k_t, v_t, *nears)


def after(value, *others):
    return lax.optimization_barrier((value, others))[0]


def settle(kv, new_rows, beta, rest_of, units):
    fresh = new_rows[:, :, None]
    lane = lax.broadcasted_iota(jnp.int32, (1, 1, UNIT), 2)

    def fix(w, carry):
        pos = lane + w * UNIT
        old = kv[:, :, lanes(w)].astype(F32)
        put = jnp.where(pos < beta, old, jnp.where(pos == beta, fresh, rest_of(old)))
        kv[:, :, lanes(w)] = put.astype(BF16)
        return carry

    lax.fori_loop(*units, fix, 0)


def stacked(q_ref):
    return jnp.concatenate([q_ref[j] for j in range(q_ref.shape[0])], axis=0).astype(BF16)


def softmax_weights(q, keys, scores, beta):
    upper = lax.broadcasted_iota(jnp.int32, (q.shape[0], 1), 0) < q.shape[0] // 2

    def chunk(i, carry):
        at = lanes(i * CHUNK, CHUNK)
        s0 = jnp.dot(q, keys[0, :, at], preferred_element_type=F32)
        s1 = jnp.dot(q, keys[1, :, at], preferred_element_type=F32)
        part = jnp.where(upper, s0, s1) * (q.shape[1] ** -0.5)
        if beta is not None:
            part = jnp.where(lax.broadcasted_iota(jnp.int32, (1, part.shape[1]), 1) + i * CHUNK * UNIT <= beta, part, -1e30)
        scores[:, at] = part
        return carry

    lax.fori_loop(0, keys.shape[-1] // (CHUNK * UNIT), chunk, 0)
    top = scores[...].max(axis=-1, keepdims=True)
    expd = jnp.exp(scores[...] - top)
    return (expd / expd.sum(axis=-1, keepdims=True)).astype(BF16)


def mix_and_project(weights, values, copy, wo, mlp, out):
    rows = weights.shape[0]
    dim = values.shape[1]
    upper = lax.broadcasted_iota(jnp.int32, (rows, 1), 0) < rows // 2
    dims = (((1,), (1,)), ((), ()))

    def chunk(i, carry):
        at = lanes(i * CHUNK, CHUNK)
        return tuple(carry[h] + lax.dot_general(weights[:, at], values[h, :, at], dims, preferred_element_type=F32) for h in range(2))

    m0, m1 = lax.fori_loop(0, values.shape[-1] // (CHUNK * UNIT), chunk, (jnp.zeros((rows, dim), F32),) * 2)
    copy.start()
    mixed = jnp.where(upper, m0, m1).astype(BF16).astype(F32)
    flat = jnp.concatenate([mixed[j:j + 1] for j in range(rows)], axis=1)
    flat = jnp.broadcast_to(flat, (8, flat.shape[1])).astype(BF16)

    def project(i, carry):
        at = lanes(i * 4, 4)
        out[:, at] = jnp.dot(flat, wo[:, at], preferred_element_type=F32)[0:1] + mlp[:, at]
        return carry

    lax.fori_loop(0, out.shape[1] // (4 * UNIT), project, 0)


def window_body(layer, size, half, n_pipe, ids, q_ref, new_ref, mlp_ref, wo_hbm, k_own, v_own, k_near, v_near, *refs):
    pipe = refs[:n_pipe]
    k_out, v_out = refs[n_pipe + 3:n_pipe + 5]
    part_ref = refs[n_pipe + 2]
    kv, edge, wo, scores, weights, sems, out_sems, wo_sem = refs[n_pipe + 5:]
    me = ids[0]
    core = lax.rem(me, 2)
    second = me // 2 == 1
    beta = ids[1 + me] - WINDOW
    last = beta // UNIT
    first, count = crossing(beta, second, 2 * half)
    direct = size is None
    over = 0 if direct else jnp.maximum(count - size, 0)
    cut = 0 if direct else size - half

    def fetch(w, low, part, dst, sem):
        high = jnp.logical_and(w <= last, jnp.logical_not(low))
        crosses = jnp.logical_xor(high, second)
        at = lanes(lax.rem(w, half))
        local = w // half == core
        idx = jnp.clip(w - first, 0, 2 * half - 1)
        stay = jnp.logical_not(crosses)

        @pl.when(jnp.logical_and(stay, local))
        def _():
            move([((k_own, v_own)[part].at[layer, me, :, :, at], dst, sem)])

        @pl.when(jnp.logical_and(stay, jnp.logical_not(local)))
        def _():
            move([((k_near, v_near)[part].at[layer, me, :, :, at], dst, sem)])

        if direct:
            for here, ref in ((local, pipe[2 * part]), (jnp.logical_not(local), pipe[2 * part + 1])):
                @pl.when(jnp.logical_and(crosses, here))
                def _(ref=ref):
                    move([(ref.at[:, :, at], dst, sem)])
            return

        @pl.when(jnp.logical_and(crosses, jnp.logical_and(idx >= cut, idx < size)))
        def _():
            move([(pipe[0].at[part, :, :, lanes(idx - cut)], dst, sem)])

        if cut:
            @pl.when(jnp.logical_and(crosses, idx < cut))
            def _():
                move([(pipe[1].at[part, :, :, lanes(idx)], dst, sem)])

        if size < 2 * half:
            @pl.when(jnp.logical_and(crosses, idx >= size))
            def _():
                move([(pipe[-1].at[part, :, :, lanes(jnp.clip(half - over + idx - size, 0, half - 1))], dst, sem)])

    wo_copy = pltpu.make_async_copy(wo_hbm.at[layer], wo, wo_sem)
    for part in range(2):
        def issue(w, carry, part=part):
            fetch(w, False, part, kv.at[part, :, :, lanes(w)], sems.at[part])
            return carry

        lax.fori_loop(0, 2 * half, issue, 0)
        fetch(last, True, part, edge.at[part], sems.at[part])
    wo_copy.start()

    def ready(part):
        pltpu.make_async_copy(kv.at[part], kv.at[part], sems.at[part]).wait()
        pltpu.make_async_copy(edge.at[part], edge.at[part], sems.at[part]).wait()
        settle(kv.at[part], new_ref[part], beta, lambda old: edge[part].astype(F32), (last, last + 1))

    ready(0)
    weights[...] = softmax_weights(stacked(q_ref), kv.at[0], scores, None)
    k_copy = pltpu.make_async_copy(kv.at[0], k_out.at[layer], out_sems.at[0])
    k_copy.start()
    ready(1)
    wo_copy.wait()
    v_copy = pltpu.make_async_copy(kv.at[1], v_out.at[layer], out_sems.at[1])
    mix_and_project(weights, kv.at[1], v_copy, wo, mlp_ref, part_ref)
    k_copy.wait()
    v_copy.wait()


def attend_window(layer, size, ids, q, new_kv, mlp, w_out, k_t, v_t, nears, pipe, k_buf, v_buf):
    heads, dim, shard = k_t.shape[2:]
    half = shard // UNIT
    n_pipe = len(pipe)
    return pl.pallas_call(
        functools.partial(window_body, layer, size, half, n_pipe),
        in_specs=[SMEM, VMEM, VMEM, VMEM] + [HBM] * (5 + n_pipe + 2),
        out_specs=[VMEM, HBM, HBM],
        out_shape=[jax.ShapeDtypeStruct(mlp.shape, F32), jax.ShapeDtypeStruct(k_buf.shape, BF16), jax.ShapeDtypeStruct(v_buf.shape, BF16)],
        scratch_shapes=[
            pltpu.VMEM((2, heads, dim, 2 * shard), BF16),
            pltpu.VMEM((2, heads, dim, UNIT), BF16),
            pltpu.VMEM(w_out.shape[1:], BF16),
            pltpu.VMEM((q.shape[0] * q.shape[1], 2 * shard), F32),
            pltpu.VMEM((q.shape[0] * q.shape[1], 2 * shard), BF16),
            pltpu.SemaphoreType.DMA((2,)),
            pltpu.SemaphoreType.DMA((2,)),
            pltpu.SemaphoreType.DMA,
        ],
        input_output_aliases={9 + n_pipe: 1, 10 + n_pipe: 2},
        cost_estimate=cost(16 * heads * dim * shard),
        name="attend_window",
    )(ids, q, new_kv, mlp, w_out, k_t, v_t, *nears, *pipe, k_buf, v_buf)


def place_body(layer, part, relations, ids, new_ref, own, near, *refs):
    blocks = {1: near}
    blocks.update(zip([r for r in relations if r > 1], refs))
    out, kv, sems, out_sem = refs[-4:]
    me = ids[0]
    length = ids[1 + me]
    shard = own.shape[-1]
    units = shard // UNIT
    spans = {r: pl.ds(pl.multiple_of(jnp.bitwise_xor(me, r) * shard, UNIT), shard) for r in relations}
    for i, r in enumerate(relations):
        src = (own, near)[r].at[layer, me] if r < 2 else blocks[r]
        move([(src, kv.at[:, :, spans[r]], sems.at[i])])
    stores = []
    for i, r in enumerate(relations):
        view = kv.at[:, :, spans[r]]
        pltpu.make_async_copy(view, view, sems.at[i]).wait()
        first = jnp.bitwise_xor(me, r) * units
        settle(kv, new_ref[part], length, jnp.zeros_like, (jnp.maximum(first, length // UNIT), first + units))
        stores.append(pltpu.make_async_copy(view, out.at[:, :, spans[r]], out_sem))
        stores[-1].start()
    for store in stores:
        store.wait()


def place(layer, part, relations, ids, new_kv, own, near, blocks, buf):
    heads, dim, shard = own.shape[2:]
    n_in = 4 + len(blocks)
    return pl.pallas_call(
        functools.partial(place_body, layer, part, relations),
        in_specs=[SMEM, VMEM] + [HBM] * (3 + len(blocks)),
        out_specs=HBM,
        out_shape=jax.ShapeDtypeStruct(buf.shape, BF16),
        scratch_shapes=[pltpu.VMEM(buf.shape, BF16), pltpu.SemaphoreType.DMA((len(relations),)), pltpu.SemaphoreType.DMA],
        input_output_aliases={n_in: 0},
        cost_estimate=cost(4 * heads * dim * shard * len(relations)),
        name="place",
    )(ids, new_kv, own, near, *blocks, buf)


def in_tp_order(tp, parts, residual):
    for t in range(4):
        at = jnp.bitwise_xor(tp, t)
        pick = parts[3]
        for r in range(3):
            pick = jnp.where(at == r, parts[r], pick)
        total = pick if t == 0 else total + pick
    return (residual.astype(F32) + total).astype(BF16)


def scores_body(layer, ids, q_ref, new_ref, own, near, far, cross, k_in, w_ref, last_ref, k_out, kv, sem, out_sem, scores):
    me = ids[0]
    length = ids[1 + me]
    shard = own.shape[-1]
    sources = [own.at[layer, me], near.at[layer, me], far, cross]
    move([(src, kv.at[:, :, pl.ds(pl.multiple_of(jnp.bitwise_xor(me, r) * shard, UNIT), shard)], sem) for r, src in enumerate(sources)])
    pltpu.make_async_copy(kv, kv, sem).wait()
    settle(kv, new_ref[0], length, jnp.zeros_like, (length // UNIT, kv.shape[-1] // UNIT))
    weights = softmax_weights(stacked(q_ref), kv, scores, length)
    copy = pltpu.make_async_copy(kv, k_out, out_sem)
    copy.start()
    newest = lax.broadcasted_iota(jnp.int32, (1, weights.shape[1]), 1) == length
    weights = weights.astype(F32)
    last_ref[...] = jnp.broadcast_to(jnp.where(newest, weights, 0.0).sum(axis=-1, keepdims=True), last_ref.shape)
    w_ref[...] = jnp.where(newest, 0.0, weights).astype(BF16)
    copy.wait()


def score_global(layer, ids, q, new_kv, k_t, near, blocks, k_buf):
    n_q = q.shape[0] * q.shape[1]
    seq = k_buf.shape[-1]
    return pl.pallas_call(
        functools.partial(scores_body, layer),
        in_specs=[SMEM, VMEM, VMEM] + [HBM] * 5,
        out_specs=[VMEM, VMEM, HBM],
        out_shape=[jax.ShapeDtypeStruct((n_q, seq), BF16), jax.ShapeDtypeStruct((n_q, UNIT), F32), jax.ShapeDtypeStruct(k_buf.shape, BF16)],
        scratch_shapes=[pltpu.VMEM(k_buf.shape, BF16), pltpu.SemaphoreType.DMA, pltpu.SemaphoreType.DMA, pltpu.VMEM((n_q, seq), F32)],
        input_output_aliases={7: 2},
        cost_estimate=cost(4 * k_buf.size),
        name="scores",
    )(ids, q, new_kv, k_t, near, *blocks, k_buf)


def greet(axis):
    me = lax.axis_index(axis)
    peers = [{axis: jnp.bitwise_xor(me, r)} for r in PEERS]
    for peer in peers:
        pl.semaphore_signal(pltpu.get_barrier_semaphore(), inc=1, device_id=peer, device_id_type=pl.DeviceIdType.MESH)
    return peers


def share(peers, src, slots, send_sems, recv_sems):
    pl.semaphore_wait(pltpu.get_barrier_semaphore(), len(PEERS))
    copies = [
        pltpu.make_async_remote_copy(src, slots.at[i], send_sems.at[i], recv_sems.at[i], device_id=peer, device_id_type=pl.DeviceIdType.MESH)
        for i, peer in enumerate(peers)
    ]
    for copy in copies:
        copy.start()
    return copies


def settled_sum(copies, mine, slots, residual):
    for copy in copies:
        copy.wait()
    return in_tp_order(lax.axis_index("tp"), [mine[...]] + [slots[i] for i in range(len(PEERS))], residual)


def finish_body(layer, ids, w_ref, last_ref, new_ref, mlp_ref, h_ref, wo_hbm, own, near, far, cross, v_in, out_ref, v_out, shards, placed, wo, part_ref, slots, sems, send_sems, recv_sems):
    me = lax.axis_index("sp")
    peers = greet("tp")
    length = ids[1 + me]
    shard = own.shape[-1]
    sources = [own.at[layer, me], near.at[layer, me], far, cross]
    loads = [pltpu.make_async_copy(src, shards.at[r], sems.at[r]) for r, src in enumerate(sources)]
    loads.append(pltpu.make_async_copy(wo_hbm.at[layer], wo, sems.at[4]))
    for load in loads:
        load.start()
    n_q = w_ref.shape[0]
    upper = lax.broadcasted_iota(jnp.int32, (n_q, 1), 0) < n_q // 2
    dims = (((1,), (1,)), ((), ()))
    mixed = last_ref[:, 0:1] * jnp.where(upper, new_ref[1, 0:1], new_ref[1, 1:2])
    for r in range(4):
        loads[r].wait()
        at = pl.ds(pl.multiple_of(jnp.bitwise_xor(me, r) * shard, UNIT), shard)
        weights = w_ref[:, at]
        m0 = lax.dot_general(weights, shards[r, 0], dims, preferred_element_type=F32)
        m1 = lax.dot_general(weights, shards[r, 1], dims, preferred_element_type=F32)
        mixed = mixed + jnp.where(upper, m0, m1)
    mixed = mixed.astype(BF16).astype(F32)
    flat = jnp.concatenate([mixed[j:j + 1] for j in range(n_q)], axis=1)
    flat = jnp.broadcast_to(flat, (8, flat.shape[1])).astype(BF16)
    loads[4].wait()
    part_ref[...] = jnp.dot(flat, wo[...], preferred_element_type=F32)[0:1] + mlp_ref[...]
    copies = share(peers, part_ref, slots, send_sems, recv_sems)
    position = lax.broadcasted_iota(jnp.int32, (1, shard), 1) + jnp.bitwise_xor(me, 3) * shard
    for head in range(placed.shape[0]):
        fresh = new_ref[1][head:head + 1].T
        old = shards[3, head].astype(F32)
        placed[head] = jnp.where(position < length, old, jnp.where(position == length, fresh, 0.0)).astype(BF16)
    out_ref[...] = settled_sum(copies, part_ref, slots, h_ref[...])
    store = pltpu.make_async_copy(placed, v_out.at[:, :, at], sems.at[3])
    store.start()
    store.wait()


def finish(layer, ids, weights, last, new_kv, mlp, residual, w_out, v_t, near, blocks, v_buf):
    heads, dim, shard = v_t.shape[2:]
    return pl.pallas_call(
        functools.partial(finish_body, layer),
        in_specs=[SMEM] + [VMEM] * 5 + [HBM] * 6,
        out_specs=[VMEM, HBM],
        out_shape=[jax.ShapeDtypeStruct(residual.shape, BF16), jax.ShapeDtypeStruct(v_buf.shape, BF16)],
        scratch_shapes=[
            pltpu.VMEM((4, heads, dim, shard), BF16),
            pltpu.VMEM((heads, dim, shard), BF16),
            pltpu.VMEM(w_out.shape[1:], BF16),
            pltpu.VMEM(mlp.shape, F32),
            pltpu.VMEM((3,) + mlp.shape, F32),
            pltpu.SemaphoreType.DMA((5,)),
            pltpu.SemaphoreType.DMA((3,)),
            pltpu.SemaphoreType.DMA((3,)),
        ],
        input_output_aliases={11: 1},
        compiler_params=pltpu.CompilerParams(collective_id=layer + 1, has_side_effects=True),
        cost_estimate=cost(16 * heads * dim * shard),
        name="finish",
    )(ids, weights, last, new_kv, mlp, residual, w_out, v_t, near, *blocks, v_buf)


def turned(proj, dim, cosine, sine):
    if cosine is None:
        return proj
    lane = lax.broadcasted_iota(jnp.int32, proj.shape, 1)
    ahead = pltpu.roll(proj, proj.shape[1] - dim // 2, 1)
    behind = pltpu.roll(proj, dim // 2, 1)
    return proj * cosine[...] + jnp.where(lax.rem(lane, dim) < dim // 2, -ahead, behind) * sine[...]


def normed(h, gain, layer):
    rows32 = h.astype(F32)
    centered = rows32 - rows32.mean(axis=-1, keepdims=True)
    variance = (centered * centered).mean(axis=-1, keepdims=True)
    return centered * lax.rsqrt(variance + NORM_EPS) * gain[...].astype(F32)[layer:layer + 1]


def over_rows(u, mats, at_once=8):
    def block(i, sums):
        rows = lanes(i * at_once, at_once)
        return tuple(t + jnp.dot(u[:, rows], m[rows, :], preferred_element_type=F32) for t, m in zip(sums, mats))

    return lax.fori_loop(0, u.shape[1] // (at_once * UNIT), block, tuple(jnp.zeros((u.shape[0], m.shape[1]), F32) for m in mats))


def rounded(proj):
    return proj.astype(BF16).astype(F32)


def heads_out(ref, row, dim):
    for head in range(ref.shape[0]):
        ref[head:head + 1, :] = row[0:1, head * dim:(head + 1) * dim]


def sum_front_body(layer, dim, n_turns, part_ref, h_ref, gain, *refs):
    cosine, sine = refs[:n_turns] or (None, None)
    sources, (h_out, q_out, new_out, mlp_out), refs = refs[n_turns:n_turns + 6], refs[n_turns + 6:n_turns + 10], refs[n_turns + 10:]
    wq, wk, wv, wg, wu, wd, slots, u, gate, up, sems, send_sems, recv_sems = refs
    peers = greet("tp")
    small = [pltpu.make_async_copy(src.at[layer], dst, sems.at[i, 0]) for i, (src, dst) in enumerate(zip(sources[:3], (wq, wk, wv)))]
    for copy in small:
        copy.start()
    steps = sems.shape[1]
    depth = wg.shape[0] // steps

    def piece(which, i):
        rows = pl.ds(pl.multiple_of(i * depth, depth), depth)
        return pltpu.make_async_copy(sources[which].at[layer, rows], (wg, wu, wd)[which - 3].at[rows], sems.at[which, i])

    def begin(i, carry):
        piece(3, i).start()
        piece(4, i).start()
        return carry

    def begin_down(i, carry):
        piece(5, i).start()
        return carry

    lax.fori_loop(0, steps, begin, 0)
    lax.fori_loop(0, steps, begin_down, 0)
    h = settled_sum(share(peers, part_ref, slots, send_sems, recv_sems), part_ref, slots, h_ref[...])
    h_out[...] = h
    u[...] = jnp.broadcast_to(normed(h, gain, layer), u.shape).astype(BF16)
    gate[...] = jnp.zeros_like(gate)
    up[...] = jnp.zeros_like(up)
    for copy in small:
        copy.wait()
    query, key_new, value_new = over_rows(u, (wq, wk, wv), 4)
    key_new = turned(key_new, dim, cosine, sine)
    heads_out(new_out.at[0], rounded(key_new), dim)
    heads_out(new_out.at[1], rounded(value_new), dim)
    width = key_new.shape[1]
    for j in range(q_out.shape[0]):
        heads_out(q_out.at[j], rounded(turned(query[:, j * width:(j + 1) * width], dim, cosine, sine)), dim)

    def widen(i, carry):
        piece(3, i).wait()
        piece(4, i).wait()
        rows = pl.ds(pl.multiple_of(i * depth, depth), depth)
        gate[...] += jnp.dot(u[:, rows], wg[rows, :], preferred_element_type=F32)
        up[...] += jnp.dot(u[:, rows], wu[rows, :], preferred_element_type=F32)
        return carry

    lax.fori_loop(0, steps, widen, 0)
    u[...] = (jax.nn.silu(gate[...]) * up[...]).astype(BF16)
    gate[...] = jnp.zeros_like(gate)

    def narrow(i, carry):
        piece(5, i).wait()
        rows = pl.ds(pl.multiple_of(i * depth, depth), depth)
        gate[...] += jnp.dot(u[:, rows], wd[rows, :], preferred_element_type=F32)
        return carry

    lax.fori_loop(0, steps, narrow, 0)
    mlp_out[...] = gate[0:1, :]


def sum_front(layer, dim, part, residual, ln_gain, turns, *weights):
    width = residual.shape[1]
    q_width, kv_width = weights[0].shape[2], weights[1].shape[2]
    wide = pltpu.VMEM((8, width), F32)
    return pl.pallas_call(
        functools.partial(sum_front_body, layer, dim, len(turns)),
        in_specs=[VMEM] * (3 + len(turns)) + [HBM] * 6,
        out_specs=[VMEM] * 4,
        out_shape=[
            jax.ShapeDtypeStruct((1, width), BF16),
            jax.ShapeDtypeStruct((FFN_STEPS, q_width // FFN_STEPS // dim, dim), F32),
            jax.ShapeDtypeStruct((2, kv_width // dim, dim), F32),
            jax.ShapeDtypeStruct((1, width), F32),
        ],
        scratch_shapes=[pltpu.VMEM(w.shape[1:], BF16) for w in weights]
        + [pltpu.VMEM((3,) + part.shape, F32), pltpu.VMEM((8, width), BF16), wide, wide, pltpu.SemaphoreType.DMA((6, 8)), pltpu.SemaphoreType.DMA((3,)), pltpu.SemaphoreType.DMA((3,))],
        compiler_params=pltpu.CompilerParams(collective_id=layer, has_side_effects=True),
        cost_estimate=cost(2 * sum(w[0].size for w in weights)),
        name="sum_front",
    )(part, residual, ln_gain, *turns, *weights)


def front_body(layer, dim, h_ref, gain, cosine, sine, wq, wk, wv, wg, wu, wd, q_out, new_out, mlp_out, u, acc):
    step = pl.program_id(0)

    @pl.when(step == 0)
    def _():
        u[...] = jnp.broadcast_to(normed(h_ref[...], gain, layer), u.shape).astype(BF16)
        acc[...] = jnp.zeros_like(acc)
        key_new, value_new = over_rows(u, (wk.at[0], wv.at[0]))
        heads_out(new_out.at[0], rounded(turned(key_new, dim, cosine, sine)), dim)
        heads_out(new_out.at[1], rounded(value_new), dim)

    query, gate, up = over_rows(u, (wq.at[0], wg.at[0], wu.at[0]))
    heads_out(q_out.at[0], rounded(turned(query, dim, cosine, sine)), dim)
    active = (jax.nn.silu(gate) * up).astype(BF16)

    def down(i, carry):
        at = lanes(i * 8, 8)
        acc[:, at] += jnp.dot(active, wd[0, :, at], preferred_element_type=F32)
        return carry

    lax.fori_loop(0, acc.shape[1] // (8 * UNIT), down, 0)

    @pl.when(step == FFN_STEPS - 1)
    def _():
        mlp_out[...] = acc[0:1, :]


def front(layer, dim, residual, ln_gain, turns, w_query, w_key, w_value, w_gate, w_up, w_down):
    width = residual.shape[1]
    q_width, kv_width, ffn = w_query.shape[2], w_key.shape[2], w_gate.shape[2]
    q_step, ffn_step = q_width // FFN_STEPS, ffn // FFN_STEPS
    whole = lambda *shape: pl.BlockSpec(shape, lambda j: (0,) * len(shape))
    col = lambda rows, cols: pl.BlockSpec((1, rows, cols), lambda j: (layer, 0, j))
    fixed = lambda rows, cols: pl.BlockSpec((1, rows, cols), lambda j: (layer, 0, 0))
    return pl.pallas_call(
        functools.partial(front_body, layer, dim),
        grid=(FFN_STEPS,),
        in_specs=[whole(1, width), whole(*ln_gain.shape)] + [whole(1, kv_width)] * len(turns)
        + [col(width, q_step), fixed(width, kv_width), fixed(width, kv_width), col(width, ffn_step), col(width, ffn_step), pl.BlockSpec((1, ffn_step, width), lambda j: (layer, j, 0))],
        out_specs=[pl.BlockSpec((1, q_step // dim, dim), lambda j: (j, 0, 0)), whole(2, kv_width // dim, dim), whole(1, width)],
        out_shape=[
            jax.ShapeDtypeStruct((FFN_STEPS, q_step // dim, dim), F32),
            jax.ShapeDtypeStruct((2, kv_width // dim, dim), F32),
            jax.ShapeDtypeStruct((1, width), F32),
        ],
        scratch_shapes=[pltpu.VMEM((8, width), BF16), pltpu.VMEM((8, width), F32)],
        compiler_params=pltpu.CompilerParams(dimension_semantics=("arbitrary",)),
        cost_estimate=cost(2 * width * (q_width + 2 * kv_width + 3 * ffn)),
        name="front",
    )(residual, ln_gain, *turns, w_query, w_key, w_value, w_gate, w_up, w_down)


def fresh_body(*refs):
    pass


def fresh_buffers(shapes):
    return pl.pallas_call(fresh_body, out_specs=[HBM] * len(shapes), out_shape=[jax.ShapeDtypeStruct(s, BF16) for s in shapes], name="fresh")()


def solution(mesh):
    cache_spec = P(None, "dp", "tp", "sp", None)
    row_spec = P(("dp", "sp"), None)
    col_spec = P(None, None, "tp")
    inner_spec = P(None, "tp", None)
    window_spec = P(None, ("dp", "sp"), "tp", None, None)
    global_spec = P(("dp", "sp"), "tp", None, None)
    in_specs = (cache_spec, cache_spec, P("dp"), row_spec, P(None, None), col_spec, col_spec, col_spec, inner_spec, col_spec, col_spec, inner_spec)
    out_specs = (row_spec, window_spec, window_spec, global_spec, global_spec)
    n_sp = mesh.shape["sp"]

    def swap(t, axis, relation):
        return lax.ppermute(t, axis, [(i, i ^ relation) for i in range(n_sp)])

    def device_step(k_cache, v_cache, lengths, hidden, ln_gain, w_query, w_key, w_value, w_out, w_gate, w_up, w_down):
        n_layers = w_query.shape[0]
        heads, shard, dim = k_cache.shape[2:]
        half = shard // UNIT
        final = n_layers - 1
        me = lax.axis_index("sp").astype(jnp.int32)
        ids = jnp.concatenate([me[None], lengths])
        k_t = jnp.swapaxes(k_cache, 3, 4)
        v_t = jnp.swapaxes(v_cache, 3, 4)

        inv_freq = 1.0 / (ROPE_BASE ** (jnp.arange(dim // 2, dtype=F32) * 2.0 / dim))
        angles = lax.dynamic_slice_in_dim(lengths, me, 1).astype(F32)[:, None] * inv_freq[None, :]
        repeat = 2 * w_key.shape[2] // dim
        turns = (jnp.tile(jnp.cos(angles), (1, repeat)), jnp.tile(jnp.sin(angles), (1, repeat)))

        _, counts = crossing(lengths - WINDOW, jnp.arange(n_sp) >= n_sp // 2, 2 * half)
        need = lax.pmax(jnp.max((counts.reshape(2, -1).sum(axis=1) + 1) // 2), "dp")
        choice = sum((need > size).astype(jnp.int32) for size in SIZES[:-1])

        def block(t, layer, relation):
            return lax.dynamic_slice(t, (layer, jnp.bitwise_xor(me, relation), 0, 0, 0), (1, 1, heads, dim, shard))[0, 0]

        weights = (w_query, w_key, w_value, w_gate, w_up, w_down)
        k_first = [swap(block(k_t, 0, r), "sp", r) for r in (2, 3)]
        v_far = swap(block(v_t, 0, 2), "sp", 2)
        v_cut = block(v_t, 0, 3)
        nears = [swap(k_t, "sp", 1), swap(v_t, "sp", 1)]
        begun = front(0, dim, hidden, ln_gain, turns, *weights)

        def run(size):
            return run_scoped(size)

        def run_scoped(size, ids=ids):
            k_win, v_win = fresh_buffers([(final, heads, dim, WINDOW)] * 2)
            pipes = [k_first + [v_far, swap(v_cut, "sp", 3)]]
            for layer in range(1, final):
                packed = pack(layer, size, ids, k_t, v_t, nears)
                pipes.append([swap(p, "sp", 2) for p in packed])
            residual, (q, new_kv, mlp) = hidden, begun
            for layer in range(n_layers):
                sliding = layer < final
                if layer:
                    residual, q, new_kv, mlp = sum_front(layer, dim, part, residual, ln_gain, turns if sliding else (), *weights)
                if layer == 1:
                    cuts = after([block(t, final, r) for t in (k_t, v_t) for r in (2, 3)], q)
                    late = [swap(c, "sp", 2 + i % 2) for i, c in enumerate(cuts)]
                if sliding:
                    if layer and size < 2 * half:
                        pipes[layer].append(swap(after(pipes[layer][0], q), "sp", 1))
                    part, k_win, v_win = attend_window(layer, size if layer else None, ids, q, new_kv, mlp, w_out, k_t, v_t, nears, pipes[layer], k_win, v_win)
                else:
                    k_glob, v_glob = fresh_buffers([(heads, dim, n_sp * shard)] * 2)
                    attn, last, k_glob = score_global(layer, ids, q, new_kv, k_t, nears[0], late[:2], k_glob)
                    ids = after(ids, attn)
                    v_glob = place(final, 1, (0, 1, 2), ids, new_kv, v_t, nears[1], late[2:3], v_glob)
                    residual, v_glob = finish(layer, ids, attn, last, new_kv, mlp, residual, w_out, v_t, nears[1], late[2:], v_glob)
            return residual, k_win, v_win, k_glob, v_glob

        if len(SIZES) == 1:
            out, k_win, v_win, k_glob, v_glob = run(SIZES[0])
        else:
            out, k_win, v_win, k_glob, v_glob = lax.switch(choice, [functools.partial(run, size) for size in SIZES])
        back = lambda t: jnp.swapaxes(t, -1, -2)
        return out, back(k_win)[:, None], back(v_win)[:, None], back(k_glob)[None], back(v_glob)[None]


    return jax.shard_map(device_step, mesh=mesh, in_specs=in_specs, out_specs=out_specs, check_vma=False)
```
